32 devices in a mesh: gx: 4 (over z), gy: 4 (over x, core), gz: 2 (over y).
Axes of the slice: x: 2, y: 2, z: 4, core: 2. Of those that a mesh axis runs over, the one named last changes fastest.
Arguments:
- residual: float32 [32, 32, 256], P('gx', 'gy', 'gz'), may hold values from -18 to 18
- direction: float32 [32, 32, 256], P('gx', 'gy', 'gz'), may hold values from -18 to 18
Outputs:
- powers: float32 [2, 4, 32, 32, 256], P(None, None, 'gx', 'gy', 'gz')
- gram_matrix: float32 [9, 9], replicated
- projections: float32 [9], replicated
The draws below stay inside these ranges and needn't reach their ends.
All inputs are finite; a program needn't handle non-finite values.
Results may differ from the reference program's by a relative error of at most 0.00029.
Values sent between devices are 32-bit elements; how exact they have to be, the bound alone decides.
A program may use at most 64 MiB of HBM per device.

```python
import jax
import jax.numpy as jnp

STEPS = 4
MARGIN = 1
SWEEPS = 3
NX = 32
NY = 32
NZ = 256
N_GX = 4
N_GY = 4
N_GZ = 2


def cell_law(key, salt):
    shape_cells = (NX, NY, NZ)
    gaussian = jnp.clip(jax.random.normal(jax.random.fold_in(key, salt), shape_cells, jnp.float32), -4.0, 4.0)
    levels = jax.random.uniform(jax.random.fold_in(key, salt + 1), shape_cells, jnp.float32)
    spread = 0.3 * jnp.exp(levels * jnp.log(10.0))
    along_x = jnp.arange(NX, dtype=jnp.float32) / max(NX - 1, 1)
    ramped = 0.5 + along_x
    return gaussian * spread * ramped[:, None, None]


def draw_residual(key, part):
    return cell_law(key, 1)


def draw_direction(key, part):
    return cell_law(key, 5)


def setup_inputs(seed: int = 0) -> dict:
    arg_keys = jax.random.split(jax.random.key(seed), 3)
    residual = draw_residual(jax.random.fold_in(arg_keys[2], 71), 0)
    direction = draw_direction(jax.random.fold_in(arg_keys[2], 71), 0)
    return dict(residual=residual, direction=direction)


SWEEP_SCALE = 1.0 / 9.0


def grid_operator(values):
    padded = jnp.pad(values, 1)
    center = padded[1:-1, 1:-1, 1:-1]
    beside = padded[2:, 1:-1, 1:-1] + padded[:-2, 1:-1, 1:-1]
    beside = beside + padded[1:-1, 2:, 1:-1] + padded[1:-1, :-2, 1:-1]
    beside = beside + padded[1:-1, 1:-1, 2:] + padded[1:-1, 1:-1, :-2]
    return 6.0 * center - beside


def block_operator(values):
    padded = jnp.pad(values, [(0, 0), (1, 1), (0, 0), (1, 1), (0, 0), (1, 1)])
    center = padded[:, 1:-1, :, 1:-1, :, 1:-1]
    beside = padded[:, 2:, :, 1:-1, :, 1:-1] + padded[:, :-2, :, 1:-1, :, 1:-1]
    beside = beside + padded[:, 1:-1, :, 2:, :, 1:-1] + padded[:, 1:-1, :, :-2, :, 1:-1]
    beside = beside + padded[:, 1:-1, :, 1:-1, :, 2:] + padded[:, 1:-1, :, 1:-1, :, :-2]
    return 6.0 * center - beside


def extend_axis(values, position, blocks, margin):
    leading = jnp.moveaxis(values, position, 0)
    length = leading.shape[0]
    block_width = length // blocks
    trailing = leading.shape[1:]
    padded = jnp.pad(leading, [(margin, margin)] + [(0, 0)] * len(trailing))
    below_part = padded[0:length].reshape((blocks, block_width) + trailing)[:, :margin]
    middle = leading.reshape((blocks, block_width) + trailing)
    above_part = padded[2 * margin:2 * margin + length].reshape((blocks, block_width) + trailing)[:, block_width - margin:]
    joined = jnp.concatenate([below_part, middle, above_part], axis=1)
    return jnp.moveaxis(joined, (0, 1), (position, position + 1))


def fold_axis(values, position, margin):
    leading = jnp.moveaxis(values, (position, position + 1), (0, 1))
    blocks = leading.shape[0]
    block_width = leading.shape[1] - 2 * margin
    trailing = leading.shape[2:]
    length = blocks * block_width
    zero_tail = [(0, 0)] * len(trailing)
    middle = leading[:, margin:margin + block_width].reshape((length,) + trailing)
    below_part = jnp.pad(leading[:, :margin], [(0, 0), (0, block_width - margin)] + zero_tail).reshape((length,) + trailing)
    above_part = jnp.pad(leading[:, block_width + margin:], [(0, 0), (block_width - margin, 0)] + zero_tail).reshape((length,) + trailing)
    combined = jnp.pad(middle, [(margin, margin)] + zero_tail)
    combined = combined + jnp.pad(below_part, [(0, 2 * margin)] + zero_tail)
    combined = combined + jnp.pad(above_part, [(2 * margin, 0)] + zero_tail)
    return jnp.moveaxis(combined[margin:margin + length], 0, position)


def extend_grid(values):
    values = extend_axis(values, 0, N_GX, MARGIN)
    values = extend_axis(values, 2, N_GY, MARGIN)
    return extend_axis(values, 4, N_GZ, MARGIN)


def fold_grid(values):
    values = fold_axis(values, 4, MARGIN)
    values = fold_axis(values, 2, MARGIN)
    return fold_axis(values, 0, MARGIN)


def precondition(values, mask):
    source = mask * extend_grid(values)
    iterate = mask * (SWEEP_SCALE * source)
    for sweep_index in range(SWEEPS - 1):
        iterate = mask * (iterate + SWEEP_SCALE * (source - block_operator(iterate)))
    return fold_grid(iterate)


def reference(residual, direction):
    mask = extend_grid(jnp.ones(residual.shape, jnp.float32))
    cell_count = NX * NY * NZ
    p_fields = [direction]
    p_images = []
    for step_index in range(STEPS):
        p_images.append(grid_operator(p_fields[-1]))
        p_fields.append(precondition(p_images[-1], mask))
    p_images.append(grid_operator(p_fields[-1]))
    z_fields = [precondition(residual, mask)]
    z_images = []
    for step_index in range(STEPS - 1):
        z_images.append(grid_operator(z_fields[-1]))
        z_fields.append(precondition(z_images[-1], mask))
    z_images.append(grid_operator(z_fields[-1]))
    basis = p_fields + z_fields
    images = p_images + z_images
    table_rows = []
    for left_field in basis:
        table_rows.append(jnp.stack([jnp.sum(left_field * right_image) for right_image in images]))
    gram_matrix = jnp.stack(table_rows) / cell_count
    projections = jnp.stack([jnp.sum(left_field * residual) for left_field in basis]) / cell_count
    powers = jnp.stack([jnp.stack(p_fields[1:]), jnp.stack(z_fields)])
    return (powers, gram_matrix, projections)
```

```python
import functools

import jax
import jax.numpy as jnp
from jax import lax
from jax.experimental import pallas as pl
from jax.experimental.pallas import tpu as pltpu
from jax.sharding import PartitionSpec as P

STEPS = 4
LANES = 128
MESH = pl.DeviceIdType.MESH
HIGHEST = lax.Precision.HIGHEST
F32 = jnp.float32
AXES = ("gx", "gy", "gz")
GAMMA, BETA, ALPHA, DELTA = 13.0 / 81.0, 5.0 / 243.0, 1.0 / 729.0, 1.0 / 1458.0
P_CHAIN, Z_CHAIN = 0, 1
REACH = ((6, 5), (7, 7))
CHUNK = 4
OFFSETS = [(dx, dy, dz) for dx in (-1, 0, 1) for dy in (-1, 0, 1) for dz in (-1, 0, 1) if (dx, dy, dz) != (0, 0, 0)]


def as_f32(flag):
    return jnp.where(flag, 1.0, 0.0).astype(F32)


def axis_terms(at, width, low, high, place, count):
    inside = (place * width + at >= 0) & (place * width + at < count * width)
    cover = ((at == -1) | (at == 0)) & low | ((at == width - 1) | (at == width)) & high
    inner = ((at == -2) | (at == 1)) & low | ((at == width - 2) | (at == width + 1)) & high
    below = (at == 1) & low | (at == width + 1) & high
    above = (at == -2) & low | (at == width - 2) & high
    mask = as_f32(inside)
    return (1.0 + as_f32(cover)) * mask, as_f32(inner), 1.0 - 0.5 * as_f32(below), 1.0 - 0.5 * as_f32(above), mask


def kernel(
    counts, dims, near, res_ref, dir_ref, pow_ref, gram_ref, proj_ref,
    main, pack, got, face, cbuf, czbuf, sbuf, szbuf, image, base, tab, ztab, t_ref, red0, red1,
    in_sem, out_sem, s_sem, r_sem, s0_sem, r0_sem, s1_sem, r1_sem,
):
    nx, ny, nz = counts
    cx, cy, cz = dims
    group = LANES // cx
    half = group // 2
    rows = 3 * cy
    place = [lax.axis_index(a) for a in AXES]
    gx, gy, gz = place
    low = [place[i] > 0 for i in range(3)]
    high = [place[i] < counts[i] - 1 for i in range(3)]
    total = 2 * STEPS + 1

    def exists(offset):
        ok = None
        for i, step in enumerate(offset):
            if step:
                test = low[i] if step < 0 else high[i]
                ok = test if ok is None else jnp.logical_and(ok, test)
        return ok

    def flip(offset):
        return tuple(-s for s in offset)

    def target(offset):
        return {AXES[i]: place[i] + s for i, s in enumerate(offset) if s}

    def ahead(axes):
        def make(k):
            out = {}
            for a in reversed(axes):
                k, step = divmod(k, counts[AXES.index(a)])
                if step:
                    out[a] = lax.rem(place[AXES.index(a)] + step, counts[AXES.index(a)])
            return out
        size = 1
        for a in axes:
            size *= counts[AXES.index(a)]
        return size, make

    loads = [
        pltpu.make_async_copy(ref, main.at[c, 0, pl.ds(cx, cx), pl.ds(cy, cy)], in_sem.at[c])
        for c, ref in ((Z_CHAIN, res_ref), (P_CHAIN, dir_ref))
    ]
    for copy in loads:
        copy.start()

    barrier = pltpu.get_barrier_semaphore()
    expected = 0
    for offset in OFFSETS:
        @pl.when(exists(offset))
        def _():
            pl.semaphore_signal(barrier, 1, device_id=target(offset), device_id_type=MESH)
        expected = expected + exists(offset).astype(jnp.int32)
    if not near:
        for axes in (("gy", "gz"), ("gx",)):
            size, make = ahead(axes)
            for k in range(1, size):
                pl.semaphore_signal(barrier, 1, device_id=make(k), device_id_type=MESH)
            expected = expected + (size - 1)

    fields = [(c, f) for c in (0, 1) for f in (0, 2)]
    for flag, xs, ys in (
        (low[0], pl.ds(0, cx), pl.ds(0, rows)), (high[0], pl.ds(2 * cx, cx), pl.ds(0, rows)),
        (low[1], pl.ds(0, 3 * cx), pl.ds(0, cy)), (high[1], pl.ds(0, 3 * cx), pl.ds(2 * cy, cy)),
    ):
        @pl.when(jnp.logical_not(flag))
        def _():
            for c, f in fields:
                main[c, f, xs, ys] = jnp.zeros((xs.size, ys.size, LANES), F32)
    for flag, ss, xs, ys in (
        (low[2], 0, pl.ds(0, 3), pl.ds(0, rows)), (high[2], 1, pl.ds(0, 3), pl.ds(0, rows)),
        (low[0], None, pl.ds(0, 1), pl.ds(0, rows)), (high[0], None, pl.ds(2, 1), pl.ds(0, rows)),
        (low[1], None, pl.ds(0, 3), pl.ds(0, cy)), (high[1], None, pl.ds(0, 3), pl.ds(2 * cy, cy)),
    ):
        @pl.when(jnp.logical_not(flag))
        def _():
            for c in (0, 1):
                for s in (0, 1):
                    for side in ((0, 1) if ss is None else (ss,)):
                        got[c, s, side, xs, ys] = jnp.zeros((xs.size, ys.size, LANES), F32)

    lane = lax.broadcasted_iota(jnp.int32, (rows, LANES), 1)
    row = lax.broadcasted_iota(jnp.int32, (rows, LANES), 0)
    wy, fy, up_y, down_y, my = axis_terms(row - cy, cy, low[1], high[1], gy, ny)
    wz, fz, up_z, down_z, mz = axis_terms(lane, cz, low[2], high[2], gz, nz)

    def x_terms(x):
        return axis_terms(jnp.int32(x), cx, low[0], high[0], gx, nx)

    D_REPS = (-3, -1, 0, 3, cx - 1, cx, cx + 2)
    D0, AM0, M0, G0, UPY, DOWNY, UPZ, DOWNZ = 0, 7, 10, 13, 18, 19, 20, 21
    wyz, myz, fyz = wy * wz, my * mz, fy + fz
    for k, x in enumerate(D_REPS):
        tab[D0 + k] = wyz * x_terms(x)[0]
    for k, x in enumerate((-3, 3, cx + 2)):
        mask = myz * x_terms(x)[4]
        tab[AM0 + k] = mask * ALPHA
        tab[M0 + k] = mask
    for k, x in enumerate((3, -2, 1, cx - 2, cx + 1)):
        tab[G0 + k] = GAMMA + DELTA * (fyz + x_terms(x)[1])
    tab[UPY], tab[DOWNY], tab[UPZ], tab[DOWNZ] = up_y, down_y, up_z, down_z
    below_1, above_6 = x_terms(1)[2], x_terms(cx - 2)[3]

    slot = (lane + half) // group % cx
    deep = (lane + half) % group - half
    is_hi = deep >= 0
    z_at = jnp.where(is_hi, deep + cz, deep)
    wzz, fzz, up_zz, down_zz, mzz = axis_terms(z_at, cz, low[2], high[2], gz, nz)
    ZD, ZAM, ZM, ZG, ZUX, ZDX, ZUZ, ZDZ = 0, 3, 6, 9, 12, 15, 18, 19
    for b in range(3):
        wx, fx, up_x, down_x, mx = axis_terms(slot + (b - 1) * cx, cx, low[0], high[0], gx, nx)
        ztab[ZD + b] = wx * wy * wzz
        ztab[ZAM + b] = mx * my * mzz * ALPHA
        ztab[ZM + b] = mx * my * mzz
        ztab[ZG + b] = GAMMA + DELTA * (fx + fy + fzz)
        ztab[ZUX + b] = up_x
        ztab[ZDX + b] = down_x
    ztab[ZUZ], ztab[ZDZ] = up_zz, down_zz
    first_lane, last_lane = lane == 0, lane == LANES - 1
    at_first, at_last = deep == 0, deep == -1
    first_slot, last_slot = slot == 0, slot == cx - 1

    def d_class(x):
        if x < 0:
            return D0 + (1 if x == -1 else 0)
        if x >= cx:
            return D0 + (5 if x == cx else 6)
        return D0 + (2 if x == 0 else 4 if x == cx - 1 else 3)

    def g_class(x):
        return G0 + {-2: 1, 1: 2, cx - 2: 3, cx + 1: 4}.get(x, 0)

    def roll_rows(v, shift):
        return pltpu.roll(v, shift % v.shape[0], 0)

    def roll_lanes(v, shift):
        shift = shift % LANES
        return v if shift == 0 else pltpu.roll(v, shift, 1)

    def rolled(v, shift, axis):
        flat = v.reshape(-1, LANES)
        return (roll_rows if axis == 0 else roll_lanes)(flat, shift).reshape(v.shape)

    def planes(reach):
        xs = list(range(-reach, cx + reach))
        return [xs[i:i + CHUNK] for i in range(0, len(xs), CHUNK)]

    def table(kind, xs):
        ks = [kind(x) for x in xs]
        if len(set(ks)) == 1:
            return tab[ks[0]][None]
        return jnp.stack([tab[k] for k in ks])

    def unpacked(z_src, xs):
        return jnp.stack([roll_lanes(z_src[(x + cx) // cx], -group * (x % cx)) for x in xs])

    def beside(src, z_src, xs, weighted):
        lo = xs[0] + cx
        mid = src[pl.ds(lo, len(xs))]
        if not weighted or not set(xs) & {1, cx - 2, -2, cx + 1}:
            along_x = src[pl.ds(lo - 1, len(xs))] + src[pl.ds(lo + 1, len(xs))]
        else:
            parts = []
            for x in xs:
                a, b = src[x + cx - 1], src[x + cx + 1]
                if x == 1:
                    a = a * below_1
                if x == cx + 1:
                    a = a * 0.5
                if x == cx - 2:
                    b = b * above_6
                if x == -2:
                    b = b * 0.5
                parts.append(a + b)
            along_x = jnp.stack(parts)
        extra = unpacked(z_src, xs)
        up = rolled(jnp.where(last_lane[None], extra, mid), 1, 1)
        down = rolled(jnp.where(first_lane[None], extra, mid), -1, 1)
        left, right = rolled(mid, 1, 0), rolled(mid, -1, 0)
        if weighted:
            up, down = up * tab[UPZ][None], down * tab[DOWNZ][None]
            left, right = left * tab[UPY][None], right * tab[DOWNY][None]
        return mid, (along_x + (left + right)) + (up + down)

    def z_beside(src, z_src, b, reach, weighted):
        mid = z_src[b]
        inject = jnp.zeros((rows, LANES), F32)
        for g in range(cx):
            x = g + (b - 1) * cx
            if -reach <= x < cx + reach:
                inject = jnp.where(slot_edge[g], roll_lanes(src[x + cx], group * g), inject)
        up = roll_lanes(jnp.where(at_last, inject, mid), 1)
        down = roll_lanes(jnp.where(at_first, inject, mid), -1)
        left, right = roll_rows(mid, 1), roll_rows(mid, -1)
        before, after = roll_lanes(mid, group), roll_lanes(mid, -group)
        if b > 0:
            before = jnp.where(first_slot, roll_lanes(z_src[b - 1], group), before)
        if b < 2:
            after = jnp.where(last_slot, roll_lanes(z_src[b + 1], -group), after)
        if weighted:
            up, down = up * ztab[ZUZ], down * ztab[ZDZ]
            left, right = left * tab[UPY], right * tab[DOWNY]
            before, after = before * ztab[ZUX + b], after * ztab[ZDX + b]
        return mid, ((before + after) + (left + right)) + (up + down)

    slot_edge = [(slot == g) & ((deep == 0) | (deep == -1)) for g in range(cx)]

    def apply_a(c, f, reach, index):
        src, z_src = main.at[c, f], pack.at[c, f]
        for xs in planes(reach):
            mid, around = beside(src, z_src, xs, False)
            value = 6.0 * mid - around
            for i, x in enumerate(xs):
                if 0 <= x < cx:
                    image[index, x] = value[i, cy:2 * cy]
            if reach > 0:
                cbuf[c, pl.ds(xs[0] + cx, len(xs))] = value * table(d_class, xs)
        if reach > 0:
            for b in range(3):
                mid, around = z_beside(src, z_src, b, reach, False)
                czbuf[c, b] = (6.0 * mid - around) * ztab[ZD + b]

    def scale_only(c, f, reach):
        for xs in planes(reach):
            ds = pl.ds(xs[0] + cx, len(xs))
            cbuf[c, ds] = main[c, f, ds] * table(d_class, xs)
        for b in range(3):
            czbuf[c, b] = pack[c, f, b] * ztab[ZD + b]

    def apply_m(c, f, reach):
        src, z_src = cbuf.at[c], czbuf.at[c]
        for xs in planes(reach + 1):
            mid, around = beside(src, z_src, xs, True)
            sbuf[c, pl.ds(xs[0] + cx, len(xs))] = BETA * mid + around * table(lambda x: AM0 + (x + cx) // cx, xs)
        for b in range(3):
            mid, around = z_beside(src, z_src, b, reach + 1, True)
            szbuf[c, b] = BETA * mid + around * ztab[ZAM + b]
        s_src, sz_src = sbuf.at[c], szbuf.at[c]
        for xs in planes(reach):
            ds = pl.ds(xs[0] + cx, len(xs))
            _, around = beside(s_src, sz_src, xs, True)
            value = src[ds] * table(g_class, xs)
            if reach > 0:
                main[c, f, ds] = value + around * table(lambda x: M0 + (x + cx) // cx, xs)
            else:
                main[c, f, ds, pl.ds(cy, cy)] = (value + around)[:, cy:2 * cy]
        if reach > 0:
            for b in range(3):
                _, around = z_beside(s_src, sz_src, b, reach, True)
                pack[c, f, b] = z_src[b] * ztab[ZG + b] + around * ztab[ZM + b]

    def copy_to(c, s, index):
        dx, dy, dz = OFFSETS[index]
        f = 2 * s
        if dz == 0:
            n = cx if dx == 0 else REACH[s][c] - (dy != 0)
            first = cx if dx <= 0 else 2 * cx - n
            there = pl.ds(first - cx * dx, n)
            source = main.at[c, f, pl.ds(first, n), pl.ds(cy, cy)]
            sink = main.at[c, f, there, pl.ds(cy - cy * dy, cy)]
        else:
            source = face.at[c, s]
            sink = got.at[c, s, 0 if dz > 0 else 1, 1 - dx, pl.ds(cy - cy * dy, cy)]
        return pltpu.make_async_remote_copy(
            source, sink, s_sem.at[c, s, index], r_sem.at[c, s, index],
            device_id=target(OFFSETS[index]), device_id_type=MESH)

    def pack_face(c, s):
        f = 2 * s
        value = jnp.zeros((cy, LANES), F32)
        for g in range(cx):
            moved = roll_lanes(main[c, f, cx + g, pl.ds(cy, cy)], group * g)
            value = jnp.where(slot[:cy] == g, moved, value)
        face[c, s] = value

    def send(c, s):
        order = sorted(range(len(OFFSETS)), key=lambda i: -sum(abs(v) for v in OFFSETS[i]))
        for index in order:
            @pl.when(exists(OFFSETS[index]))
            def _():
                copy_to(c, s, index).start()

    def receive(c, s):
        for index, offset in enumerate(OFFSETS):
            @pl.when(exists(flip(offset)))
            def _():
                copy_to(c, s, index).wait_recv()
        pack[c, 2 * s] = jnp.where(is_hi[None], got[c, s, 1], got[c, s, 0])

    def done_sending(c, s):
        for index, offset in enumerate(OFFSETS):
            @pl.when(exists(offset))
            def _():
                copy_to(c, s, index).wait_send()

    def own(c, f):
        return main[c, f, pl.ds(cx, cx), pl.ds(cy, cy)].reshape(cx * cy, LANES)

    outs = []

    def emit(c, f, slot_out):
        copy = pltpu.make_async_copy(
            main.at[c, f, pl.ds(cx, cx), pl.ds(cy, cy)], pow_ref.at[c, slot_out], out_sem.at[c, slot_out])
        copy.start()
        outs.append(copy)

    place_of = {a: (P_CHAIN, a) for a in range(STEPS + 1)}
    place_of.update({STEPS + 1 + k: (Z_CHAIN, k + 1) for k in range(STEPS)})
    ready = []

    def account(a):
        ready.append(a)
        picture = image[a].reshape(cx * cy, LANES)
        for b in ready:
            part = jnp.sum(own(*place_of[b]) * picture, axis=0, keepdims=True)
            t_ref[pl.ds(a * total + b, 1), :] = part
            if a != b:
                t_ref[pl.ds(b * total + a, 1), :] = part
        t_ref[pl.ds(total * total + a, 1), :] = jnp.sum(
            own(*place_of[a]) * own(Z_CHAIN, 0), axis=0, keepdims=True)

    t_ref[...] = jnp.zeros_like(t_ref)
    for copy in loads:
        copy.wait()
    for c in (Z_CHAIN, P_CHAIN):
        pack_face(c, 0)
    pl.semaphore_wait(barrier, expected)
    send(Z_CHAIN, 0)
    send(P_CHAIN, 0)

    first_z = STEPS + 1
    receive(Z_CHAIN, 0)
    scale_only(Z_CHAIN, 0, 5)
    apply_m(Z_CHAIN, 1, 3)
    emit(Z_CHAIN, 1, 0)
    apply_a(Z_CHAIN, 1, 2, first_z)
    apply_m(Z_CHAIN, 2, 0)
    pack_face(Z_CHAIN, 1)
    send(Z_CHAIN, 1)
    emit(Z_CHAIN, 2, 1)

    receive(P_CHAIN, 0)
    apply_a(P_CHAIN, 0, 5, 0)
    apply_m(P_CHAIN, 1, 3)
    emit(P_CHAIN, 1, 0)
    apply_a(P_CHAIN, 1, 2, 1)
    apply_m(P_CHAIN, 2, 0)
    pack_face(P_CHAIN, 1)
    send(P_CHAIN, 1)
    emit(P_CHAIN, 2, 1)
    for a in (0, 1, first_z):
        account(a)

    receive(Z_CHAIN, 1)
    apply_a(Z_CHAIN, 2, 6, first_z + 1)
    apply_m(Z_CHAIN, 3, 4)
    emit(Z_CHAIN, 3, 2)
    apply_a(Z_CHAIN, 3, 3, first_z + 2)
    apply_m(Z_CHAIN, 4, 1)
    emit(Z_CHAIN, 4, 3)
    apply_a(Z_CHAIN, 4, 0, first_z + 3)
    for a in (first_z + 1, first_z + 2, first_z + 3):
        account(a)

    receive(P_CHAIN, 1)
    apply_a(P_CHAIN, 2, 6, 2)
    account(2)
    apply_m(P_CHAIN, 3, 4)
    emit(P_CHAIN, 3, 2)
    apply_a(P_CHAIN, 3, 3, 3)
    account(3)
    apply_m(P_CHAIN, 4, 1)
    emit(P_CHAIN, 4, 3)
    apply_a(P_CHAIN, 4, 0, 4)
    account(4)

    value = lax.dot_general(
        jnp.ones((8, LANES), F32), t_ref[...], (((1,), (1,)), ((), ())),
        precision=HIGHEST, preferred_element_type=F32)[0:1]

    def gather(value, axes, buffer, send_sem, recv_sem):
        size, make = ahead(axes)
        buffer[0] = value

        def copy(k):
            return pltpu.make_async_remote_copy(
                buffer.at[0], buffer.at[k], send_sem.at[k], recv_sem.at[k],
                device_id=make(k), device_id_type=MESH)

        for k in range(1, size):
            copy(k).start()
        for k in range(1, size):
            copy(k).wait_recv()
        result = jnp.zeros_like(value)
        for k in range(size):
            rest, at = k, 0
            scale = 1
            for a in reversed(axes):
                n = counts[AXES.index(a)]
                rest, want = divmod(rest, n)
                at = at + scale * lax.rem(place[AXES.index(a)] + n - want, n)
                scale *= n
            result = result + buffer[at]
        for k in range(1, size):
            copy(k).wait_send()
        return result

    if near:
        value = gather(value, AXES, red0, s0_sem, r0_sem)
    else:
        value = gather(value, ("gy", "gz"), red0, s0_sem, r0_sem)
        value = gather(value, ("gx",), red1, s1_sem, r1_sem)
    value = value * (1.0 / (nx * cx * ny * cy * nz * cz))
    for a in range(total):
        gram_ref[a:a + 1, :] = value[0:1, a * total:(a + 1) * total]
    proj_ref[...] = value[0:1, total * total:total * total + total]
    for c in (0, 1):
        for s in (0, 1):
            done_sending(c, s)
    for copy in outs:
        copy.wait()


def solution(mesh):
    counts = tuple(mesh.shape[a] for a in AXES)
    near = max(counts) <= 4
    devices = counts[0] * counts[1] * counts[2]
    plane = devices if near else counts[1] * counts[2]

    def local(residual, direction):
        dims = residual.shape
        cx, cy, cz = dims
        assert cz == LANES and LANES % cx == 0 and cy % 8 == 0
        assert min(cx, cy, LANES // cx // 2) > max(max(r) for r in REACH)
        total = 2 * STEPS + 1
        fields = STEPS + 1
        dma = pltpu.SemaphoreType.DMA
        vm = pl.BlockSpec(memory_space=pltpu.VMEM)
        hbm = pl.BlockSpec(memory_space=pl.ANY)
        ext = (3 * cx, 3 * cy, LANES)
        zext = (3, 3 * cy, LANES)
        n = len(OFFSETS)
        powers, gram, proj = pl.pallas_call(
            functools.partial(kernel, counts, dims, near),
            out_shape=(
                jax.ShapeDtypeStruct((2, STEPS) + dims, F32),
                jax.ShapeDtypeStruct((total, total), F32),
                jax.ShapeDtypeStruct((1, total), F32),
            ),
            in_specs=[hbm, hbm],
            out_specs=(hbm, vm, vm),
            scratch_shapes=[
                pltpu.VMEM((2, fields) + ext, F32),
                pltpu.VMEM((2, fields) + zext, F32),
                pltpu.VMEM((2, 2, 2) + zext, F32),
                pltpu.VMEM((2, 2, cy, LANES), F32),
                pltpu.VMEM((2,) + ext, F32),
                pltpu.VMEM((2,) + zext, F32),
                pltpu.VMEM((2,) + ext, F32),
                pltpu.VMEM((2,) + zext, F32),
                pltpu.VMEM((total, cx, cy, LANES), F32),
                pltpu.VMEM((1, 8, LANES), F32),
                pltpu.VMEM((22, 3 * cy, LANES), F32),
                pltpu.VMEM((20, 3 * cy, LANES), F32),
                pltpu.VMEM((LANES, LANES), F32),
                pltpu.VMEM((plane, 1, LANES), F32),
                pltpu.VMEM((counts[0], 1, LANES), F32),
                dma((2,)), dma((2, STEPS)),
                dma((2, 2, n)), dma((2, 2, n)),
                dma((plane,)), dma((plane,)),
                dma((counts[0],)), dma((counts[0],)),
            ],
            compiler_params=pltpu.CompilerParams(collective_id=0, has_side_effects=True),
            name="powers_basis",
        )(residual, direction)
        return powers, gram, proj.reshape(total)

    placed = (P("gx", "gy", "gz"), P("gx", "gy", "gz"))
    return jax.shard_map(
        local,
        mesh=mesh,
        in_specs=placed,
        out_specs=(P(None, None, "gx", "gy", "gz"), P(), P()),
        check_vma=False,
    )
```

```python
import functools

import jax
import jax.numpy as jnp
from jax import lax
from jax.experimental import pallas as pl
from jax.experimental.pallas import tpu as pltpu
from jax.sharding import PartitionSpec as P

STEPS = 4
LANES = 128
MESH = pl.DeviceIdType.MESH
HIGHEST = lax.Precision.HIGHEST
F32 = jnp.float32
AXES = ("gx", "gy", "gz")
GAMMA, BETA, ALPHA, DELTA = 13.0 / 81.0, 5.0 / 243.0, 1.0 / 729.0, 1.0 / 1458.0
P_CHAIN, Z_CHAIN = 0, 1
REACH = ((6, 5), (7, 7))
CHUNK = 4
OFFSETS = [(dx, dy, dz) for dx in (-1, 0, 1) for dy in (-1, 0, 1) for dz in (-1, 0, 1) if (dx, dy, dz) != (0, 0, 0)]


def as_f32(flag):
    return jnp.where(flag, 1.0, 0.0).astype(F32)


def axis_terms(at, width, low, high, place, count):
    inside = (place * width + at >= 0) & (place * width + at < count * width)
    cover = ((at == -1) | (at == 0)) & low | ((at == width - 1) | (at == width)) & high
    inner = ((at == -2) | (at == 1)) & low | ((at == width - 2) | (at == width + 1)) & high
    below = (at == 1) & low | (at == width + 1) & high
    above = (at == -2) & low | (at == width - 2) & high
    mask = as_f32(inside)
    return (1.0 + as_f32(cover)) * mask, as_f32(inner), 1.0 - 0.5 * as_f32(below), 1.0 - 0.5 * as_f32(above), mask


def kernel(
    counts, dims, near, res_ref, dir_ref, pow_ref, gram_ref, proj_ref,
    main, pack, got, face, cbuf, czbuf, sbuf, szbuf, image, zsum, ubuf, tab, ztab, t_ref, red0, red1, spare,
    in_sem, out_sem, s_sem, r_sem, s0_sem, r0_sem, s1_sem, r1_sem,
):
    nx, ny, nz = counts
    cx, cy, cz = dims
    group = LANES // cx
    half = group // 2
    rows = 3 * cy
    place = [lax.axis_index(a) for a in AXES]
    gx, gy, gz = place
    low = [place[i] > 0 for i in range(3)]
    high = [place[i] < counts[i] - 1 for i in range(3)]
    total = 2 * STEPS + 1

    def exists(offset):
        ok = None
        for i, step in enumerate(offset):
            if step:
                test = low[i] if step < 0 else high[i]
                ok = test if ok is None else jnp.logical_and(ok, test)
        return ok

    def flip(offset):
        return tuple(-s for s in offset)

    def target(offset):
        return {AXES[i]: place[i] + s for i, s in enumerate(offset) if s}

    def ahead(axes):
        def make(k):
            out = {}
            for a in reversed(axes):
                k, step = divmod(k, counts[AXES.index(a)])
                if step:
                    out[a] = lax.rem(place[AXES.index(a)] + step, counts[AXES.index(a)])
            return out
        size = 1
        for a in axes:
            size *= counts[AXES.index(a)]
        return size, make

    loads = [
        pltpu.make_async_copy(ref, main.at[c, 0, pl.ds(cx, cx), pl.ds(cy, cy)], in_sem.at[c])
        for c, ref in ((Z_CHAIN, res_ref), (P_CHAIN, dir_ref))
    ]
    for copy in loads:
        copy.start()

    barrier = pltpu.get_barrier_semaphore()
    expected = 0
    for offset in OFFSETS:
        @pl.when(exists(offset))
        def _():
            pl.semaphore_signal(barrier, 1, device_id=target(offset), device_id_type=MESH)
        expected = expected + exists(offset).astype(jnp.int32)
    if not near:
        for axes in (("gy", "gz"), ("gx",)):
            size, make = ahead(axes)
            for k in range(1, size):
                pl.semaphore_signal(barrier, 1, device_id=make(k), device_id_type=MESH)
            expected = expected + (size - 1)

    fields = [(c, f) for c in (0, 1) for f in (0, 2)]
    for flag, xs, ys in (
        (low[0], pl.ds(0, cx), pl.ds(0, rows)), (high[0], pl.ds(2 * cx, cx), pl.ds(0, rows)),
        (low[1], pl.ds(0, 3 * cx), pl.ds(0, cy)), (high[1], pl.ds(0, 3 * cx), pl.ds(2 * cy, cy)),
    ):
        @pl.when(jnp.logical_not(flag))
        def _():
            for c, f in fields:
                main[c, f, xs, ys] = jnp.zeros((xs.size, ys.size, LANES), F32)
    for flag, ss, xs, ys in (
        (low[2], 0, pl.ds(0, 3), pl.ds(0, rows)), (high[2], 1, pl.ds(0, 3), pl.ds(0, rows)),
        (low[0], None, pl.ds(0, 1), pl.ds(0, rows)), (high[0], None, pl.ds(2, 1), pl.ds(0, rows)),
        (low[1], None, pl.ds(0, 3), pl.ds(0, cy)), (high[1], None, pl.ds(0, 3), pl.ds(2 * cy, cy)),
    ):
        @pl.when(jnp.logical_not(flag))
        def _():
            for c in (0, 1):
                for s in (0, 1):
                    for side in ((0, 1) if ss is None else (ss,)):
                        got[c, s, side, xs, ys] = jnp.zeros((xs.size, ys.size, LANES), F32)

    lane = lax.broadcasted_iota(jnp.int32, (rows, LANES), 1)
    row = lax.broadcasted_iota(jnp.int32, (rows, LANES), 0)
    wy, fy, up_y, down_y, my = axis_terms(row - cy, cy, low[1], high[1], gy, ny)
    wz, fz, up_z, down_z, mz = axis_terms(lane, cz, low[2], high[2], gz, nz)

    def x_terms(x):
        return axis_terms(jnp.int32(x), cx, low[0], high[0], gx, nx)

    D_REPS = (-3, -1, 0, 3, cx - 1, cx, cx + 2)
    D0, AM0, M0, G0, UPY, DOWNY, UPZ, DOWNZ = 0, 7, 10, 13, 18, 19, 20, 21
    wyz, myz, fyz = wy * wz, my * mz, fy + fz
    for k, x in enumerate(D_REPS):
        tab[D0 + k] = wyz * x_terms(x)[0]
    for k, x in enumerate((-3, 3, cx + 2)):
        mask = myz * x_terms(x)[4]
        tab[AM0 + k] = mask * ALPHA
        tab[M0 + k] = mask
    for k, x in enumerate((3, -2, 1, cx - 2, cx + 1)):
        tab[G0 + k] = GAMMA + DELTA * (fyz + x_terms(x)[1])
    tab[UPY], tab[DOWNY], tab[UPZ], tab[DOWNZ] = up_y, down_y, up_z, down_z
    below_1, above_6 = x_terms(1)[2], x_terms(cx - 2)[3]

    slot = (lane + half) // group % cx
    deep = (lane + half) % group - half
    is_hi = deep >= 0
    z_at = jnp.where(is_hi, deep + cz, deep)
    wzz, fzz, up_zz, down_zz, mzz = axis_terms(z_at, cz, low[2], high[2], gz, nz)
    ZD, ZAM, ZM, ZG, ZUX, ZDX, ZUZ, ZDZ = 0, 3, 6, 9, 12, 15, 18, 19
    for b in range(3):
        wx, fx, up_x, down_x, mx = axis_terms(slot + (b - 1) * cx, cx, low[0], high[0], gx, nx)
        ztab[ZD + b] = wx * wy * wzz
        ztab[ZAM + b] = mx * my * mzz * ALPHA
        ztab[ZM + b] = mx * my * mzz
        ztab[ZG + b] = GAMMA + DELTA * (fx + fy + fzz)
        ztab[ZUX + b] = up_x
        ztab[ZDX + b] = down_x
    ztab[ZUZ], ztab[ZDZ] = up_zz, down_zz
    first_lane, last_lane = lane == 0, lane == LANES - 1
    at_first, at_last = deep == 0, deep == -1
    first_slot, last_slot = slot == 0, slot == cx - 1

    def d_class(x):
        if x < 0:
            return D0 + (1 if x == -1 else 0)
        if x >= cx:
            return D0 + (5 if x == cx else 6)
        return D0 + (2 if x == 0 else 4 if x == cx - 1 else 3)

    def g_class(x):
        return G0 + {-2: 1, 1: 2, cx - 2: 3, cx + 1: 4}.get(x, 0)

    def roll_rows(v, shift):
        return pltpu.roll(v, shift % v.shape[0], 0)

    def roll_lanes(v, shift):
        shift = shift % LANES
        return v if shift == 0 else pltpu.roll(v, shift, 1)

    def rolled(v, shift, axis):
        flat = v.reshape(-1, LANES)
        return (roll_rows if axis == 0 else roll_lanes)(flat, shift).reshape(v.shape)

    def planes(reach):
        xs = list(range(-reach, cx + reach))
        return [xs[i:i + CHUNK] for i in range(0, len(xs), CHUNK)]

    def table(kind, xs):
        ks = [kind(x) for x in xs]
        if len(set(ks)) == 1:
            return tab[ks[0]][None]
        return jnp.stack([tab[k] for k in ks])

    def unpacked(z_src, xs):
        return jnp.stack([roll_lanes(z_src[(x + cx) // cx], -group * (x % cx)) for x in xs])

    def beside(src, z_src, xs, weighted):
        lo = xs[0] + cx
        mid = src[pl.ds(lo, len(xs))]
        if not weighted or not set(xs) & {1, cx - 2, -2, cx + 1}:
            along_x = src[pl.ds(lo - 1, len(xs))] + src[pl.ds(lo + 1, len(xs))]
        else:
            parts = []
            for x in xs:
                a, b = src[x + cx - 1], src[x + cx + 1]
                if x == 1:
                    a = a * below_1
                if x == cx + 1:
                    a = a * 0.5
                if x == cx - 2:
                    b = b * above_6
                if x == -2:
                    b = b * 0.5
                parts.append(a + b)
            along_x = jnp.stack(parts)
        left, right = rolled(mid, 1, 0), rolled(mid, -1, 0)
        if weighted:
            left, right = left * tab[UPY][None], right * tab[DOWNY][None]
        return mid, (along_x + (left + right)) + zsum[pl.ds(lo, len(xs))]

    def sweep_z(src, z_src, reach, weighted):
        xs = list(range(-reach, cx + reach))
        for x in xs:
            ubuf[x + cx] = roll_lanes(z_src[(x + cx) // cx], -group * (x % cx))
        for x in xs:
            extra, mid = ubuf[x + cx], src[x + cx]
            up = roll_lanes(jnp.where(last_lane, extra, mid), 1)
            down = roll_lanes(jnp.where(first_lane, extra, mid), -1)
            if weighted:
                up, down = up * tab[UPZ], down * tab[DOWNZ]
            zsum[x + cx] = up + down

    def z_beside(src, z_src, b, reach, weighted):
        mid = z_src[b]
        inject = jnp.zeros((rows, LANES), F32)
        for g in range(cx):
            x = g + (b - 1) * cx
            if -reach <= x < cx + reach:
                inject = jnp.where(slot_edge[g], roll_lanes(src[x + cx], group * g), inject)
        up = roll_lanes(jnp.where(at_last, inject, mid), 1)
        down = roll_lanes(jnp.where(at_first, inject, mid), -1)
        left, right = roll_rows(mid, 1), roll_rows(mid, -1)
        before, after = roll_lanes(mid, group), roll_lanes(mid, -group)
        if b > 0:
            before = jnp.where(first_slot, roll_lanes(z_src[b - 1], group), before)
        if b < 2:
            after = jnp.where(last_slot, roll_lanes(z_src[b + 1], -group), after)
        if weighted:
            up, down = up * ztab[ZUZ], down * ztab[ZDZ]
            left, right = left * tab[UPY], right * tab[DOWNY]
            before, after = before * ztab[ZUX + b], after * ztab[ZDX + b]
        return mid, ((before + after) + (left + right)) + (up + down)

    slot_edge = [(slot == g) & ((deep == 0) | (deep == -1)) for g in range(cx)]

    def apply_a(c, f, reach, index):
        src, z_src = main.at[c, f], pack.at[c, f]
        sweep_z(src, z_src, reach, False)
        for xs in planes(reach):
            mid, around = beside(src, z_src, xs, False)
            value = 6.0 * mid - around
            for i, x in enumerate(xs):
                if 0 <= x < cx:
                    image[index, x] = value[i, cy:2 * cy]
            if reach > 0:
                cbuf[c, pl.ds(xs[0] + cx, len(xs))] = value * table(d_class, xs)
        if reach > 0:
            for b in range(3):
                mid, around = z_beside(src, z_src, b, reach, False)
                czbuf[c, b] = (6.0 * mid - around) * ztab[ZD + b]

    def scale_only(c, f, reach):
        for xs in planes(reach):
            ds = pl.ds(xs[0] + cx, len(xs))
            cbuf[c, ds] = main[c, f, ds] * table(d_class, xs)
        for b in range(3):
            czbuf[c, b] = pack[c, f, b] * ztab[ZD + b]

    def apply_m(c, f, reach):
        src, z_src = cbuf.at[c], czbuf.at[c]
        sweep_z(src, z_src, reach + 1, True)
        for xs in planes(reach + 1):
            mid, around = beside(src, z_src, xs, True)
            sbuf[c, pl.ds(xs[0] + cx, len(xs))] = BETA * mid + around * table(lambda x: AM0 + (x + cx) // cx, xs)
        for b in range(3):
            mid, around = z_beside(src, z_src, b, reach + 1, True)
            szbuf[c, b] = BETA * mid + around * ztab[ZAM + b]
        s_src, sz_src = sbuf.at[c], szbuf.at[c]
        sweep_z(s_src, sz_src, reach, True)
        for xs in planes(reach):
            ds = pl.ds(xs[0] + cx, len(xs))
            _, around = beside(s_src, sz_src, xs, True)
            value = src[ds] * table(g_class, xs)
            if reach > 0:
                main[c, f, ds] = value + around * table(lambda x: M0 + (x + cx) // cx, xs)
            else:
                main[c, f, ds, pl.ds(cy, cy)] = (value + around)[:, cy:2 * cy]
        if reach > 0:
            for b in range(3):
                _, around = z_beside(s_src, sz_src, b, reach, True)
                pack[c, f, b] = z_src[b] * ztab[ZG + b] + around * ztab[ZM + b]

    def copy_to(c, s, index):
        dx, dy, dz = OFFSETS[index]
        f = 2 * s
        if dz == 0:
            n = cx if dx == 0 else REACH[s][c] - (dy != 0)
            first = cx if dx <= 0 else 2 * cx - n
            there = pl.ds(first - cx * dx, n)
            source = main.at[c, f, pl.ds(first, n), pl.ds(cy, cy)]
            sink = main.at[c, f, there, pl.ds(cy - cy * dy, cy)]
        else:
            source = face.at[c, s]
            sink = got.at[c, s, 0 if dz > 0 else 1, 1 - dx, pl.ds(cy - cy * dy, cy)]
        return pltpu.make_async_remote_copy(
            source, sink, s_sem.at[0], r_sem.at[c, s],
            device_id=target(OFFSETS[index]), device_id_type=MESH)

    def pack_face(c, s):
        f = 2 * s
        value = jnp.zeros((cy, LANES), F32)
        for g in range(cx):
            moved = roll_lanes(main[c, f, cx + g, pl.ds(cy, cy)], group * g)
            value = jnp.where(slot[:cy] == g, moved, value)
        face[c, s] = value

    def send(c, s):
        order = sorted(range(len(OFFSETS)), key=lambda i: -sum(abs(v) for v in OFFSETS[i]))
        for index in order:
            @pl.when(exists(OFFSETS[index]))
            def _():
                copy_to(c, s, index).start()

    around_it = [low[i].astype(jnp.int32) + high[i].astype(jnp.int32) for i in range(3)]
    choices = [{1: (0,), 2: (1,)}.get(n, (1, 2)) for n in counts]

    def tiles_of(c, s, ax, ay, az):
        planes_in = ax * REACH[s][c] + ay * cx + ax * ay * (REACH[s][c] - 1)
        return (planes_in + az * (1 + ax) * (1 + ay)) * (cy // 8)

    def wait_bytes(sem, tiles):
        view = spare.at[pl.ds(0, tiles)]
        pltpu.make_async_copy(view, view, sem).wait()

    def wait_exchanges(sem, pairs):
        for ax in choices[0]:
            for ay in choices[1]:
                for az in choices[2]:
                    here = (around_it[0] == ax) & (around_it[1] == ay) & (around_it[2] == az)
                    tiles = sum(tiles_of(c, s, ax, ay, az) for c, s in pairs)
                    if tiles:
                        @pl.when(here)
                        def _():
                            wait_bytes(sem, tiles)

    def receive(c, s):
        wait_exchanges(r_sem.at[c, s], [(c, s)])
        pack[c, 2 * s] = jnp.where(is_hi[None], got[c, s, 1], got[c, s, 0])

    def own(c, f):
        return main[c, f, pl.ds(cx, cx), pl.ds(cy, cy)].reshape(cx * cy, LANES)

    def emit(c, f, slot_out):
        copy = pltpu.make_async_copy(
            main.at[c, f, pl.ds(cx, cx), pl.ds(cy, cy)], pow_ref.at[c, slot_out], out_sem.at[0])
        copy.start()

    place_of = {a: (P_CHAIN, a) for a in range(STEPS + 1)}
    place_of.update({STEPS + 1 + k: (Z_CHAIN, k + 1) for k in range(STEPS)})
    ready = []

    def account(a):
        ready.append(a)
        picture = image[a].reshape(cx * cy, LANES)
        for b in ready:
            part = jnp.sum(own(*place_of[b]) * picture, axis=0, keepdims=True)
            t_ref[pl.ds(a * total + b, 1), :] = part
            if a != b:
                t_ref[pl.ds(b * total + a, 1), :] = part
        t_ref[pl.ds(total * total + a, 1), :] = jnp.sum(
            own(*place_of[a]) * own(Z_CHAIN, 0), axis=0, keepdims=True)

    t_ref[...] = jnp.zeros_like(t_ref)
    for copy in loads:
        copy.wait()
    for c in (Z_CHAIN, P_CHAIN):
        pack_face(c, 0)
    pl.semaphore_wait(barrier, expected)
    send(Z_CHAIN, 0)
    send(P_CHAIN, 0)

    first_z = STEPS + 1
    receive(Z_CHAIN, 0)
    scale_only(Z_CHAIN, 0, 5)
    apply_m(Z_CHAIN, 1, 3)
    emit(Z_CHAIN, 1, 0)
    apply_a(Z_CHAIN, 1, 2, first_z)
    apply_m(Z_CHAIN, 2, 0)
    pack_face(Z_CHAIN, 1)
    send(Z_CHAIN, 1)
    emit(Z_CHAIN, 2, 1)

    receive(P_CHAIN, 0)
    apply_a(P_CHAIN, 0, 5, 0)
    apply_m(P_CHAIN, 1, 3)
    emit(P_CHAIN, 1, 0)
    apply_a(P_CHAIN, 1, 2, 1)
    apply_m(P_CHAIN, 2, 0)
    pack_face(P_CHAIN, 1)
    send(P_CHAIN, 1)
    emit(P_CHAIN, 2, 1)
    for a in (0, 1, first_z):
        account(a)

    receive(Z_CHAIN, 1)
    apply_a(Z_CHAIN, 2, 6, first_z + 1)
    apply_m(Z_CHAIN, 3, 4)
    emit(Z_CHAIN, 3, 2)
    apply_a(Z_CHAIN, 3, 3, first_z + 2)
    apply_m(Z_CHAIN, 4, 1)
    emit(Z_CHAIN, 4, 3)
    apply_a(Z_CHAIN, 4, 0, first_z + 3)
    for a in (first_z + 1, first_z + 2, first_z + 3):
        account(a)

    receive(P_CHAIN, 1)
    apply_a(P_CHAIN, 2, 6, 2)
    account(2)
    apply_m(P_CHAIN, 3, 4)
    emit(P_CHAIN, 3, 2)
    apply_a(P_CHAIN, 3, 3, 3)
    account(3)
    apply_m(P_CHAIN, 4, 1)
    emit(P_CHAIN, 4, 3)
    apply_a(P_CHAIN, 4, 0, 4)
    account(4)

    value = lax.dot_general(
        jnp.ones((8, LANES), F32), t_ref[...], (((1,), (1,)), ((), ())),
        precision=HIGHEST, preferred_element_type=F32)[0:1]

    def gather(value, axes, buffer, send_sem, recv_sem, meanwhile=lambda: None):
        size, make = ahead(axes)
        buffer[0] = value

        def copy(k):
            return pltpu.make_async_remote_copy(
                buffer.at[0], buffer.at[k], send_sem.at[0], recv_sem.at[0],
                device_id=make(k), device_id_type=MESH)

        for k in range(1, size):
            copy(k).start()
        meanwhile()
        rest = buffer.at[pl.ds(1, size - 1)]
        pltpu.make_async_copy(rest, rest, send_sem.at[0]).wait()
        pltpu.make_async_copy(rest, rest, recv_sem.at[0]).wait()
        result = jnp.zeros_like(value)
        for k in range(size):
            rest, at = k, 0
            scale = 1
            for a in reversed(axes):
                n = counts[AXES.index(a)]
                rest, want = divmod(rest, n)
                at = at + scale * lax.rem(place[AXES.index(a)] + n - want, n)
                scale *= n
            result = result + buffer[at]
        return result

    def finish():
        wait_exchanges(s_sem.at[0], [(c, s) for c in (0, 1) for s in (0, 1)])
        wait_bytes(out_sem.at[0], 2 * STEPS * cx * (cy // 8))

    if near:
        value = gather(value, AXES, red0, s0_sem, r0_sem, finish)
    else:
        value = gather(value, ("gy", "gz"), red0, s0_sem, r0_sem, finish)
        value = gather(value, ("gx",), red1, s1_sem, r1_sem)
    value = value * (1.0 / (nx * cx * ny * cy * nz * cz))
    for a in range(total):
        gram_ref[a:a + 1, :] = value[0:1, a * total:(a + 1) * total]
    proj_ref[...] = value[0:1, total * total:total * total + total]


def solution(mesh):
    counts = tuple(mesh.shape[a] for a in AXES)
    near = max(counts) <= 4
    devices = counts[0] * counts[1] * counts[2]
    plane = devices if near else counts[1] * counts[2]

    def local(residual, direction):
        dims = residual.shape
        cx, cy, cz = dims
        assert cz == LANES and LANES % cx == 0 and cy % 8 == 0
        assert min(cx, cy, LANES // cx // 2) > max(max(r) for r in REACH)
        total = 2 * STEPS + 1
        fields = STEPS + 1
        dma = pltpu.SemaphoreType.DMA
        vm = pl.BlockSpec(memory_space=pltpu.VMEM)
        hbm = pl.BlockSpec(memory_space=pl.ANY)
        ext = (3 * cx, 3 * cy, LANES)
        zext = (3, 3 * cy, LANES)
        powers, gram, proj = pl.pallas_call(
            functools.partial(kernel, counts, dims, near),
            out_shape=(
                jax.ShapeDtypeStruct((2, STEPS) + dims, F32),
                jax.ShapeDtypeStruct((total, total), F32),
                jax.ShapeDtypeStruct((1, total), F32),
            ),
            in_specs=[hbm, hbm],
            out_specs=(hbm, vm, vm),
            scratch_shapes=[
                pltpu.VMEM((2, fields) + ext, F32),
                pltpu.VMEM((2, fields) + zext, F32),
                pltpu.VMEM((2, 2, 2) + zext, F32),
                pltpu.VMEM((2, 2, cy, LANES), F32),
                pltpu.VMEM((2,) + ext, F32),
                pltpu.VMEM((2,) + zext, F32),
                pltpu.VMEM((2,) + ext, F32),
                pltpu.VMEM((2,) + zext, F32),
                pltpu.VMEM((total, cx, cy, LANES), F32),
                pltpu.VMEM(ext, F32),
                pltpu.VMEM(ext, F32),
                pltpu.VMEM((22, 3 * cy, LANES), F32),
                pltpu.VMEM((20, 3 * cy, LANES), F32),
                pltpu.VMEM((LANES, LANES), F32),
                pltpu.VMEM((plane, 1, LANES), F32),
                pltpu.VMEM((counts[0], 1, LANES), F32),
                pltpu.VMEM((4 * 9 * cx * (cy // 8), 8, LANES), F32),
                dma((2,)), dma((1,)),
                dma((1,)), dma((2, 2)),
                dma((1,)), dma((1,)),
                dma((1,)), dma((1,)),
            ],
            compiler_params=pltpu.CompilerParams(collective_id=0, has_side_effects=True),
            name="powers_basis",
        )(residual, direction)
        return powers, gram, proj.reshape(total)

    placed = (P("gx", "gy", "gz"), P("gx", "gy", "gz"))
    return jax.shard_map(
        local,
        mesh=mesh,
        in_specs=placed,
        out_specs=(P(None, None, "gx", "gy", "gz"), P(), P()),
        check_vma=False,
    )
```

```python
import functools

import jax
import jax.numpy as jnp
from jax import lax
from jax.experimental import pallas as pl
from jax.experimental.pallas import tpu as pltpu
from jax.sharding import PartitionSpec as P

STEPS = 4
LANES = 128
MESH = pl.DeviceIdType.MESH
HIGHEST = lax.Precision.HIGHEST
F32 = jnp.float32
AXES = ("gx", "gy", "gz")
GAMMA, BETA, ALPHA, DELTA = 13.0 / 81.0, 5.0 / 243.0, 1.0 / 729.0, 1.0 / 1458.0
P_CHAIN, Z_CHAIN = 0, 1
REACH = ((6, 5), (7, 7))
CHUNK = 4
RUN = 4
OFFSETS = [(dx, dy, dz) for dx in (-1, 0, 1) for dy in (-1, 0, 1) for dz in (-1, 0, 1) if (dx, dy, dz) != (0, 0, 0)]


def as_f32(flag):
    return jnp.where(flag, 1.0, 0.0).astype(F32)


def axis_terms(at, width, low, high, place, count):
    inside = (place * width + at >= 0) & (place * width + at < count * width)
    cover = ((at == -1) | (at == 0)) & low | ((at == width - 1) | (at == width)) & high
    inner = ((at == -2) | (at == 1)) & low | ((at == width - 2) | (at == width + 1)) & high
    below = (at == 1) & low | (at == width + 1) & high
    above = (at == -2) & low | (at == width - 2) & high
    mask = as_f32(inside)
    return (1.0 + as_f32(cover)) * mask, as_f32(inner), 1.0 - 0.5 * as_f32(below), 1.0 - 0.5 * as_f32(above), mask


def kernel(
    counts, dims, near, res_ref, dir_ref, pow_ref, gram_ref, proj_ref,
    raw, main, pack, got, face, flat, cbuf, czbuf, sbuf, szbuf, image, zsum, zzsum, tab, ztab, up_tab, down_tab, d_tab, g_tab, t_ref, red0, red1, spare,
    in_sem, out_sem, s_sem, r_sem, s0_sem, r0_sem, s1_sem, r1_sem,
):
    nx, ny, nz = counts
    cx, cy, cz = dims
    group = LANES // cx
    half = group // 2
    rows = 3 * cy
    place = [lax.axis_index(a) for a in AXES]
    gx, gy, gz = place
    low = [place[i] > 0 for i in range(3)]
    high = [place[i] < counts[i] - 1 for i in range(3)]
    total = 2 * STEPS + 1

    def exists(offset):
        ok = None
        for i, step in enumerate(offset):
            if step:
                test = low[i] if step < 0 else high[i]
                ok = test if ok is None else jnp.logical_and(ok, test)
        return ok

    def flip(offset):
        return tuple(-s for s in offset)

    def target(offset):
        return {AXES[i]: place[i] + s for i, s in enumerate(offset) if s}

    def ahead(axes):
        def make(k):
            out = {}
            for a in reversed(axes):
                k, step = divmod(k, counts[AXES.index(a)])
                if step:
                    out[a] = lax.rem(place[AXES.index(a)] + step, counts[AXES.index(a)])
            return out
        size = 1
        for a in axes:
            size *= counts[AXES.index(a)]
        return size, make

    loads = [
        pltpu.make_async_copy(ref, raw.at[c, 0, pl.ds(cx, cx), pl.ds(cy, cy)], in_sem.at[c])
        for c, ref in ((Z_CHAIN, res_ref), (P_CHAIN, dir_ref))
    ]
    for copy in loads:
        copy.start()

    barrier = pltpu.get_barrier_semaphore()
    expected = 0
    for offset in OFFSETS:
        @pl.when(exists(offset))
        def _():
            pl.semaphore_signal(barrier, 1, device_id=target(offset), device_id_type=MESH)
        expected = expected + exists(offset).astype(jnp.int32)
    if not near:
        for axes in (("gy", "gz"), ("gx",)):
            size, make = ahead(axes)
            for k in range(1, size):
                pl.semaphore_signal(barrier, 1, device_id=make(k), device_id_type=MESH)
            expected = expected + (size - 1)

    fields = [(c, f) for c in (0, 1) for f in (0, 1)]
    for flag, xs, ys in (
        (low[0], pl.ds(0, cx), pl.ds(0, rows)), (high[0], pl.ds(2 * cx, cx), pl.ds(0, rows)),
        (low[1], pl.ds(0, 3 * cx), pl.ds(0, cy)), (high[1], pl.ds(0, 3 * cx), pl.ds(2 * cy, cy)),
    ):
        @pl.when(jnp.logical_not(flag))
        def _():
            for c, f in fields:
                raw[c, f, xs, ys] = jnp.zeros((xs.size, ys.size, LANES), F32)
    for flag, ss, xs, ys in (
        (low[2], 0, pl.ds(0, 3), pl.ds(0, rows)), (high[2], 1, pl.ds(0, 3), pl.ds(0, rows)),
        (low[0], None, pl.ds(0, 1), pl.ds(0, rows)), (high[0], None, pl.ds(2, 1), pl.ds(0, rows)),
        (low[1], None, pl.ds(0, 3), pl.ds(0, cy)), (high[1], None, pl.ds(0, 3), pl.ds(2 * cy, cy)),
    ):
        @pl.when(jnp.logical_not(flag))
        def _():
            for c in (0, 1):
                for s in (0, 1):
                    for side in ((0, 1) if ss is None else (ss,)):
                        got[c, s, side, xs, ys] = jnp.zeros((xs.size, ys.size, LANES), F32)

    lane = lax.broadcasted_iota(jnp.int32, (rows, LANES), 1)
    row = lax.broadcasted_iota(jnp.int32, (rows, LANES), 0)
    wy, fy, up_y, down_y, my = axis_terms(row - cy, cy, low[1], high[1], gy, ny)
    wz, fz, up_z, down_z, mz = axis_terms(lane, cz, low[2], high[2], gz, nz)

    def x_terms(x):
        return axis_terms(jnp.int32(x), cx, low[0], high[0], gx, nx)

    AM0, M0, UPY, DOWNY = 0, 3, 6, 7
    wyz, myz, gyz = wy * wz, my * mz, GAMMA + DELTA * (fy + fz)
    for k, x in enumerate((-3, 3, cx + 2)):
        mask = myz * x_terms(x)[4]
        tab[AM0 + k] = mask * ALPHA
        tab[M0 + k] = mask
    tab[UPY], tab[DOWNY] = up_y, down_y
    runs = 3 * cx // RUN

    def turn(x):
        return group * ((x + cx) // RUN)

    for g in range(runs):
        up_tab[g] = pltpu.roll(up_z[:cy], group * g, 1) if g else up_z[:cy]
        down_tab[g] = pltpu.roll(down_z[:cy], group * g, 1) if g else down_z[:cy]
        d_run = pltpu.roll(wyz, group * g, 1) if g else wyz
        g_run = pltpu.roll(gyz, group * g, 1) if g else gyz
        for k in range(RUN * g, RUN * g + RUN):
            cover, inner = x_terms(k - cx)[:2]
            d_tab[k] = d_run * cover
            g_tab[k] = g_run + DELTA * inner
    below_1, above_6 = x_terms(1)[2], x_terms(cx - 2)[3]

    slot = (lane + half) // group % cx
    deep = (lane + half) % group - half
    is_hi = deep >= 0
    z_at = jnp.where(is_hi, deep + cz, deep)
    wzz, fzz, up_zz, down_zz, mzz = axis_terms(z_at, cz, low[2], high[2], gz, nz)
    ZD, ZAM, ZM, ZG, ZUX, ZDX = (RUN * k for k in range(6))
    ZUZ, ZDZ = 6 * RUN, 6 * RUN + 1
    for b in range(RUN):
        wx, fx, up_x, down_x, mx = axis_terms(slot * RUN + (b - cx), cx, low[0], high[0], gx, nx)
        ztab[ZD + b] = wx * wy * wzz
        ztab[ZAM + b] = mx * my * mzz * ALPHA
        ztab[ZM + b] = mx * my * mzz
        ztab[ZG + b] = GAMMA + DELTA * (fx + fy + fzz)
        ztab[ZUX + b] = up_x
        ztab[ZDX + b] = down_x
    ztab[ZUZ], ztab[ZDZ] = up_zz, down_zz
    at_first, at_last = deep == 0, deep == -1
    is_first = [lane == group * g for g in range(runs)]
    is_last = [lane == (group * g - 1) % LANES for g in range(runs)]
    is_edge = [is_first[g] | is_last[g] for g in range(runs)]

    def roll_rows(v, shift):
        return pltpu.roll(v, shift % v.shape[0], 0)

    def roll_lanes(v, shift):
        shift = shift % LANES
        return v if shift == 0 else pltpu.roll(v, shift, 1)

    def rolled(v, shift, axis):
        flat = v.reshape(-1, LANES)
        return (roll_rows if axis == 0 else roll_lanes)(flat, shift).reshape(v.shape)

    def planes(reach):
        xs = list(range(-reach, cx + reach))
        return [xs[i:i + CHUNK] for i in range(0, len(xs), CHUNK)]

    def table(at, xs):
        ks = [at + (x + cx) // cx for x in xs]
        if len(set(ks)) == 1:
            return tab[ks[0]][None]
        return jnp.stack([tab[k] for k in ks])

    def thrice(v):
        return jnp.concatenate([v] * 3, axis=0)

    flips = [0]

    def stream(src, z_src, reach, weighted):
        flips[0] ^= 1
        out, z_out = zsum.at[flips[0]], zzsum.at[flips[0]]
        for b in range(RUN):
            mid = z_src[b]
            inject = jnp.zeros((rows, LANES), F32)
            for g in range(runs):
                x = g * RUN + b - cx
                if -reach <= x < cx + reach:
                    inject = jnp.where(is_edge[g], src[x + cx], inject)
            up = roll_lanes(jnp.where(at_last, inject, mid), 1)
            down = roll_lanes(jnp.where(at_first, inject, mid), -1)
            if weighted:
                up, down = up * ztab[ZUZ], down * ztab[ZDZ]
            part = up + down
            if b == 0:
                before = roll_lanes(z_src[RUN - 1], group)
                part = part + (before * ztab[ZUX] if weighted else before)
            if b == RUN - 1:
                after = roll_lanes(z_src[0], -group)
                part = part + (after * ztab[ZDX + b] if weighted else after)
            z_out[b] = part
        for x in range(-reach, cx + reach):
            g, b = divmod(x + cx, RUN)
            mid, extra = src[x + cx], z_src[b]
            up = roll_lanes(jnp.where(is_last[g], extra, mid), 1)
            down = roll_lanes(jnp.where(is_first[g], extra, mid), -1)
            if weighted:
                up, down = up * thrice(up_tab[g]), down * thrice(down_tab[g])
            part = up + down
            if b == 0:
                part = part + roll_lanes(src[x + cx - 1], group)
            if b == RUN - 1:
                part = part + roll_lanes(src[x + cx + 1], -group)
            out[x + cx] = part
        return out, z_out

    def beside(src, sums, xs, weighted):
        lo = xs[0] + cx
        mid = src[pl.ds(lo, len(xs))]
        parts = []
        for x in xs:
            b = (x + cx) % RUN
            part = sums[x + cx]
            if b > 0:
                value = src[x + cx - 1]
                if weighted and x == 1:
                    value = value * below_1
                if weighted and x == cx + 1:
                    value = value * 0.5
                part = part + value
            if b < RUN - 1:
                value = src[x + cx + 1]
                if weighted and x == cx - 2:
                    value = value * above_6
                if weighted and x == -2:
                    value = value * 0.5
                part = part + value
            parts.append(part)
        left, right = rolled(mid, 1, 0), rolled(mid, -1, 0)
        if weighted:
            left, right = left * tab[UPY][None], right * tab[DOWNY][None]
        return mid, jnp.stack(parts) + (left + right)

    def z_beside(z_src, z_sums, b, weighted):
        mid = z_src[b]
        left, right = roll_rows(mid, 1), roll_rows(mid, -1)
        if weighted:
            left, right = left * tab[UPY], right * tab[DOWNY]
        around = z_sums[b] + (left + right)
        if b > 0:
            around = around + (z_src[b - 1] * ztab[ZUX + b] if weighted else z_src[b - 1])
        if b < RUN - 1:
            around = around + (z_src[b + 1] * ztab[ZDX + b] if weighted else z_src[b + 1])
        return mid, around

    def apply_a(c, f, reach, index):
        src, z_src = main.at[c, f], pack.at[c, f]
        sums, z_sums = stream(src, z_src, reach, False)
        if reach > 0:
            for b in range(RUN):
                mid, around = z_beside(z_src, z_sums, b, False)
                czbuf[c, b] = (6.0 * mid - around) * ztab[ZD + b]
        for xs in planes(reach):
            mid, around = beside(src, sums, xs, False)
            value = 6.0 * mid - around
            for i, x in enumerate(xs):
                if 0 <= x < cx:
                    image[index, x] = value[i, cy:2 * cy]
            if reach > 0:
                ds = pl.ds(xs[0] + cx, len(xs))
                cbuf[c, ds] = value * d_tab[ds]

    def scale_only(c, f, reach):
        for b in range(RUN):
            czbuf[c, b] = pack[c, f, b] * ztab[ZD + b]
        for xs in planes(reach):
            ds = pl.ds(xs[0] + cx, len(xs))
            cbuf[c, ds] = main[c, f, ds] * d_tab[ds]

    def apply_m(c, f, reach):
        src, z_src = cbuf.at[c], czbuf.at[c]
        sums, z_sums = stream(src, z_src, reach + 1, True)
        for b in range(RUN):
            mid, around = z_beside(z_src, z_sums, b, True)
            szbuf[c, b] = BETA * mid + around * ztab[ZAM + b]
        for xs in planes(reach + 1):
            mid, around = beside(src, sums, xs, True)
            sbuf[c, pl.ds(xs[0] + cx, len(xs))] = BETA * mid + around * table(AM0, xs)
        s_src, sz_src = sbuf.at[c], szbuf.at[c]
        sums, z_sums = stream(s_src, sz_src, reach, True)
        if reach > 0:
            for b in range(RUN):
                _, around = z_beside(sz_src, z_sums, b, True)
                pack[c, f, b] = z_src[b] * ztab[ZG + b] + around * ztab[ZM + b]
        for xs in planes(reach):
            ds = pl.ds(xs[0] + cx, len(xs))
            _, around = beside(s_src, sums, xs, True)
            value = src[ds] * g_tab[ds]
            if reach > 0:
                main[c, f, ds] = value + around * table(M0, xs)
            else:
                main[c, f, ds, pl.ds(cy, cy)] = (value + around)[:, cy:2 * cy]

    def copy_to(c, s, index):
        dx, dy, dz = OFFSETS[index]
        if dz == 0:
            n = cx if dx == 0 else REACH[s][c] - (dy != 0)
            first = cx if dx <= 0 else 2 * cx - n
            there = pl.ds(first - cx * dx, n)
            source = raw.at[c, s, pl.ds(first, n), pl.ds(cy, cy)]
            sink = raw.at[c, s, there, pl.ds(cy - cy * dy, cy)]
        else:
            source = face.at[c, s]
            sink = got.at[c, s, 0 if dz > 0 else 1, 1 - dx, pl.ds(cy - cy * dy, cy)]
        return pltpu.make_async_remote_copy(
            source, sink, s_sem.at[0], r_sem.at[c, s],
            device_id=target(OFFSETS[index]), device_id_type=MESH)

    per_block = cx // RUN

    def pack_face(c, s):
        value = jnp.zeros((cy, LANES), F32)
        for i in range(RUN):
            joined = main[c, 2 * s, cx + i, pl.ds(cy, cy)]
            for h in range(1, per_block):
                other = main[c, 2 * s, cx + h * RUN + i, pl.ds(cy, cy)]
                joined = jnp.where(slot[:cy] == per_block + h, other, joined)
            moved = roll_lanes(joined, group * (per_block * i - per_block))
            value = jnp.where(slot[:cy] // per_block == i, moved, value)
        face[c, s] = value

    def turn_own(c):
        for x in range(cx):
            main[c, 0, x + cx, pl.ds(cy, cy)] = roll_lanes(raw[c, 0, x + cx, pl.ds(cy, cy)], turn(x))

    def turn_back(c, f, out):
        for x in range(cx):
            out[x] = roll_lanes(main[c, f, x + cx, pl.ds(cy, cy)], -turn(x))

    def send(c, s):
        order = sorted(range(len(OFFSETS)), key=lambda i: -sum(abs(v) for v in OFFSETS[i]))
        for index in order:
            @pl.when(exists(OFFSETS[index]))
            def _():
                copy_to(c, s, index).start()

    around_it = [low[i].astype(jnp.int32) + high[i].astype(jnp.int32) for i in range(3)]
    choices = [{1: (0,), 2: (1,)}.get(n, (1, 2)) for n in counts]

    def tiles_of(c, s, ax, ay, az):
        planes_in = ax * REACH[s][c] + ay * cx + ax * ay * (REACH[s][c] - 1)
        return (planes_in + az * (1 + ax) * (1 + ay)) * (cy // 8)

    def wait_bytes(sem, tiles):
        view = spare.at[pl.ds(0, tiles)]
        pltpu.make_async_copy(view, view, sem).wait()

    def wait_exchanges(sem, pairs):
        for ax in choices[0]:
            for ay in choices[1]:
                for az in choices[2]:
                    here = (around_it[0] == ax) & (around_it[1] == ay) & (around_it[2] == az)
                    tiles = sum(tiles_of(c, s, ax, ay, az) for c, s in pairs)
                    if tiles:
                        @pl.when(here)
                        def _():
                            wait_bytes(sem, tiles)

    def receive(c, s):
        wait_exchanges(r_sem.at[c, s], [(c, s)])
        f = 2 * s
        faces = [jnp.where(is_hi, got[c, s, 1, k], got[c, s, 0, k]) for k in range(3)]
        for b in range(RUN):
            value = jnp.zeros((rows, LANES), F32)
            for k in range(3):
                moved = roll_lanes(faces[k], group * per_block * (k - b))
                value = jnp.where(slot // per_block == k, moved, value)
            pack[c, f, b] = value
        for x in range(-REACH[s][c], cx + REACH[s][c]):
            if 0 <= x < cx:
                for y in (0, 2 * cy):
                    main[c, f, x + cx, pl.ds(y, cy)] = roll_lanes(raw[c, s, x + cx, pl.ds(y, cy)], turn(x))
            else:
                main[c, f, x + cx] = roll_lanes(raw[c, s, x + cx], turn(x))

    def own(c, f):
        return main[c, f, pl.ds(cx, cx), pl.ds(cy, cy)].reshape(cx * cy, LANES)

    def emit(c, f, slot_out):
        turn_back(c, f, pow_ref.at[c, slot_out])

    place_of = {a: (P_CHAIN, a) for a in range(STEPS + 1)}
    place_of.update({STEPS + 1 + k: (Z_CHAIN, k + 1) for k in range(STEPS)})
    ready = []

    def account(a):
        ready.append(a)
        picture = image[a].reshape(cx * cy, LANES)
        for b in ready:
            part = jnp.sum(own(*place_of[b]) * picture, axis=0, keepdims=True)
            t_ref[pl.ds(a * total + b, 1), :] = part
            if a != b:
                t_ref[pl.ds(b * total + a, 1), :] = part
        t_ref[pl.ds(total * total + a, 1), :] = jnp.sum(
            own(*place_of[a]) * own(Z_CHAIN, 0), axis=0, keepdims=True)

    t_ref[...] = jnp.zeros_like(t_ref)
    for copy in loads:
        copy.wait()
    for c in (Z_CHAIN, P_CHAIN):
        turn_own(c)
        pack_face(c, 0)
    pl.semaphore_wait(barrier, expected)
    send(Z_CHAIN, 0)
    send(P_CHAIN, 0)

    first_z = STEPS + 1
    receive(Z_CHAIN, 0)
    scale_only(Z_CHAIN, 0, 5)
    apply_m(Z_CHAIN, 1, 3)
    emit(Z_CHAIN, 1, 0)
    apply_a(Z_CHAIN, 1, 2, first_z)
    apply_m(Z_CHAIN, 2, 0)
    turn_back(Z_CHAIN, 2, raw.at[Z_CHAIN, 1, pl.ds(cx, cx), pl.ds(cy, cy)])
    pack_face(Z_CHAIN, 1)
    send(Z_CHAIN, 1)
    emit(Z_CHAIN, 2, 1)

    receive(P_CHAIN, 0)
    apply_a(P_CHAIN, 0, 5, 0)
    apply_m(P_CHAIN, 1, 3)
    emit(P_CHAIN, 1, 0)
    apply_a(P_CHAIN, 1, 2, 1)
    apply_m(P_CHAIN, 2, 0)
    turn_back(P_CHAIN, 2, raw.at[P_CHAIN, 1, pl.ds(cx, cx), pl.ds(cy, cy)])
    pack_face(P_CHAIN, 1)
    send(P_CHAIN, 1)
    emit(P_CHAIN, 2, 1)
    for a in (0, 1, first_z):
        account(a)

    receive(Z_CHAIN, 1)
    apply_a(Z_CHAIN, 2, 6, first_z + 1)
    apply_m(Z_CHAIN, 3, 4)
    emit(Z_CHAIN, 3, 2)
    apply_a(Z_CHAIN, 3, 3, first_z + 2)
    apply_m(Z_CHAIN, 4, 1)
    emit(Z_CHAIN, 4, 3)
    apply_a(Z_CHAIN, 4, 0, first_z + 3)
    for a in (first_z + 1, first_z + 2, first_z + 3):
        account(a)

    receive(P_CHAIN, 1)
    apply_a(P_CHAIN, 2, 6, 2)
    account(2)
    apply_m(P_CHAIN, 3, 4)
    emit(P_CHAIN, 3, 2)
    apply_a(P_CHAIN, 3, 3, 3)
    account(3)
    apply_m(P_CHAIN, 4, 1)
    emit(P_CHAIN, 4, 3)
    apply_a(P_CHAIN, 4, 0, 4)
    account(4)

    value = lax.dot_general(
        jnp.ones((8, LANES), F32), t_ref[...], (((1,), (1,)), ((), ())),
        precision=HIGHEST, preferred_element_type=F32)[0:1]

    def gather(value, axes, buffer, send_sem, recv_sem, meanwhile=lambda: None):
        size, make = ahead(axes)
        buffer[0] = value

        def copy(k):
            return pltpu.make_async_remote_copy(
                buffer.at[0], buffer.at[k], send_sem.at[0], recv_sem.at[0],
                device_id=make(k), device_id_type=MESH)

        for k in range(1, size):
            copy(k).start()
        meanwhile()
        rest = buffer.at[pl.ds(1, size - 1)]
        pltpu.make_async_copy(rest, rest, send_sem.at[0]).wait()
        pltpu.make_async_copy(rest, rest, recv_sem.at[0]).wait()
        result = jnp.zeros_like(value)
        for k in range(size):
            rest, at = k, 0
            scale = 1
            for a in reversed(axes):
                n = counts[AXES.index(a)]
                rest, want = divmod(rest, n)
                at = at + scale * lax.rem(place[AXES.index(a)] + n - want, n)
                scale *= n
            result = result + buffer[at]
        return result

    def finish():
        wait_exchanges(s_sem.at[0], [(c, s) for c in (0, 1) for s in (0, 1)])

    if near:
        value = gather(value, AXES, red0, s0_sem, r0_sem, finish)
    else:
        value = gather(value, ("gy", "gz"), red0, s0_sem, r0_sem, finish)
        value = gather(value, ("gx",), red1, s1_sem, r1_sem)
    value = value * (1.0 / (nx * cx * ny * cy * nz * cz))
    for a in range(total):
        gram_ref[a:a + 1, :] = value[0:1, a * total:(a + 1) * total]
    proj_ref[...] = value[0:1, total * total:total * total + total]


def store(pow_ref, gram_ref, proj_ref, pow_out, gram_out, proj_out, sem):
    pairs = ((pow_ref, pow_out), (gram_ref, gram_out), (proj_ref, proj_out))
    copies = [pltpu.make_async_copy(a, b, sem.at[i]) for i, (a, b) in enumerate(pairs)]
    for copy in copies:
        copy.start()
    for copy in copies:
        copy.wait()


def solution(mesh):
    counts = tuple(mesh.shape[a] for a in AXES)
    near = max(counts) <= 4
    devices = counts[0] * counts[1] * counts[2]
    plane = devices if near else counts[1] * counts[2]

    def local(residual, direction):
        dims = residual.shape
        cx, cy, cz = dims
        assert cz == LANES and LANES % cx == 0 and cy % 8 == 0
        assert min(cx, cy, LANES // cx // 2) > max(max(r) for r in REACH)
        total = 2 * STEPS + 1
        fields = STEPS + 1
        dma = pltpu.SemaphoreType.DMA
        vm = pl.BlockSpec(memory_space=pltpu.VMEM)
        hbm = pl.BlockSpec(memory_space=pltpu.HBM)
        ext = (3 * cx, 3 * cy, LANES)
        zext = (RUN, 3 * cy, LANES)
        powers, gram, proj = pl.pallas_call(
            functools.partial(kernel, counts, dims, near),
            out_shape=(
                jax.ShapeDtypeStruct((2, STEPS) + dims, F32),
                jax.ShapeDtypeStruct((total, total), F32),
                jax.ShapeDtypeStruct((1, total), F32),
            ),
            in_specs=[hbm, hbm],
            out_specs=(vm, vm, vm),
            scratch_shapes=[
                pltpu.VMEM((2, 2) + ext, F32),
                pltpu.VMEM((2, fields) + ext, F32),
                pltpu.VMEM((2, fields) + zext, F32),
                pltpu.VMEM((2, 2, 2, 3, 3 * cy, LANES), F32),
                pltpu.VMEM((2, 2, cy, LANES), F32),
                pltpu.VMEM((2, STEPS) + dims, F32),
                pltpu.VMEM((2,) + ext, F32),
                pltpu.VMEM((2,) + zext, F32),
                pltpu.VMEM((2,) + ext, F32),
                pltpu.VMEM((2,) + zext, F32),
                pltpu.VMEM((total,) + dims, F32),
                pltpu.VMEM((2,) + ext, F32),
                pltpu.VMEM((2,) + zext, F32),
                pltpu.VMEM((8, 3 * cy, LANES), F32),
                pltpu.VMEM((6 * RUN + 2, 3 * cy, LANES), F32),
                pltpu.VMEM((3 * cx // RUN, cy, LANES), F32),
                pltpu.VMEM((3 * cx // RUN, cy, LANES), F32),
                pltpu.VMEM(ext, F32),
                pltpu.VMEM(ext, F32),
                pltpu.VMEM((LANES, LANES), F32),
                pltpu.VMEM((plane, 1, LANES), F32),
                pltpu.VMEM((counts[0], 1, LANES), F32),
                pltpu.VMEM((4 * 9 * cx * (cy // 8), 8, LANES), F32),
                dma((2,)), dma((1,)),
                dma((1,)), dma((2, 2)),
                dma((1,)), dma((1,)),
                dma((1,)), dma((1,)),
            ],
            compiler_params=pltpu.CompilerParams(collective_id=0, has_side_effects=True, vmem_limit_bytes=24 << 20),
            name="powers_basis",
        )(*[pltpu.with_memory_space_constraint(v, pltpu.HBM) for v in (residual, direction)])
        powers, gram, proj = pl.pallas_call(
            store,
            out_shape=(
                jax.ShapeDtypeStruct((2, STEPS) + dims, F32),
                jax.ShapeDtypeStruct((total, total), F32),
                jax.ShapeDtypeStruct((1, total), F32),
            ),
            in_specs=[vm, vm, vm],
            out_specs=(hbm, hbm, hbm),
            scratch_shapes=[dma((3,))],
            compiler_params=pltpu.CompilerParams(vmem_limit_bytes=1 << 20),
            name="store",
        )(powers, gram, proj)
        return powers, gram, proj.reshape(total)

    placed = (P("gx", "gy", "gz"), P("gx", "gy", "gz"))
    return jax.shard_map(
        local,
        mesh=mesh,
        in_specs=placed,
        out_specs=(P(None, None, "gx", "gy", "gz"), P(), P()),
        check_vma=False,
    )
```

```python
import functools

import jax
import jax.numpy as jnp
from jax import lax
from jax.experimental import pallas as pl
from jax.experimental.pallas import tpu as pltpu
from jax.sharding import PartitionSpec as P

STEPS = 4
LANES = 128
MESH = pl.DeviceIdType.MESH
HIGHEST = lax.Precision.HIGHEST
F32 = jnp.float32
AXES = ("gx", "gy", "gz")
GAMMA, BETA, ALPHA, DELTA = 13.0 / 81.0, 5.0 / 243.0, 1.0 / 729.0, 1.0 / 1458.0
P_CHAIN, Z_CHAIN = 0, 1
REACH = ((6, 5), (7, 7))
CHUNK = 4
RUN = 4
OFFSETS = [(dx, dy, dz) for dx in (-1, 0, 1) for dy in (-1, 0, 1) for dz in (-1, 0, 1) if (dx, dy, dz) != (0, 0, 0)]


def as_f32(flag):
    return jnp.where(flag, 1.0, 0.0).astype(F32)


def axis_terms(at, width, low, high, place, count):
    inside = (place * width + at >= 0) & (place * width + at < count * width)
    cover = ((at == -1) | (at == 0)) & low | ((at == width - 1) | (at == width)) & high
    inner = ((at == -2) | (at == 1)) & low | ((at == width - 2) | (at == width + 1)) & high
    below = (at == 1) & low | (at == width + 1) & high
    above = (at == -2) & low | (at == width - 2) & high
    mask = as_f32(inside)
    return (1.0 + as_f32(cover)) * mask, as_f32(inner), 1.0 - 0.5 * as_f32(below), 1.0 - 0.5 * as_f32(above), mask


def kernel(
    counts, dims, near, res_ref, dir_ref, pow_ref, gram_ref, proj_ref,
    raw, main, pack, got, face, flat, cbuf, czbuf, sbuf, szbuf, image, zsum, zzsum, tab, ztab, half_tab, d_tab, g_tab, t_ref, red0, red1, spare,
    in_sem, out_sem, s_sem, r_sem, s0_sem, r0_sem, s1_sem, r1_sem,
):
    nx, ny, nz = counts
    cx, cy, cz = dims
    group = LANES // cx
    half = group // 2
    rows = 3 * cy
    place = [lax.axis_index(a) for a in AXES]
    gx, gy, gz = place
    low = [place[i] > 0 for i in range(3)]
    high = [place[i] < counts[i] - 1 for i in range(3)]
    total = 2 * STEPS + 1

    def exists(offset):
        ok = None
        for i, step in enumerate(offset):
            if step:
                test = low[i] if step < 0 else high[i]
                ok = test if ok is None else jnp.logical_and(ok, test)
        return ok

    def flip(offset):
        return tuple(-s for s in offset)

    def target(offset):
        return {AXES[i]: place[i] + s for i, s in enumerate(offset) if s}

    def ahead(axes):
        def make(k):
            out = {}
            for a in reversed(axes):
                k, step = divmod(k, counts[AXES.index(a)])
                if step:
                    out[a] = lax.rem(place[AXES.index(a)] + step, counts[AXES.index(a)])
            return out
        size = 1
        for a in axes:
            size *= counts[AXES.index(a)]
        return size, make

    loads = [
        pltpu.make_async_copy(ref, raw.at[c, 0, pl.ds(cx, cx), pl.ds(cy, cy)], in_sem.at[c])
        for c, ref in ((Z_CHAIN, res_ref), (P_CHAIN, dir_ref))
    ]
    for copy in loads:
        copy.start()

    barrier = pltpu.get_barrier_semaphore()
    expected = 0
    far_first = sorted(range(len(OFFSETS)), key=lambda i: -sum(abs(v) for v in OFFSETS[i]))
    for offset in [OFFSETS[i] for i in far_first]:
        @pl.when(exists(offset))
        def _():
            pl.semaphore_signal(barrier, 1, device_id=target(offset), device_id_type=MESH)
        expected = expected + exists(offset).astype(jnp.int32)
    if not near:
        for axes in (("gy", "gz"), ("gx",)):
            size, make = ahead(axes)
            for k in range(1, size):
                pl.semaphore_signal(barrier, 1, device_id=make(k), device_id_type=MESH)
            expected = expected + (size - 1)

    row = lax.broadcasted_iota(jnp.int32, (cy, LANES), 0)
    lane = lax.broadcasted_iota(jnp.int32, (cy, LANES), 1)
    top, bottom = row == 0, row == cy - 1
    runs = 3 * cx // RUN
    slot = (lane + half) // group % cx
    deep = (lane + half) % group - half
    is_hi = deep >= 0
    at_first, at_last = deep == 0, deep == -1
    is_first = [lane == group * g for g in range(runs)]
    is_last = [lane == (group * g - 1) % LANES for g in range(runs)]
    is_edge = [is_first[g] | is_last[g] for g in range(runs)]

    def x_terms(x):
        return axis_terms(jnp.int32(x), cx, low[0], high[0], gx, nx)

    below_1, above_6 = x_terms(1)[2], x_terms(cx - 2)[3]

    def turn(x):
        return group * ((x + cx) // RUN)

    TALL, SHORT = 3, 2
    AM0, M0, UPY, DOWNY = 0, 3, 6, 7
    ZD, ZAM, ZM, ZG, ZUX, ZDX = (RUN * k for k in range(6))

    def fill_tables():
        half_z = 1.0 - 0.5 * (as_f32((lane == 0) & low[2]) + as_f32((lane == LANES - 1) & high[2]))
        for g in range(runs):
            half_tab[g] = roll_lanes(half_z, group * g)
        half_tab[runs] = 1.0 - 0.5 * as_f32(at_first | at_last)
        wz, fz, _, _, mz = axis_terms(lane, cz, low[2], high[2], gz, nz)
        z_at = jnp.where(is_hi, deep + cz, deep)
        wzz, fzz, _, _, mzz = axis_terms(z_at, cz, low[2], high[2], gz, nz)
        along = [axis_terms(slot * RUN + (b - cx), cx, low[0], high[0], gx, nx) for b in range(RUN)]
        for high_rows in (TALL, SHORT):
            t = TALL - high_rows
            for k in range(high_rows):
                ds = pl.ds(k * cy, cy)
                if high_rows == TALL:
                    y = row + (k - 1) * cy
                elif k == 0:
                    y = jnp.where(row < cy // 2, row + cy, row - cy)
                else:
                    y = row
                wy, fy, up_y, down_y, my = axis_terms(y, cy, low[1], high[1], gy, ny)
                wyz, myz, gyz = wy * wz, my * mz, GAMMA + DELTA * (fy + fz)
                for n, x in enumerate((-3, 3, cx + 2)):
                    mask = myz * x_terms(x)[4]
                    tab[t, AM0 + n, ds] = mask * ALPHA
                    tab[t, M0 + n, ds] = mask
                tab[t, UPY, ds], tab[t, DOWNY, ds] = up_y, down_y
                for g in range(runs):
                    d_run, g_run = roll_lanes(wyz, group * g), roll_lanes(gyz, group * g)
                    for n in range(RUN * g, RUN * g + RUN):
                        cover, inner = x_terms(n - cx)[:2]
                        d_tab[t, n, ds] = d_run * cover
                        g_tab[t, n, ds] = g_run + DELTA * inner
                for b in range(RUN):
                    wx, fx, up_x, down_x, mx = along[b]
                    ztab[t, ZD + b, ds] = wx * wy * wzz
                    ztab[t, ZAM + b, ds] = mx * my * mzz * ALPHA
                    ztab[t, ZM + b, ds] = mx * my * mzz
                    ztab[t, ZG + b, ds] = GAMMA + DELTA * (fx + fy + fzz)
                    ztab[t, ZUX + b, ds] = up_x
                    ztab[t, ZDX + b, ds] = down_x

    def fill_zeros():
        fields = [(c, f) for c in (0, 1) for f in (0, 1)]
        for flag, xs, ys in (
            (low[0], pl.ds(0, cx), pl.ds(0, rows)), (high[0], pl.ds(2 * cx, cx), pl.ds(0, rows)),
            (low[1], pl.ds(0, 3 * cx), pl.ds(0, cy)), (high[1], pl.ds(0, 3 * cx), pl.ds(2 * cy, cy)),
        ):
            @pl.when(jnp.logical_not(flag))
            def _():
                for c, f in fields:
                    raw[c, f, xs, ys] = jnp.zeros((xs.size, ys.size, LANES), F32)
        for flag, ss, xs, ys in (
            (low[2], 0, pl.ds(0, 3), pl.ds(0, rows)), (high[2], 1, pl.ds(0, 3), pl.ds(0, rows)),
            (low[0], None, pl.ds(0, 1), pl.ds(0, rows)), (high[0], None, pl.ds(2, 1), pl.ds(0, rows)),
            (low[1], None, pl.ds(0, 3), pl.ds(0, cy)), (high[1], None, pl.ds(0, 3), pl.ds(2 * cy, cy)),
        ):
            @pl.when(jnp.logical_not(flag))
            def _():
                for c in (0, 1):
                    for s in (0, 1):
                        for side in ((0, 1) if ss is None else (ss,)):
                            got[c, s, side, xs, ys] = jnp.zeros((xs.size, ys.size, LANES), F32)

    def roll_rows(v, shift):
        return pltpu.roll(v, shift % v.shape[0], 0)

    def roll_lanes(v, shift):
        shift = shift % LANES
        return v if shift == 0 else pltpu.roll(v, shift, 1)

    def planes(reach):
        xs = list(range(-reach, cx + reach))
        return [xs[i:i + CHUNK] for i in range(0, len(xs), CHUNK)]

    def table(t, at, xs, n):
        ks = [at + (x + cx) // cx for x in xs]
        if len(set(ks)) == 1:
            return tab[t, ks[0], pl.ds(0, n)][None]
        return jnp.stack([tab[t, k, pl.ds(0, n)] for k in ks])

    def spread(v, tiles):
        return jnp.concatenate([v] * tiles, axis=0)

    def wide(mask, tiles):
        return jnp.concatenate([mask] * tiles, axis=0)

    def put(dst, xs, value, reach, tiles):
        for i, x in enumerate(xs):
            if reach > 0 and -reach < x < cx + reach - 1:
                dst[x + cx, pl.ds(0, tiles * cy)] = value[i]
            else:
                dst[x + cx, pl.ds(cy, cy)] = value[i, cy:2 * cy]

    flips = [0]

    def stream(src, z_src, reach, weighted, tiles):
        flips[0] ^= 1
        out, z_out = zsum.at[flips[0]], zzsum.at[flips[0]]
        t, n = TALL - tiles, tiles * cy
        ds = pl.ds(0, n)
        for x in range(-reach, cx + reach):
            g, b = divmod(x + cx, RUN)
            mid, extra = src[x + cx, ds], z_src[b, ds]
            if weighted:
                mid = mid * spread(half_tab[g], tiles)
            up = roll_lanes(jnp.where(wide(is_last[g], tiles), extra, mid), 1)
            down = roll_lanes(jnp.where(wide(is_first[g], tiles), extra, mid), -1)
            part = up + down
            if b == 0:
                part = part + roll_lanes(src[x + cx - 1, ds], group)
            if b == RUN - 1:
                part = part + roll_lanes(src[x + cx + 1, ds], -group)
            put(out, [x], part[None], reach, tiles)
        for b in range(RUN if reach > 0 else 0):
            mid = z_src[b, ds]
            inject = jnp.zeros((n, LANES), F32)
            for g in range(runs):
                x = g * RUN + b - cx
                if -reach <= x < cx + reach:
                    inject = jnp.where(wide(is_edge[g], tiles), src[x + cx, ds], inject)
            if weighted:
                mid = mid * spread(half_tab[runs], tiles)
            part = roll_lanes(jnp.where(wide(at_last, tiles), inject, mid), 1)
            part = part + roll_lanes(jnp.where(wide(at_first, tiles), inject, mid), -1)
            if b == 0:
                before = roll_lanes(z_src[RUN - 1, ds], group)
                part = part + (before * ztab[t, ZUX, ds] if weighted else before)
            if b == RUN - 1:
                after = roll_lanes(z_src[0, ds], -group)
                part = part + (after * ztab[t, ZDX + b, ds] if weighted else after)
            z_out[b, ds] = part
        return out, z_out

    def along_y(parts, weighted, tiles):
        t = TALL - tiles
        ahead_of = [pltpu.roll(v, 1, v.ndim - 2) for v in parts]
        behind = [pltpu.roll(v, cy - 1, v.ndim - 2) for v in parts]
        sums = []
        for k in range(tiles):
            left, right = ahead_of[k], behind[k]
            before = k - 1 if tiles == TALL else 1 - k
            after = k + 1 if tiles == TALL else 1 - k
            if before >= 0:
                left = jnp.where(top, ahead_of[before], left)
            if after < tiles:
                right = jnp.where(bottom, behind[after], right)
            if weighted and not (tiles == TALL and k == 0):
                left = left * tab[t, UPY, pl.ds(k * cy, cy)]
            if weighted and not (tiles == TALL and k == 2):
                right = right * tab[t, DOWNY, pl.ds(k * cy, cy)]
            sums.append(left + right)
        return jnp.concatenate(sums, axis=-2)

    def beside(src, sums, xs, weighted, tiles):
        lo = xs[0] + cx
        ds = pl.ds(0, tiles * cy)
        mid = src[pl.ds(lo, len(xs)), ds]
        parts = []
        for x in xs:
            b = (x + cx) % RUN
            part = sums[x + cx, ds]
            if b > 0:
                value = src[x + cx - 1, ds]
                if weighted and x == 1:
                    value = value * below_1
                if weighted and x == cx + 1:
                    value = value * 0.5
                part = part + value
            if b < RUN - 1:
                value = src[x + cx + 1, ds]
                if weighted and x == cx - 2:
                    value = value * above_6
                if weighted and x == -2:
                    value = value * 0.5
                part = part + value
            columns = [src[x + cx, pl.ds(k * cy, cy)] for k in range(tiles)]
            parts.append(part + along_y(columns, weighted, tiles))
        return mid, jnp.stack(parts)

    def z_beside(z_src, z_sums, b, weighted, tiles):
        t, ds = TALL - tiles, pl.ds(0, tiles * cy)
        around = z_sums[b, ds] + along_y([z_src[b, pl.ds(k * cy, cy)] for k in range(tiles)], weighted, tiles)
        if b > 0:
            value = z_src[b - 1, ds]
            around = around + (value * ztab[t, ZUX + b, ds] if weighted else value)
        if b < RUN - 1:
            value = z_src[b + 1, ds]
            around = around + (value * ztab[t, ZDX + b, ds] if weighted else value)
        return z_src[b, ds], around

    def shorten(v):
        outer = jnp.where(row < cy // 2, v[..., 2 * cy:, :], v[..., :cy, :])
        return jnp.concatenate([outer, v[..., cy:2 * cy, :]], axis=-2)

    def apply_a(c, f, reach, index, tiles):
        t, n = TALL - tiles, tiles * cy
        src, z_src = main.at[c, f], pack.at[c, f]
        sums, z_sums = stream(src, z_src, reach, False, tiles)
        for b in range(RUN if reach > 0 else 0):
            mid, around = z_beside(z_src, z_sums, b, False, tiles)
            czbuf[c, b, pl.ds(0, n)] = (6.0 * mid - around) * ztab[t, ZD + b, pl.ds(0, n)]
        for xs in planes(reach):
            mid, around = beside(src, sums, xs, False, tiles)
            value = 6.0 * mid - around
            for i, x in enumerate(xs):
                if 0 <= x < cx:
                    image[index, x] = value[i, cy:2 * cy]
            if reach > 0:
                ds = pl.ds(xs[0] + cx, len(xs))
                put(cbuf.at[c], xs, value * d_tab[t, ds, pl.ds(0, n)], reach, tiles)

    def scale_only(c, f, reach):
        for b in range(RUN):
            czbuf[c, b] = pack[c, f, b] * ztab[0, ZD + b]
        for xs in planes(reach):
            ds = pl.ds(xs[0] + cx, len(xs))
            put(cbuf.at[c], xs, main[c, f, ds] * d_tab[0, ds], reach, TALL)

    def apply_m(c, f, reach, tiles):
        t, n = TALL - tiles, tiles * cy
        rows = pl.ds(0, n)
        src, z_src = cbuf.at[c], czbuf.at[c]
        sums, z_sums = stream(src, z_src, reach + 1, True, tiles)
        for b in range(RUN):
            mid, around = z_beside(z_src, z_sums, b, True, tiles)
            szbuf[c, b, rows] = BETA * mid + around * ztab[t, ZAM + b, rows]
        for xs in planes(reach + 1):
            mid, around = beside(src, sums, xs, True, tiles)
            put(sbuf.at[c], xs, BETA * mid + around * table(t, AM0, xs, n), reach + 1, tiles)
        s_src, sz_src = sbuf.at[c], szbuf.at[c]
        sums, z_sums = stream(s_src, sz_src, reach, True, tiles)
        for b in range(RUN if reach > 0 else 0):
            _, around = z_beside(sz_src, z_sums, b, True, tiles)
            value = z_src[b, rows] * ztab[t, ZG + b, rows] + around * ztab[t, ZM + b, rows]
            pack[c, f, b, pl.ds(0, SHORT * cy)] = shorten(value) if tiles == TALL else value
        for xs in planes(reach):
            ds = pl.ds(xs[0] + cx, len(xs))
            _, around = beside(s_src, sums, xs, True, tiles)
            value = src[ds, rows] * g_tab[t, ds, rows]
            if reach > 0:
                value = value + around * table(t, M0, xs, n)
            else:
                value = value + around
            if tiles == TALL:
                value = shorten(value)
            put(main.at[c, f], xs, value, reach, SHORT)

    def parts_of(c, s, index):
        dx, dy, dz = OFFSETS[index]
        reach = REACH[s][c]
        if dz or dx == 0:
            return [(0, cx, cy)]
        if dy == 0:
            return [(0, reach, cy)]
        full = max(0, reach - cy // 2 - 1)
        return [p for p in ((0, full, cy), (full, reach - 1 - full, cy // 2)) if p[1] > 0]

    def copy_to(c, s, index, part):
        dx, dy, dz = OFFSETS[index]
        if dz == 0:
            skip, n, h = part
            first = cx + skip if dx <= 0 else 2 * cx - skip - n
            here = pl.ds(cy if dy <= 0 else 2 * cy - h, h)
            there = pl.ds(here.start - cy * dy, h)
            source = raw.at[c, s, pl.ds(first, n), here]
            sink = raw.at[c, s, pl.ds(first - cx * dx, n), there]
        else:
            source = face.at[c, s]
            sink = got.at[c, s, 0 if dz > 0 else 1, 1 - dx, pl.ds(cy - cy * dy, cy)]
        return pltpu.make_async_remote_copy(
            source, sink, s_sem.at[0], r_sem.at[c, s],
            device_id=target(OFFSETS[index]), device_id_type=MESH)

    per_block = cx // RUN

    def pack_face(c, s):
        value = jnp.zeros((cy, LANES), F32)
        for i in range(RUN):
            joined = main[c, 2 * s, cx + i, pl.ds(cy, cy)]
            for h in range(1, per_block):
                other = main[c, 2 * s, cx + h * RUN + i, pl.ds(cy, cy)]
                joined = jnp.where(slot == per_block + h, other, joined)
            moved = roll_lanes(joined, group * (per_block * i - per_block))
            value = jnp.where(slot // per_block == i, moved, value)
        face[c, s] = value

    def turn_own(c):
        for x in range(cx):
            main[c, 0, x + cx, pl.ds(cy, cy)] = roll_lanes(raw[c, 0, x + cx, pl.ds(cy, cy)], turn(x))

    def turn_back(c, f, out):
        for x in range(cx):
            out[x] = roll_lanes(main[c, f, x + cx, pl.ds(cy, cy)], -turn(x))

    def send(c, s):
        for index in far_first:
            @pl.when(exists(OFFSETS[index]))
            def _():
                for part in parts_of(c, s, index):
                    copy_to(c, s, index, part).start()

    around_it = [low[i].astype(jnp.int32) + high[i].astype(jnp.int32) for i in range(3)]
    choices = [{1: (0,), 2: (1,)}.get(n, (1, 2)) for n in counts]

    def tiles_of(c, s, ax, ay, az):
        sizes = {o: sum(n * h for _, n, h in parts_of(c, s, i)) for i, o in enumerate(OFFSETS)}
        in_rows = ax * sizes[1, 0, 0] + ay * sizes[0, 1, 0] + ax * ay * sizes[1, 1, 0]
        return (in_rows + az * (1 + ax) * (1 + ay) * cy) // 4

    def wait_bytes(sem, tiles):
        view = spare.at[pl.ds(0, tiles)]
        pltpu.make_async_copy(view, view, sem).wait()

    def wait_exchanges(sem, pairs):
        for ax in choices[0]:
            for ay in choices[1]:
                for az in choices[2]:
                    here = (around_it[0] == ax) & (around_it[1] == ay) & (around_it[2] == az)
                    tiles = sum(tiles_of(c, s, ax, ay, az) for c, s in pairs)
                    if tiles:
                        @pl.when(here)
                        def _():
                            wait_bytes(sem, tiles)

    def receive(c, s):
        wait_exchanges(r_sem.at[c, s], [(c, s)])
        f = 2 * s
        hi, at_block = wide(is_hi, TALL), [wide(slot // per_block == k, TALL) for k in range(3)]
        faces = [jnp.where(hi, got[c, s, 1, k], got[c, s, 0, k]) for k in range(3)]
        for b in range(RUN):
            value = jnp.zeros((TALL * cy, LANES), F32)
            for k in range(3):
                moved = roll_lanes(faces[k], group * per_block * (k - b))
                value = jnp.where(at_block[k], moved, value)
            pack[c, f, b] = value
        for x in range(-REACH[s][c], cx + REACH[s][c]):
            if 0 <= x < cx:
                for y in (0, 2 * cy):
                    main[c, f, x + cx, pl.ds(y, cy)] = roll_lanes(raw[c, s, x + cx, pl.ds(y, cy)], turn(x))
            else:
                main[c, f, x + cx] = roll_lanes(raw[c, s, x + cx], turn(x))

    def own(c, f):
        return main[c, f, pl.ds(cx, cx), pl.ds(cy, cy)].reshape(cx * cy, LANES)

    def emit(c, f, slot_out):
        turn_back(c, f, pow_ref.at[c, slot_out])

    place_of = {a: (P_CHAIN, a) for a in range(STEPS + 1)}
    place_of.update({STEPS + 1 + k: (Z_CHAIN, k + 1) for k in range(STEPS)})
    ready = []

    def account(a):
        ready.append(a)
        picture = image[a].reshape(cx * cy, LANES)
        for b in ready:
            part = jnp.sum(own(*place_of[b]) * picture, axis=0, keepdims=True)
            t_ref[pl.ds(a * total + b, 1), :] = part
            if a != b:
                t_ref[pl.ds(b * total + a, 1), :] = part
        t_ref[pl.ds(total * total + a, 1), :] = jnp.sum(
            own(*place_of[a]) * own(Z_CHAIN, 0), axis=0, keepdims=True)

    for copy in loads:
        copy.wait()
    for c in (Z_CHAIN, P_CHAIN):
        value = jnp.zeros((cy, LANES), F32)
        for x in range(cx):
            at = per_block * (x % RUN) + x // RUN
            value = jnp.where(slot == at, roll_lanes(raw[c, 0, x + cx, pl.ds(cy, cy)], group * at), value)
        face[c, 0] = value
    pl.semaphore_wait(barrier, expected)
    for c in (Z_CHAIN, P_CHAIN):
        send(c, 0)
    for c in (Z_CHAIN, P_CHAIN):
        turn_own(c)
    fill_zeros()
    fill_tables()
    t_ref[...] = jnp.zeros_like(t_ref)

    def finish_first(c):
        turn_back(c, 2, raw.at[c, 1, pl.ds(cx, cx), pl.ds(cy, cy)])
        pack_face(c, 1)
        send(c, 1)

    first_z = STEPS + 1
    receive(Z_CHAIN, 0)
    scale_only(Z_CHAIN, 0, 5)
    apply_m(Z_CHAIN, 1, 3, TALL)
    apply_a(Z_CHAIN, 1, 2, first_z, SHORT)
    apply_m(Z_CHAIN, 2, 0, SHORT)
    finish_first(Z_CHAIN)

    receive(P_CHAIN, 0)
    apply_a(P_CHAIN, 0, 5, 0, TALL)
    apply_m(P_CHAIN, 1, 3, TALL)
    apply_a(P_CHAIN, 1, 2, 1, SHORT)
    apply_m(P_CHAIN, 2, 0, SHORT)
    finish_first(P_CHAIN)
    for c in (Z_CHAIN, P_CHAIN):
        emit(c, 1, 0)
        emit(c, 2, 1)
    for a in (0, 1, first_z):
        account(a)

    receive(Z_CHAIN, 1)
    apply_a(Z_CHAIN, 2, 6, first_z + 1, TALL)
    apply_m(Z_CHAIN, 3, 4, TALL)
    apply_a(Z_CHAIN, 3, 3, first_z + 2, SHORT)
    apply_m(Z_CHAIN, 4, 1, SHORT)
    apply_a(Z_CHAIN, 4, 0, first_z + 3, SHORT)
    for k in (1, 2, 3):
        account(first_z + k)
    for k in (3, 4):
        emit(Z_CHAIN, k, k - 1)

    receive(P_CHAIN, 1)
    apply_a(P_CHAIN, 2, 6, 2, TALL)
    account(2)
    apply_m(P_CHAIN, 3, 4, TALL)
    emit(P_CHAIN, 3, 2)
    apply_a(P_CHAIN, 3, 3, 3, SHORT)
    account(3)
    apply_m(P_CHAIN, 4, 1, SHORT)
    emit(P_CHAIN, 4, 3)
    apply_a(P_CHAIN, 4, 0, 4, SHORT)
    account(4)

    value = lax.dot_general(
        jnp.ones((8, LANES), F32), t_ref[...], (((1,), (1,)), ((), ())),
        precision=HIGHEST, preferred_element_type=F32)[0:1]

    def far_order(size, axes):
        def hops(k):
            far = 0
            for a in reversed(axes):
                n = counts[AXES.index(a)]
                k, step = divmod(k, n)
                far += min(step, n - step)
            return -far
        return sorted(range(1, size), key=hops)

    def gather(value, axes, buffer, send_sem, recv_sem, meanwhile=lambda: None):
        size, make = ahead(axes)
        buffer[0] = value

        def copy(k):
            return pltpu.make_async_remote_copy(
                buffer.at[0], buffer.at[k], send_sem.at[0], recv_sem.at[0],
                device_id=make(k), device_id_type=MESH)

        for k in far_order(size, axes):
            copy(k).start()
        meanwhile()
        rest = buffer.at[pl.ds(1, size - 1)]
        pltpu.make_async_copy(rest, rest, send_sem.at[0]).wait()
        pltpu.make_async_copy(rest, rest, recv_sem.at[0]).wait()
        result = jnp.zeros_like(value)
        for k in range(size):
            rest, at = k, 0
            scale = 1
            for a in reversed(axes):
                n = counts[AXES.index(a)]
                rest, want = divmod(rest, n)
                at = at + scale * lax.rem(place[AXES.index(a)] + n - want, n)
                scale *= n
            result = result + buffer[at]
        return result

    def finish():
        wait_exchanges(s_sem.at[0], [(c, s) for c in (0, 1) for s in (0, 1)])

    if near:
        value = gather(value, AXES, red0, s0_sem, r0_sem, finish)
    else:
        value = gather(value, ("gy", "gz"), red0, s0_sem, r0_sem, finish)
        value = gather(value, ("gx",), red1, s1_sem, r1_sem)
    value = value * (1.0 / (nx * cx * ny * cy * nz * cz))
    for a in range(total):
        gram_ref[a:a + 1, :] = value[0:1, a * total:(a + 1) * total]
    proj_ref[...] = value[0:1, total * total:total * total + total]


def store(pow_ref, gram_ref, proj_ref, pow_out, gram_out, proj_out, sem):
    pairs = ((pow_ref, pow_out), (gram_ref, gram_out), (proj_ref, proj_out))
    copies = [pltpu.make_async_copy(a, b, sem.at[i]) for i, (a, b) in enumerate(pairs)]
    for copy in copies:
        copy.start()
    for copy in copies:
        copy.wait()


def solution(mesh):
    counts = tuple(mesh.shape[a] for a in AXES)
    near = max(counts) <= 4
    devices = counts[0] * counts[1] * counts[2]
    plane = devices if near else counts[1] * counts[2]

    def local(residual, direction):
        dims = residual.shape
        cx, cy, cz = dims
        assert cz == LANES and LANES % cx == 0 and cy % 8 == 0
        assert min(cx, cy, LANES // cx // 2) > max(max(r) for r in REACH)
        total = 2 * STEPS + 1
        fields = STEPS + 1
        dma = pltpu.SemaphoreType.DMA
        vm = pl.BlockSpec(memory_space=pltpu.VMEM)
        hbm = pl.BlockSpec(memory_space=pltpu.HBM)
        ext = (3 * cx, 3 * cy, LANES)
        zext = (RUN, 3 * cy, LANES)
        powers, gram, proj = pl.pallas_call(
            functools.partial(kernel, counts, dims, near),
            out_shape=(
                jax.ShapeDtypeStruct((2, STEPS) + dims, F32),
                jax.ShapeDtypeStruct((total, total), F32),
                jax.ShapeDtypeStruct((1, total), F32),
            ),
            in_specs=[hbm, hbm],
            out_specs=(vm, vm, vm),
            scratch_shapes=[
                pltpu.VMEM((2, 2) + ext, F32),
                pltpu.VMEM((2, fields) + ext, F32),
                pltpu.VMEM((2, fields) + zext, F32),
                pltpu.VMEM((2, 2, 2, 3, 3 * cy, LANES), F32),
                pltpu.VMEM((2, 2, cy, LANES), F32),
                pltpu.VMEM((2, STEPS) + dims, F32),
                pltpu.VMEM((2,) + ext, F32),
                pltpu.VMEM((2,) + zext, F32),
                pltpu.VMEM((2,) + ext, F32),
                pltpu.VMEM((2,) + zext, F32),
                pltpu.VMEM((total,) + dims, F32),
                pltpu.VMEM((2,) + ext, F32),
                pltpu.VMEM((2,) + zext, F32),
                pltpu.VMEM((2, 8, 3 * cy, LANES), F32),
                pltpu.VMEM((2, 6 * RUN, 3 * cy, LANES), F32),
                pltpu.VMEM((3 * cx // RUN + 1, cy, LANES), F32),
                pltpu.VMEM((2,) + ext, F32),
                pltpu.VMEM((2,) + ext, F32),
                pltpu.VMEM((LANES, LANES), F32),
                pltpu.VMEM((plane, 1, LANES), F32),
                pltpu.VMEM((counts[0], 1, LANES), F32),
                pltpu.VMEM((4 * 9 * cx * (cy // 4), 4, LANES), F32),
                dma((2,)), dma((1,)),
                dma((1,)), dma((2, 2)),
                dma((1,)), dma((1,)),
                dma((1,)), dma((1,)),
            ],
            compiler_params=pltpu.CompilerParams(collective_id=0, has_side_effects=True, vmem_limit_bytes=24 << 20),
            name="powers_basis",
        )(*[pltpu.with_memory_space_constraint(v, pltpu.HBM) for v in (residual, direction)])
        powers, gram, proj = pl.pallas_call(
            store,
            out_shape=(
                jax.ShapeDtypeStruct((2, STEPS) + dims, F32),
                jax.ShapeDtypeStruct((total, total), F32),
                jax.ShapeDtypeStruct((1, total), F32),
            ),
            in_specs=[vm, vm, vm],
            out_specs=(hbm, hbm, hbm),
            scratch_shapes=[dma((3,))],
            compiler_params=pltpu.CompilerParams(vmem_limit_bytes=1 << 20),
            name="store",
        )(powers, gram, proj)
        return powers, gram, proj.reshape(total)

    placed = (P("gx", "gy", "gz"), P("gx", "gy", "gz"))
    return jax.shard_map(
        local,
        mesh=mesh,
        in_specs=placed,
        out_specs=(P(None, None, "gx", "gy", "gz"), P(), P()),
        check_vma=False,
    )
```

```python
import functools

import jax
import jax.numpy as jnp
from jax import lax
from jax.experimental import pallas as pl
from jax.experimental.pallas import tpu as pltpu
from jax.sharding import PartitionSpec as P

STEPS = 4
LANES = 128
MESH = pl.DeviceIdType.MESH
HIGHEST = lax.Precision.HIGHEST
F32 = jnp.float32
AXES = ("gx", "gy", "gz")
GAMMA, BETA, ALPHA, DELTA = 13.0 / 81.0, 5.0 / 243.0, 1.0 / 729.0, 1.0 / 1458.0
P_CHAIN, Z_CHAIN = 0, 1
REACH = ((7, 6), (6, 6))
CHUNK = 4
RUN = 4
OFFSETS = [(dx, dy, dz) for dx in (-1, 0, 1) for dy in (-1, 0, 1) for dz in (-1, 0, 1) if (dx, dy, dz) != (0, 0, 0)]


def as_f32(flag):
    return jnp.where(flag, 1.0, 0.0).astype(F32)


def axis_terms(at, width, low, high, place, count):
    inside = (place * width + at >= 0) & (place * width + at < count * width)
    cover = ((at == -1) | (at == 0)) & low | ((at == width - 1) | (at == width)) & high
    inner = ((at == -2) | (at == 1)) & low | ((at == width - 2) | (at == width + 1)) & high
    below = (at == 1) & low | (at == width + 1) & high
    above = (at == -2) & low | (at == width - 2) & high
    mask = as_f32(inside)
    return (1.0 + as_f32(cover)) * mask, as_f32(inner), 1.0 - 0.5 * as_f32(below), 1.0 - 0.5 * as_f32(above), mask


def kernel(
    counts, dims, near, res_ref, dir_ref, pow_ref, gram_ref, proj_ref,
    raw, main, pack, got, face, flat, cbuf, czbuf, sbuf, szbuf, image, zsum, zzsum, tab, ztab, half_tab, d_tab, g_tab, t_ref, red0, red1, spare,
    in_sem, out_sem, s_sem, r_sem, s0_sem, r0_sem, s1_sem, r1_sem,
):
    nx, ny, nz = counts
    cx, cy, cz = dims
    group = LANES // cx
    half = group // 2
    rows = 3 * cy
    place = [lax.axis_index(a) for a in AXES]
    gx, gy, gz = place
    low = [place[i] > 0 for i in range(3)]
    high = [place[i] < counts[i] - 1 for i in range(3)]
    total = 2 * STEPS + 1

    def exists(offset):
        ok = None
        for i, step in enumerate(offset):
            if step:
                test = low[i] if step < 0 else high[i]
                ok = test if ok is None else jnp.logical_and(ok, test)
        return ok

    def flip(offset):
        return tuple(-s for s in offset)

    def target(offset):
        return {AXES[i]: place[i] + s for i, s in enumerate(offset) if s}

    def ahead(axes):
        def make(k):
            out = {}
            for a in reversed(axes):
                k, step = divmod(k, counts[AXES.index(a)])
                if step:
                    out[a] = lax.rem(place[AXES.index(a)] + step, counts[AXES.index(a)])
            return out
        size = 1
        for a in axes:
            size *= counts[AXES.index(a)]
        return size, make

    loads = [
        pltpu.make_async_copy(ref, raw.at[c, 0, pl.ds(cx, cx), pl.ds(cy, cy)], in_sem.at[c])
        for c, ref in ((Z_CHAIN, res_ref), (P_CHAIN, dir_ref))
    ]
    for copy in loads:
        copy.start()

    barrier = pltpu.get_barrier_semaphore()
    expected = 0
    far_first = sorted(range(len(OFFSETS)), key=lambda i: -sum(abs(v) for v in OFFSETS[i]))
    for offset in [OFFSETS[i] for i in far_first]:
        @pl.when(exists(offset))
        def _():
            pl.semaphore_signal(barrier, 1, device_id=target(offset), device_id_type=MESH)
        expected = expected + exists(offset).astype(jnp.int32)
    if not near:
        for axes in (("gy", "gz"), ("gx",)):
            size, make = ahead(axes)
            for k in range(1, size):
                pl.semaphore_signal(barrier, 1, device_id=make(k), device_id_type=MESH)
            expected = expected + (size - 1)

    row = lax.broadcasted_iota(jnp.int32, (cy, LANES), 0)
    lane = lax.broadcasted_iota(jnp.int32, (cy, LANES), 1)
    top, bottom = row == 0, row == cy - 1
    runs = 3 * cx // RUN
    slot = (lane + half) // group % cx
    deep = (lane + half) % group - half
    is_hi = deep >= 0
    at_first, at_last = deep == 0, deep == -1
    is_first = [lane == group * g for g in range(runs)]
    is_last = [lane == (group * g - 1) % LANES for g in range(runs)]
    is_edge = [is_first[g] | is_last[g] for g in range(runs)]

    def x_terms(x):
        return axis_terms(jnp.int32(x), cx, low[0], high[0], gx, nx)

    below_1, above_6 = x_terms(1)[2], x_terms(cx - 2)[3]

    def turn(x):
        return group * ((x + cx) // RUN)

    TALL, SHORT = 3, 2
    AM0, M0, UPY, DOWNY = 0, 3, 6, 7
    ZD, ZAM, ZM, ZG, ZUX, ZDX = (RUN * k for k in range(6))

    def fill_tables():
        half_z = 1.0 - 0.5 * (as_f32((lane == 0) & low[2]) + as_f32((lane == LANES - 1) & high[2]))
        for g in range(runs):
            half_tab[g] = roll_lanes(half_z, group * g)
        half_tab[runs] = 1.0 - 0.5 * as_f32(at_first | at_last)
        wz, fz, _, _, mz = axis_terms(lane, cz, low[2], high[2], gz, nz)
        z_at = jnp.where(is_hi, deep + cz, deep)
        wzz, fzz, _, _, mzz = axis_terms(z_at, cz, low[2], high[2], gz, nz)
        along = [axis_terms(slot * RUN + (b - cx), cx, low[0], high[0], gx, nx) for b in range(RUN)]
        for high_rows in (TALL, SHORT):
            t = TALL - high_rows
            for k in range(high_rows):
                ds = pl.ds(k * cy, cy)
                if high_rows == TALL:
                    y = row + (k - 1) * cy
                elif k == 0:
                    y = jnp.where(row < cy // 2, row + cy, row - cy)
                else:
                    y = row
                wy, fy, up_y, down_y, my = axis_terms(y, cy, low[1], high[1], gy, ny)
                wyz, myz, gyz = wy * wz, my * mz, GAMMA + DELTA * (fy + fz)
                for n, x in enumerate((-3, 3, cx + 2)):
                    mask = myz * x_terms(x)[4]
                    tab[t, AM0 + n, ds] = mask * ALPHA
                    tab[t, M0 + n, ds] = mask
                tab[t, UPY, ds], tab[t, DOWNY, ds] = up_y, down_y
                for g in range(runs):
                    d_run, g_run = roll_lanes(wyz, group * g), roll_lanes(gyz, group * g)
                    for n in range(RUN * g, RUN * g + RUN):
                        cover, inner = x_terms(n - cx)[:2]
                        d_tab[t, n, ds] = d_run * cover
                        g_tab[t, n, ds] = g_run + DELTA * inner
                for b in range(RUN):
                    wx, fx, up_x, down_x, mx = along[b]
                    ztab[t, ZD + b, ds] = wx * wy * wzz
                    ztab[t, ZAM + b, ds] = mx * my * mzz * ALPHA
                    ztab[t, ZM + b, ds] = mx * my * mzz
                    ztab[t, ZG + b, ds] = GAMMA + DELTA * (fx + fy + fzz)
                    ztab[t, ZUX + b, ds] = up_x
                    ztab[t, ZDX + b, ds] = down_x

    def fill_zeros():
        fields = [(c, f) for c in (0, 1) for f in (0, 1)]
        for flag, xs, ys in (
            (low[0], pl.ds(0, cx), pl.ds(0, rows)), (high[0], pl.ds(2 * cx, cx), pl.ds(0, rows)),
            (low[1], pl.ds(0, 3 * cx), pl.ds(0, cy)), (high[1], pl.ds(0, 3 * cx), pl.ds(2 * cy, cy)),
        ):
            @pl.when(jnp.logical_not(flag))
            def _():
                for c, f in fields:
                    raw[c, f, xs, ys] = jnp.zeros((xs.size, ys.size, LANES), F32)
        for flag, ss, xs, ys in (
            (low[2], 0, pl.ds(0, 3), pl.ds(0, rows)), (high[2], 1, pl.ds(0, 3), pl.ds(0, rows)),
            (low[0], None, pl.ds(0, 1), pl.ds(0, rows)), (high[0], None, pl.ds(2, 1), pl.ds(0, rows)),
            (low[1], None, pl.ds(0, 3), pl.ds(0, cy)), (high[1], None, pl.ds(0, 3), pl.ds(2 * cy, cy)),
        ):
            @pl.when(jnp.logical_not(flag))
            def _():
                for c in (0, 1):
                    for s in (0, 1):
                        for side in ((0, 1) if ss is None else (ss,)):
                            got[c, s, side, xs, ys] = jnp.zeros((xs.size, ys.size, LANES), F32)

    def roll_rows(v, shift):
        return pltpu.roll(v, shift % v.shape[0], 0)

    def roll_lanes(v, shift):
        shift = shift % LANES
        return v if shift == 0 else pltpu.roll(v, shift, 1)

    def planes(reach):
        xs = list(range(-reach, cx + reach))
        return [xs[i:i + CHUNK] for i in range(0, len(xs), CHUNK)]

    def table(t, at, xs, n):
        ks = [at + (x + cx) // cx for x in xs]
        if len(set(ks)) == 1:
            return tab[t, ks[0], pl.ds(0, n)][None]
        return jnp.stack([tab[t, k, pl.ds(0, n)] for k in ks])

    def spread(v, tiles):
        return jnp.concatenate([v] * tiles, axis=0)

    def wide(mask, tiles):
        return jnp.concatenate([mask] * tiles, axis=0)

    def put(dst, xs, value, reach, tiles):
        for i, x in enumerate(xs):
            if reach > 0 and -reach < x < cx + reach - 1:
                dst[x + cx, pl.ds(0, tiles * cy)] = value[i]
            else:
                dst[x + cx, pl.ds(cy, cy)] = value[i, cy:2 * cy]

    flips = [0]

    def stream(src, z_src, reach, weighted, tiles):
        flips[0] ^= 1
        out, z_out = zsum.at[flips[0]], zzsum.at[flips[0]]
        t, n = TALL - tiles, tiles * cy
        ds = pl.ds(0, n)
        for x in range(-reach, cx + reach):
            g, b = divmod(x + cx, RUN)
            mid, extra = src[x + cx, ds], z_src[b, ds]
            if weighted:
                mid = mid * spread(half_tab[g], tiles)
            up = roll_lanes(jnp.where(wide(is_last[g], tiles), extra, mid), 1)
            down = roll_lanes(jnp.where(wide(is_first[g], tiles), extra, mid), -1)
            part = up + down
            if b == 0:
                part = part + roll_lanes(src[x + cx - 1, ds], group)
            if b == RUN - 1:
                part = part + roll_lanes(src[x + cx + 1, ds], -group)
            put(out, [x], part[None], reach, tiles)
        for b in range(RUN if reach > 0 else 0):
            mid = z_src[b, ds]
            inject = jnp.zeros((n, LANES), F32)
            for g in range(runs):
                x = g * RUN + b - cx
                if -reach <= x < cx + reach:
                    inject = jnp.where(wide(is_edge[g], tiles), src[x + cx, ds], inject)
            if weighted:
                mid = mid * spread(half_tab[runs], tiles)
            part = roll_lanes(jnp.where(wide(at_last, tiles), inject, mid), 1)
            part = part + roll_lanes(jnp.where(wide(at_first, tiles), inject, mid), -1)
            if b == 0:
                before = roll_lanes(z_src[RUN - 1, ds], group)
                part = part + (before * ztab[t, ZUX, ds] if weighted else before)
            if b == RUN - 1:
                after = roll_lanes(z_src[0, ds], -group)
                part = part + (after * ztab[t, ZDX + b, ds] if weighted else after)
            z_out[b, ds] = part
        return out, z_out

    def along_y(parts, weighted, tiles):
        t = TALL - tiles
        ahead_of = [pltpu.roll(v, 1, v.ndim - 2) for v in parts]
        behind = [pltpu.roll(v, cy - 1, v.ndim - 2) for v in parts]
        sums = []
        for k in range(tiles):
            left, right = ahead_of[k], behind[k]
            before = k - 1 if tiles == TALL else 1 - k
            after = k + 1 if tiles == TALL else 1 - k
            if before >= 0:
                left = jnp.where(top, ahead_of[before], left)
            if after < tiles:
                right = jnp.where(bottom, behind[after], right)
            if weighted and not (tiles == TALL and k == 0):
                left = left * tab[t, UPY, pl.ds(k * cy, cy)]
            if weighted and not (tiles == TALL and k == 2):
                right = right * tab[t, DOWNY, pl.ds(k * cy, cy)]
            sums.append(left + right)
        return jnp.concatenate(sums, axis=-2)

    def beside(src, sums, xs, weighted, tiles):
        lo = xs[0] + cx
        ds = pl.ds(0, tiles * cy)
        mid = src[pl.ds(lo, len(xs)), ds]
        parts = []
        for x in xs:
            b = (x + cx) % RUN
            part = sums[x + cx, ds]
            if b > 0:
                value = src[x + cx - 1, ds]
                if weighted and x == 1:
                    value = value * below_1
                if weighted and x == cx + 1:
                    value = value * 0.5
                part = part + value
            if b < RUN - 1:
                value = src[x + cx + 1, ds]
                if weighted and x == cx - 2:
                    value = value * above_6
                if weighted and x == -2:
                    value = value * 0.5
                part = part + value
            columns = [src[x + cx, pl.ds(k * cy, cy)] for k in range(tiles)]
            parts.append(part + along_y(columns, weighted, tiles))
        return mid, jnp.stack(parts)

    def z_beside(z_src, z_sums, b, weighted, tiles):
        t, ds = TALL - tiles, pl.ds(0, tiles * cy)
        around = z_sums[b, ds] + along_y([z_src[b, pl.ds(k * cy, cy)] for k in range(tiles)], weighted, tiles)
        if b > 0:
            value = z_src[b - 1, ds]
            around = around + (value * ztab[t, ZUX + b, ds] if weighted else value)
        if b < RUN - 1:
            value = z_src[b + 1, ds]
            around = around + (value * ztab[t, ZDX + b, ds] if weighted else value)
        return z_src[b, ds], around

    def shorten(v):
        outer = jnp.where(row < cy // 2, v[..., 2 * cy:, :], v[..., :cy, :])
        return jnp.concatenate([outer, v[..., cy:2 * cy, :]], axis=-2)

    def apply_a(c, f, reach, index, tiles):
        t, n = TALL - tiles, tiles * cy
        src, z_src = main.at[c, f], pack.at[c, f]
        sums, z_sums = stream(src, z_src, reach, False, tiles)
        for b in range(RUN if reach > 0 else 0):
            mid, around = z_beside(z_src, z_sums, b, False, tiles)
            czbuf[c, b, pl.ds(0, n)] = (6.0 * mid - around) * ztab[t, ZD + b, pl.ds(0, n)]
        for xs in planes(reach):
            mid, around = beside(src, sums, xs, False, tiles)
            value = 6.0 * mid - around
            for i, x in enumerate(xs):
                if 0 <= x < cx:
                    image[index, x] = value[i, cy:2 * cy]
            ds = pl.ds(xs[0] + cx, len(xs))
            put(cbuf.at[c], xs, value * d_tab[t, ds, pl.ds(0, n)], reach, tiles)

    def apply_m(c, f, reach, tiles):
        t, n = TALL - tiles, tiles * cy
        rows = pl.ds(0, n)
        src, z_src = cbuf.at[c], czbuf.at[c]
        sums, z_sums = stream(src, z_src, reach + 1, True, tiles)
        for b in range(RUN):
            mid, around = z_beside(z_src, z_sums, b, True, tiles)
            szbuf[c, b, rows] = BETA * mid + around * ztab[t, ZAM + b, rows]
        for xs in planes(reach + 1):
            mid, around = beside(src, sums, xs, True, tiles)
            put(sbuf.at[c], xs, BETA * mid + around * table(t, AM0, xs, n), reach + 1, tiles)
        s_src, sz_src = sbuf.at[c], szbuf.at[c]
        sums, z_sums = stream(s_src, sz_src, reach, True, tiles)
        for b in range(RUN if reach > 0 else 0):
            _, around = z_beside(sz_src, z_sums, b, True, tiles)
            value = z_src[b, rows] * ztab[t, ZG + b, rows] + around * ztab[t, ZM + b, rows]
            pack[c, f, b, pl.ds(0, SHORT * cy)] = shorten(value) if tiles == TALL else value
        for xs in planes(reach):
            ds = pl.ds(xs[0] + cx, len(xs))
            _, around = beside(s_src, sums, xs, True, tiles)
            value = src[ds, rows] * g_tab[t, ds, rows]
            if reach > 0:
                value = value + around * table(t, M0, xs, n)
            else:
                value = value + around
            if tiles == TALL:
                value = shorten(value)
            put(main.at[c, f], xs, value, reach, SHORT)

    def parts_of(c, s, index):
        dx, dy, dz = OFFSETS[index]
        reach = REACH[s][c]
        if dz:
            return [(0, 1, cy // 2 if dx and dy and reach - 2 <= cy // 2 else cy)]
        if dx == 0:
            return [(0, cx, cy)]
        if dy == 0:
            return [(0, reach, cy)]
        full = max(0, reach - cy // 2 - 1)
        return [p for p in ((0, full, cy), (full, reach - 1 - full, cy // 2)) if p[1] > 0]

    def copy_to(c, s, index, part):
        dx, dy, dz = OFFSETS[index]
        if dz == 0:
            skip, n, h = part
            first = cx + skip if dx <= 0 else 2 * cx - skip - n
            here = pl.ds(cy if dy <= 0 else 2 * cy - h, h)
            there = pl.ds(here.start - cy * dy, h)
            source = raw.at[c, s, pl.ds(first, n), here]
            sink = raw.at[c, s, pl.ds(first - cx * dx, n), there]
        else:
            skip, n, h = part
            here = pl.ds(0 if dy <= 0 else cy - h, h)
            source = face.at[c, s, here]
            sink = got.at[c, s, 0 if dz > 0 else 1, 1 - dx, pl.ds(here.start + cy - cy * dy, h)]
        return pltpu.make_async_remote_copy(
            source, sink, s_sem.at[0], r_sem.at[c, s],
            device_id=target(OFFSETS[index]), device_id_type=MESH)

    per_block = cx // RUN

    def pack_face(c, s, source):
        value = jnp.zeros((cy, LANES), F32)
        for i in range(RUN):
            joined = source(i)
            for h in range(1, per_block):
                other = source(h * RUN + i)
                joined = jnp.where(slot == per_block + h, other, joined)
            moved = roll_lanes(joined, group * (per_block * i - per_block))
            value = jnp.where(slot // per_block == i, moved, value)
        face[c, s] = value

    def turn_own(c):
        for x in range(cx):
            main[c, 0, x + cx, pl.ds(cy, cy)] = roll_lanes(raw[c, 0, x + cx, pl.ds(cy, cy)], turn(x))

    def turn_back(source, out):
        for x in range(cx):
            out[x] = roll_lanes(source(x), -turn(x))

    def send(c, s):
        for index in far_first:
            @pl.when(exists(OFFSETS[index]))
            def _():
                for part in parts_of(c, s, index):
                    copy_to(c, s, index, part).start()

    around_it = [low[i].astype(jnp.int32) + high[i].astype(jnp.int32) for i in range(3)]
    choices = [{1: (0,), 2: (1,)}.get(n, (1, 2)) for n in counts]

    def tiles_of(c, s, ax, ay, az):
        sizes = {o: sum(n * h for _, n, h in parts_of(c, s, i)) for i, o in enumerate(OFFSETS)}
        in_rows = ax * sizes[1, 0, 0] + ay * sizes[0, 1, 0] + ax * ay * sizes[1, 1, 0]
        in_rows += az * (sizes[0, 0, 1] + ax * sizes[1, 0, 1] + ay * sizes[0, 1, 1] + ax * ay * sizes[1, 1, 1])
        return in_rows // 4

    def wait_bytes(sem, tiles):
        view = spare.at[pl.ds(0, tiles)]
        pltpu.make_async_copy(view, view, sem).wait()

    def wait_exchanges(sem, pairs):
        for ax in choices[0]:
            for ay in choices[1]:
                for az in choices[2]:
                    here = (around_it[0] == ax) & (around_it[1] == ay) & (around_it[2] == az)
                    tiles = sum(tiles_of(c, s, ax, ay, az) for c, s in pairs)
                    if tiles:
                        @pl.when(here)
                        def _():
                            wait_bytes(sem, tiles)

    def receive(c, s):
        wait_exchanges(r_sem.at[c, s], [(c, s)])
        scaled = s == 1 or c == Z_CHAIN
        into, z_into = (cbuf.at[c], czbuf.at[c]) if scaled else (main.at[c, 0], pack.at[c, 0])
        hi, at_block = wide(is_hi, TALL), [wide(slot // per_block == k, TALL) for k in range(3)]
        faces = [jnp.where(hi, got[c, s, 1, k], got[c, s, 0, k]) for k in range(3)]
        for b in range(RUN):
            value = jnp.zeros((TALL * cy, LANES), F32)
            for k in range(3):
                moved = roll_lanes(faces[k], group * per_block * (k - b))
                value = jnp.where(at_block[k], moved, value)
            z_into[b] = value * ztab[0, ZD + b] if scaled else value
        reach = REACH[s][c]
        for x in range(-reach, cx + reach):
            if 0 <= x < cx:
                ys = [0, 2 * cy]
            elif x in (-reach, cx + reach - 1):
                ys = [cy]
            else:
                ys = [0, cy, 2 * cy]
            for y in ys:
                ds = pl.ds(y, cy)
                value = roll_lanes(raw[c, s, x + cx, ds], turn(x))
                into[x + cx, ds] = value * d_tab[0, x + cx, ds] if scaled else value
            if scaled and s == 0 and 0 <= x < cx:
                ds = pl.ds(cy, cy)
                into[x + cx, ds] = main[c, 0, x + cx, ds] * d_tab[0, x + cx, ds]

    def own(c, f):
        return main[c, f, pl.ds(cx, cx), pl.ds(cy, cy)].reshape(cx * cy, LANES)

    def emit(c, f, slot_out):
        turn_back(lambda x: main[c, f, x + cx, pl.ds(cy, cy)], pow_ref.at[c, slot_out])

    place_of = {a: (P_CHAIN, a) for a in range(STEPS + 1)}
    place_of.update({STEPS + 1 + k: (Z_CHAIN, k + 1) for k in range(STEPS)})
    ready = []

    def account(a):
        ready.append(a)
        picture = image[a].reshape(cx * cy, LANES)
        for b in ready:
            part = jnp.sum(own(*place_of[b]) * picture, axis=0, keepdims=True)
            t_ref[pl.ds(a * total + b, 1), :] = part
            if a != b:
                t_ref[pl.ds(b * total + a, 1), :] = part
        t_ref[pl.ds(total * total + a, 1), :] = jnp.sum(
            own(*place_of[a]) * own(Z_CHAIN, 0), axis=0, keepdims=True)

    for copy in loads:
        copy.wait()
    for c in (Z_CHAIN, P_CHAIN):
        value = jnp.zeros((cy, LANES), F32)
        for x in range(cx):
            at = per_block * (x % RUN) + x // RUN
            value = jnp.where(slot == at, roll_lanes(raw[c, 0, x + cx, pl.ds(cy, cy)], group * at), value)
        face[c, 0] = value
    pl.semaphore_wait(barrier, expected)
    for c in (Z_CHAIN, P_CHAIN):
        send(c, 0)
    for c in (Z_CHAIN, P_CHAIN):
        turn_own(c)
    fill_zeros()
    fill_tables()
    t_ref[...] = jnp.zeros_like(t_ref)

    def finish_first(c, index):
        turn_back(lambda x: image[index, x], raw.at[c, 1, pl.ds(cx, cx), pl.ds(cy, cy)])
        pack_face(c, 1, lambda x: image[index, x])
        send(c, 1)

    first_z = STEPS + 1
    receive(Z_CHAIN, 0)
    apply_m(Z_CHAIN, 1, 4, TALL)
    apply_a(Z_CHAIN, 1, 3, first_z, SHORT)
    apply_m(Z_CHAIN, 2, 1, SHORT)
    apply_a(Z_CHAIN, 2, 0, first_z + 1, SHORT)
    finish_first(Z_CHAIN, first_z + 1)

    receive(P_CHAIN, 0)
    apply_a(P_CHAIN, 0, 6, 0, TALL)
    apply_m(P_CHAIN, 1, 4, TALL)
    apply_a(P_CHAIN, 1, 3, 1, SHORT)
    apply_m(P_CHAIN, 2, 1, SHORT)
    apply_a(P_CHAIN, 2, 0, 2, SHORT)
    finish_first(P_CHAIN, 2)
    for c in (Z_CHAIN, P_CHAIN):
        emit(c, 1, 0)
        emit(c, 2, 1)
    for a in (0, 1, 2, first_z, first_z + 1):
        account(a)

    receive(Z_CHAIN, 1)
    apply_m(Z_CHAIN, 3, 4, TALL)
    apply_a(Z_CHAIN, 3, 3, first_z + 2, SHORT)
    apply_m(Z_CHAIN, 4, 1, SHORT)
    apply_a(Z_CHAIN, 4, 0, first_z + 3, SHORT)
    for k in (2, 3):
        account(first_z + k)
    for k in (3, 4):
        emit(Z_CHAIN, k, k - 1)

    receive(P_CHAIN, 1)
    apply_m(P_CHAIN, 3, 4, TALL)
    emit(P_CHAIN, 3, 2)
    apply_a(P_CHAIN, 3, 3, 3, SHORT)
    account(3)
    apply_m(P_CHAIN, 4, 1, SHORT)
    emit(P_CHAIN, 4, 3)
    apply_a(P_CHAIN, 4, 0, 4, SHORT)
    account(4)

    value = lax.dot_general(
        jnp.ones((8, LANES), F32), t_ref[...], (((1,), (1,)), ((), ())),
        precision=HIGHEST, preferred_element_type=F32)[0:1]

    def far_order(size, axes):
        def hops(k):
            far = 0
            for a in reversed(axes):
                n = counts[AXES.index(a)]
                k, step = divmod(k, n)
                far += min(step, n - step)
            return -far
        return sorted(range(1, size), key=hops)

    def gather(value, axes, buffer, send_sem, recv_sem, meanwhile=lambda: None):
        size, make = ahead(axes)
        buffer[0] = value

        def copy(k):
            return pltpu.make_async_remote_copy(
                buffer.at[0], buffer.at[k], send_sem.at[0], recv_sem.at[0],
                device_id=make(k), device_id_type=MESH)

        for k in far_order(size, axes):
            copy(k).start()
        meanwhile()
        rest = buffer.at[pl.ds(1, size - 1)]
        pltpu.make_async_copy(rest, rest, send_sem.at[0]).wait()
        pltpu.make_async_copy(rest, rest, recv_sem.at[0]).wait()
        result = jnp.zeros_like(value)
        for k in range(size):
            rest, at = k, 0
            scale = 1
            for a in reversed(axes):
                n = counts[AXES.index(a)]
                rest, want = divmod(rest, n)
                at = at + scale * lax.rem(place[AXES.index(a)] + n - want, n)
                scale *= n
            result = result + buffer[at]
        return result

    def finish():
        wait_exchanges(s_sem.at[0], [(c, s) for c in (0, 1) for s in (0, 1)])

    if near:
        value = gather(value, AXES, red0, s0_sem, r0_sem, finish)
    else:
        value = gather(value, ("gy", "gz"), red0, s0_sem, r0_sem, finish)
        value = gather(value, ("gx",), red1, s1_sem, r1_sem)
    value = value * (1.0 / (nx * cx * ny * cy * nz * cz))
    for a in range(total):
        gram_ref[a:a + 1, :] = value[0:1, a * total:(a + 1) * total]
    proj_ref[...] = value[0:1, total * total:total * total + total]


def store(pow_ref, gram_ref, proj_ref, pow_out, gram_out, proj_out, sem):
    pairs = ((pow_ref, pow_out), (gram_ref, gram_out), (proj_ref, proj_out))
    copies = [pltpu.make_async_copy(a, b, sem.at[i]) for i, (a, b) in enumerate(pairs)]
    for copy in copies:
        copy.start()
    for copy in copies:
        copy.wait()


def solution(mesh):
    counts = tuple(mesh.shape[a] for a in AXES)
    near = max(counts) <= 4
    devices = counts[0] * counts[1] * counts[2]
    plane = devices if near else counts[1] * counts[2]

    def local(residual, direction):
        dims = residual.shape
        cx, cy, cz = dims
        assert cz == LANES and LANES % cx == 0 and cy % 8 == 0
        assert min(cx, cy, LANES // cx // 2) > max(max(r) for r in REACH)
        total = 2 * STEPS + 1
        fields = STEPS + 1
        dma = pltpu.SemaphoreType.DMA
        vm = pl.BlockSpec(memory_space=pltpu.VMEM)
        hbm = pl.BlockSpec(memory_space=pltpu.HBM)
        ext = (3 * cx, 3 * cy, LANES)
        zext = (RUN, 3 * cy, LANES)
        powers, gram, proj = pl.pallas_call(
            functools.partial(kernel, counts, dims, near),
            out_shape=(
                jax.ShapeDtypeStruct((2, STEPS) + dims, F32),
                jax.ShapeDtypeStruct((total, total), F32),
                jax.ShapeDtypeStruct((1, total), F32),
            ),
            in_specs=[hbm, hbm],
            out_specs=(vm, vm, vm),
            scratch_shapes=[
                pltpu.VMEM((2, 2) + ext, F32),
                pltpu.VMEM((2, fields) + ext, F32),
                pltpu.VMEM((2, fields) + zext, F32),
                pltpu.VMEM((2, 2, 2, 3, 3 * cy, LANES), F32),
                pltpu.VMEM((2, 2, cy, LANES), F32),
                pltpu.VMEM((2, STEPS) + dims, F32),
                pltpu.VMEM((2,) + ext, F32),
                pltpu.VMEM((2,) + zext, F32),
                pltpu.VMEM((2,) + ext, F32),
                pltpu.VMEM((2,) + zext, F32),
                pltpu.VMEM((total,) + dims, F32),
                pltpu.VMEM((2,) + ext, F32),
                pltpu.VMEM((2,) + zext, F32),
                pltpu.VMEM((2, 8, 3 * cy, LANES), F32),
                pltpu.VMEM((2, 6 * RUN, 3 * cy, LANES), F32),
                pltpu.VMEM((3 * cx // RUN + 1, cy, LANES), F32),
                pltpu.VMEM((2,) + ext, F32),
                pltpu.VMEM((2,) + ext, F32),
                pltpu.VMEM((LANES, LANES), F32),
                pltpu.VMEM((plane, 1, LANES), F32),
                pltpu.VMEM((counts[0], 1, LANES), F32),
                pltpu.VMEM((4 * 9 * cx * (cy // 4), 4, LANES), F32),
                dma((2,)), dma((1,)),
                dma((1,)), dma((2, 2)),
                dma((1,)), dma((1,)),
                dma((1,)), dma((1,)),
            ],
            compiler_params=pltpu.CompilerParams(collective_id=0, has_side_effects=True, vmem_limit_bytes=24 << 20),
            name="powers_basis",
        )(*[pltpu.with_memory_space_constraint(v, pltpu.HBM) for v in (residual, direction)])
        powers, gram, proj = pl.pallas_call(
            store,
            out_shape=(
                jax.ShapeDtypeStruct((2, STEPS) + dims, F32),
                jax.ShapeDtypeStruct((total, total), F32),
                jax.ShapeDtypeStruct((1, total), F32),
            ),
            in_specs=[vm, vm, vm],
            out_specs=(hbm, hbm, hbm),
            scratch_shapes=[dma((3,))],
            compiler_params=pltpu.CompilerParams(vmem_limit_bytes=1 << 20),
            name="store",
        )(powers, gram, proj)
        return powers, gram, proj.reshape(total)

    placed = (P("gx", "gy", "gz"), P("gx", "gy", "gz"))
    return jax.shard_map(
        local,
        mesh=mesh,
        in_specs=placed,
        out_specs=(P(None, None, "gx", "gy", "gz"), P(), P()),
        check_vma=False,
    )
```

```python
import functools

import jax
import jax.numpy as jnp
from jax import lax
from jax.experimental import pallas as pl
from jax.experimental.pallas import tpu as pltpu
from jax.sharding import PartitionSpec as P

STEPS = 4
LANES = 128
MESH = pl.DeviceIdType.MESH
HIGHEST = lax.Precision.HIGHEST
F32 = jnp.float32
AXES = ("gx", "gy", "gz")
GAMMA, BETA, ALPHA, DELTA = 13.0 / 81.0, 5.0 / 243.0, 1.0 / 729.0, 1.0 / 1458.0
P_CHAIN, Z_CHAIN = 0, 1
REACH = ((7, 5), (6, 7))
CHUNK = 4
RUN = 4
OFFSETS = [(dx, dy, dz) for dx in (-1, 0, 1) for dy in (-1, 0, 1) for dz in (-1, 0, 1) if (dx, dy, dz) != (0, 0, 0)]


def as_f32(flag):
    return jnp.where(flag, 1.0, 0.0).astype(F32)


def axis_terms(at, width, low, high, place, count):
    inside = (place * width + at >= 0) & (place * width + at < count * width)
    cover = ((at == -1) | (at == 0)) & low | ((at == width - 1) | (at == width)) & high
    inner = ((at == -2) | (at == 1)) & low | ((at == width - 2) | (at == width + 1)) & high
    below = (at == 1) & low | (at == width + 1) & high
    above = (at == -2) & low | (at == width - 2) & high
    mask = as_f32(inside)
    return (1.0 + as_f32(cover)) * mask, as_f32(inner), 1.0 - 0.5 * as_f32(below), 1.0 - 0.5 * as_f32(above), mask


def kernel(
    counts, dims, near, res_ref, dir_ref, pow_ref, gram_ref, proj_ref,
    raw, main, pack, got, face, flat, cbuf, czbuf, sbuf, szbuf, image, zsum, zzsum, tab, ztab, half_tab, d_tab, g_tab, t_ref, red0, red1, spare,
    in_sem, out_sem, s_sem, r_sem, s0_sem, r0_sem, s1_sem, r1_sem,
):
    nx, ny, nz = counts
    cx, cy, cz = dims
    group = LANES // cx
    half = group // 2
    rows = 3 * cy
    place = [lax.axis_index(a) for a in AXES]
    gx, gy, gz = place
    low = [place[i] > 0 for i in range(3)]
    high = [place[i] < counts[i] - 1 for i in range(3)]
    total = 2 * STEPS + 1

    def exists(offset):
        ok = None
        for i, step in enumerate(offset):
            if step:
                test = low[i] if step < 0 else high[i]
                ok = test if ok is None else jnp.logical_and(ok, test)
        return ok

    def flip(offset):
        return tuple(-s for s in offset)

    def target(offset):
        return {AXES[i]: place[i] + s for i, s in enumerate(offset) if s}

    def ahead(axes):
        def make(k):
            out = {}
            for a in reversed(axes):
                k, step = divmod(k, counts[AXES.index(a)])
                if step:
                    out[a] = lax.rem(place[AXES.index(a)] + step, counts[AXES.index(a)])
            return out
        size = 1
        for a in axes:
            size *= counts[AXES.index(a)]
        return size, make

    loads = [
        pltpu.make_async_copy(ref, raw.at[c, 0, pl.ds(cx, cx), pl.ds(cy, cy)], in_sem.at[c])
        for c, ref in ((Z_CHAIN, res_ref), (P_CHAIN, dir_ref))
    ]
    for copy in loads:
        copy.start()

    barrier = pltpu.get_barrier_semaphore()
    expected = 0
    far_first = sorted(range(len(OFFSETS)), key=lambda i: -sum(abs(v) for v in OFFSETS[i]))
    for offset in [OFFSETS[i] for i in far_first]:
        @pl.when(exists(offset))
        def _():
            pl.semaphore_signal(barrier, 1, device_id=target(offset), device_id_type=MESH)
        expected = expected + exists(offset).astype(jnp.int32)
    if not near:
        for axes in (("gy", "gz"), ("gx",)):
            size, make = ahead(axes)
            for k in range(1, size):
                pl.semaphore_signal(barrier, 1, device_id=make(k), device_id_type=MESH)
            expected = expected + (size - 1)

    row = lax.broadcasted_iota(jnp.int32, (cy, LANES), 0)
    lane = lax.broadcasted_iota(jnp.int32, (cy, LANES), 1)
    top, bottom = row == 0, row == cy - 1
    runs = 3 * cx // RUN
    slot = (lane + half) // group % cx
    deep = (lane + half) % group - half
    is_hi = deep >= 0
    at_first, at_last = deep == 0, deep == -1
    is_first = [lane == group * g for g in range(runs)]
    is_last = [lane == (group * g - 1) % LANES for g in range(runs)]
    is_edge = [is_first[g] | is_last[g] for g in range(runs)]

    def x_terms(x):
        return axis_terms(jnp.int32(x), cx, low[0], high[0], gx, nx)

    below_1, above_6 = x_terms(1)[2], x_terms(cx - 2)[3]

    def turn(x):
        return group * ((x + cx) // RUN)

    TALL, SHORT = 3, 2
    AM0, M0, UPY, DOWNY = 0, 3, 6, 7
    ZD, ZAM, ZM, ZG, ZUX, ZDX = (RUN * k for k in range(6))

    def fill_tables():
        half_z = 1.0 - 0.5 * (as_f32((lane == 0) & low[2]) + as_f32((lane == LANES - 1) & high[2]))
        for g in range(runs):
            half_tab[g] = roll_lanes(half_z, group * g)
        half_tab[runs] = 1.0 - 0.5 * as_f32(at_first | at_last)
        wz, fz, _, _, mz = axis_terms(lane, cz, low[2], high[2], gz, nz)
        z_at = jnp.where(is_hi, deep + cz, deep)
        wzz, fzz, _, _, mzz = axis_terms(z_at, cz, low[2], high[2], gz, nz)
        along = [axis_terms(slot * RUN + (b - cx), cx, low[0], high[0], gx, nx) for b in range(RUN)]
        for high_rows in (TALL, SHORT):
            t = TALL - high_rows
            for k in range(high_rows):
                ds = pl.ds(k * cy, cy)
                if high_rows == TALL:
                    y = row + (k - 1) * cy
                elif k == 0:
                    y = jnp.where(row < cy // 2, row + cy, row - cy)
                else:
                    y = row
                wy, fy, up_y, down_y, my = axis_terms(y, cy, low[1], high[1], gy, ny)
                wyz, myz, gyz = wy * wz, my * mz, GAMMA + DELTA * (fy + fz)
                for n, x in enumerate((-3, 3, cx + 2)):
                    mask = myz * x_terms(x)[4]
                    tab[t, AM0 + n, ds] = mask * ALPHA
                    tab[t, M0 + n, ds] = mask
                tab[t, UPY, ds], tab[t, DOWNY, ds] = up_y, down_y
                for g in range(runs):
                    d_run, g_run = roll_lanes(wyz, group * g), roll_lanes(gyz, group * g)
                    for n in range(RUN * g, RUN * g + RUN):
                        cover, inner = x_terms(n - cx)[:2]
                        d_tab[t, n, ds] = d_run * cover
                        g_tab[t, n, ds] = g_run + DELTA * inner
                for b in range(RUN):
                    wx, fx, up_x, down_x, mx = along[b]
                    ztab[t, ZD + b, ds] = wx * wy * wzz
                    ztab[t, ZAM + b, ds] = mx * my * mzz * ALPHA
                    ztab[t, ZM + b, ds] = mx * my * mzz
                    ztab[t, ZG + b, ds] = GAMMA + DELTA * (fx + fy + fzz)
                    ztab[t, ZUX + b, ds] = up_x
                    ztab[t, ZDX + b, ds] = down_x

    def fill_zeros():
        fields = [(c, f) for c in (0, 1) for f in (0, 1)]
        for flag, xs, ys in (
            (low[0], pl.ds(0, cx), pl.ds(0, rows)), (high[0], pl.ds(2 * cx, cx), pl.ds(0, rows)),
            (low[1], pl.ds(0, 3 * cx), pl.ds(0, cy)), (high[1], pl.ds(0, 3 * cx), pl.ds(2 * cy, cy)),
        ):
            @pl.when(jnp.logical_not(flag))
            def _():
                for c, f in fields:
                    raw[c, f, xs, ys] = jnp.zeros((xs.size, ys.size, LANES), F32)
        for flag, ss, xs, ys in (
            (low[2], 0, pl.ds(0, 3), pl.ds(0, rows)), (high[2], 1, pl.ds(0, 3), pl.ds(0, rows)),
            (low[0], None, pl.ds(0, 1), pl.ds(0, rows)), (high[0], None, pl.ds(2, 1), pl.ds(0, rows)),
            (low[1], None, pl.ds(0, 3), pl.ds(0, cy)), (high[1], None, pl.ds(0, 3), pl.ds(2 * cy, cy)),
        ):
            @pl.when(jnp.logical_not(flag))
            def _():
                for c in (0, 1):
                    for s in (0, 1):
                        for side in ((0, 1) if ss is None else (ss,)):
                            got[c, s, side, xs, ys] = jnp.zeros((xs.size, ys.size, LANES), F32)

    def roll_rows(v, shift):
        return pltpu.roll(v, shift % v.shape[0], 0)

    def roll_lanes(v, shift):
        shift = shift % LANES
        return v if shift == 0 else pltpu.roll(v, shift, 1)

    def planes(reach):
        xs = list(range(-reach, cx + reach))
        return [xs[i:i + CHUNK] for i in range(0, len(xs), CHUNK)]

    def table(t, at, xs, n):
        ks = [at + (x + cx) // cx for x in xs]
        if len(set(ks)) == 1:
            return tab[t, ks[0], pl.ds(0, n)][None]
        return jnp.stack([tab[t, k, pl.ds(0, n)] for k in ks])

    def spread(v, tiles):
        return jnp.concatenate([v] * tiles, axis=0)

    def wide(mask, tiles):
        return jnp.concatenate([mask] * tiles, axis=0)

    def put(dst, xs, value, reach, tiles):
        for i, x in enumerate(xs):
            if reach > 0 and -reach < x < cx + reach - 1:
                dst[x + cx, pl.ds(0, tiles * cy)] = value[i]
            else:
                dst[x + cx, pl.ds(cy, cy)] = value[i, cy:2 * cy]

    flips = [0]

    def stream(src, z_src, reach, weighted, tiles):
        flips[0] ^= 1
        out, z_out = zsum.at[flips[0]], zzsum.at[flips[0]]
        t, n = TALL - tiles, tiles * cy
        ds = pl.ds(0, n)
        for x in range(-reach, cx + reach):
            g, b = divmod(x + cx, RUN)
            mid, extra = src[x + cx, ds], z_src[b, ds]
            if weighted:
                mid = mid * spread(half_tab[g], tiles)
            up = roll_lanes(jnp.where(wide(is_last[g], tiles), extra, mid), 1)
            down = roll_lanes(jnp.where(wide(is_first[g], tiles), extra, mid), -1)
            part = up + down
            if b == 0:
                part = part + roll_lanes(src[x + cx - 1, ds], group)
            if b == RUN - 1:
                part = part + roll_lanes(src[x + cx + 1, ds], -group)
            put(out, [x], part[None], reach, tiles)
        for b in range(RUN if reach > 0 else 0):
            mid = z_src[b, ds]
            inject = jnp.zeros((n, LANES), F32)
            for g in range(runs):
                x = g * RUN + b - cx
                if -reach <= x < cx + reach:
                    inject = jnp.where(wide(is_edge[g], tiles), src[x + cx, ds], inject)
            if weighted:
                mid = mid * spread(half_tab[runs], tiles)
            part = roll_lanes(jnp.where(wide(at_last, tiles), inject, mid), 1)
            part = part + roll_lanes(jnp.where(wide(at_first, tiles), inject, mid), -1)
            if b == 0:
                before = roll_lanes(z_src[RUN - 1, ds], group)
                part = part + (before * ztab[t, ZUX, ds] if weighted else before)
            if b == RUN - 1:
                after = roll_lanes(z_src[0, ds], -group)
                part = part + (after * ztab[t, ZDX + b, ds] if weighted else after)
            z_out[b, ds] = part
        return out, z_out

    def along_y(parts, weighted, tiles):
        t = TALL - tiles
        ahead_of = [pltpu.roll(v, 1, v.ndim - 2) for v in parts]
        behind = [pltpu.roll(v, cy - 1, v.ndim - 2) for v in parts]
        sums = []
        for k in range(tiles):
            left, right = ahead_of[k], behind[k]
            before = k - 1 if tiles == TALL else 1 - k
            after = k + 1 if tiles == TALL else 1 - k
            if before >= 0:
                left = jnp.where(top, ahead_of[before], left)
            if after < tiles:
                right = jnp.where(bottom, behind[after], right)
            if weighted and not (tiles == TALL and k == 0):
                left = left * tab[t, UPY, pl.ds(k * cy, cy)]
            if weighted and not (tiles == TALL and k == 2):
                right = right * tab[t, DOWNY, pl.ds(k * cy, cy)]
            sums.append(left + right)
        return jnp.concatenate(sums, axis=-2)

    def beside(src, sums, xs, weighted, tiles):
        lo = xs[0] + cx
        ds = pl.ds(0, tiles * cy)
        mid = src[pl.ds(lo, len(xs)), ds]
        parts = []
        for x in xs:
            b = (x + cx) % RUN
            part = sums[x + cx, ds]
            if b > 0:
                value = src[x + cx - 1, ds]
                if weighted and x == 1:
                    value = value * below_1
                if weighted and x == cx + 1:
                    value = value * 0.5
                part = part + value
            if b < RUN - 1:
                value = src[x + cx + 1, ds]
                if weighted and x == cx - 2:
                    value = value * above_6
                if weighted and x == -2:
                    value = value * 0.5
                part = part + value
            columns = [src[x + cx, pl.ds(k * cy, cy)] for k in range(tiles)]
            parts.append(part + along_y(columns, weighted, tiles))
        return mid, jnp.stack(parts)

    def z_beside(z_src, z_sums, b, weighted, tiles):
        t, ds = TALL - tiles, pl.ds(0, tiles * cy)
        around = z_sums[b, ds] + along_y([z_src[b, pl.ds(k * cy, cy)] for k in range(tiles)], weighted, tiles)
        if b > 0:
            value = z_src[b - 1, ds]
            around = around + (value * ztab[t, ZUX + b, ds] if weighted else value)
        if b < RUN - 1:
            value = z_src[b + 1, ds]
            around = around + (value * ztab[t, ZDX + b, ds] if weighted else value)
        return z_src[b, ds], around

    def shorten(v):
        outer = jnp.where(row < cy // 2, v[..., 2 * cy:, :], v[..., :cy, :])
        return jnp.concatenate([outer, v[..., cy:2 * cy, :]], axis=-2)

    def apply_a(c, f, reach, index, tiles):
        t, n = TALL - tiles, tiles * cy
        src, z_src = main.at[c, f], pack.at[c, f]
        sums, z_sums = stream(src, z_src, reach, False, tiles)
        for b in range(RUN if reach > 0 else 0):
            mid, around = z_beside(z_src, z_sums, b, False, tiles)
            czbuf[c, b, pl.ds(0, n)] = (6.0 * mid - around) * ztab[t, ZD + b, pl.ds(0, n)]
        for xs in planes(reach):
            mid, around = beside(src, sums, xs, False, tiles)
            value = 6.0 * mid - around
            for i, x in enumerate(xs):
                if 0 <= x < cx:
                    image[index, x] = value[i, cy:2 * cy]
            ds = pl.ds(xs[0] + cx, len(xs))
            put(cbuf.at[c], xs, value * d_tab[t, ds, pl.ds(0, n)], reach, tiles)

    def apply_m(c, f, reach, tiles):
        t, n = TALL - tiles, tiles * cy
        rows = pl.ds(0, n)
        src, z_src = cbuf.at[c], czbuf.at[c]
        sums, z_sums = stream(src, z_src, reach + 1, True, tiles)
        for b in range(RUN):
            mid, around = z_beside(z_src, z_sums, b, True, tiles)
            szbuf[c, b, rows] = BETA * mid + around * ztab[t, ZAM + b, rows]
        for xs in planes(reach + 1):
            mid, around = beside(src, sums, xs, True, tiles)
            put(sbuf.at[c], xs, BETA * mid + around * table(t, AM0, xs, n), reach + 1, tiles)
        s_src, sz_src = sbuf.at[c], szbuf.at[c]
        sums, z_sums = stream(s_src, sz_src, reach, True, tiles)
        for b in range(RUN if reach > 0 else 0):
            _, around = z_beside(sz_src, z_sums, b, True, tiles)
            value = z_src[b, rows] * ztab[t, ZG + b, rows] + around * ztab[t, ZM + b, rows]
            pack[c, f, b, pl.ds(0, SHORT * cy)] = shorten(value) if tiles == TALL else value
        for xs in planes(reach):
            ds = pl.ds(xs[0] + cx, len(xs))
            _, around = beside(s_src, sums, xs, True, tiles)
            value = src[ds, rows] * g_tab[t, ds, rows]
            if reach > 0:
                value = value + around * table(t, M0, xs, n)
            else:
                value = value + around
            if tiles == TALL:
                value = shorten(value)
            put(main.at[c, f], xs, value, reach, SHORT)

    def parts_of(c, s, index):
        dx, dy, dz = OFFSETS[index]
        reach = REACH[s][c]
        if dz:
            return [(0, 1, cy // 2 if dx and dy and reach - 2 <= cy // 2 else cy)]
        if dx == 0:
            return [(0, cx, cy)]
        if dy == 0:
            return [(0, reach, cy)]
        full = max(0, reach - cy // 2 - 1)
        return [p for p in ((0, full, cy), (full, reach - 1 - full, cy // 2)) if p[1] > 0]

    def copy_to(c, s, index, part):
        dx, dy, dz = OFFSETS[index]
        if dz == 0:
            skip, n, h = part
            first = cx + skip if dx <= 0 else 2 * cx - skip - n
            here = pl.ds(cy if dy <= 0 else 2 * cy - h, h)
            there = pl.ds(here.start - cy * dy, h)
            source = raw.at[c, s, pl.ds(first, n), here]
            sink = raw.at[c, s, pl.ds(first - cx * dx, n), there]
        else:
            skip, n, h = part
            here = pl.ds(0 if dy <= 0 else cy - h, h)
            source = face.at[c, s, here]
            sink = got.at[c, s, 0 if dz > 0 else 1, 1 - dx, pl.ds(here.start + cy - cy * dy, h)]
        return pltpu.make_async_remote_copy(
            source, sink, s_sem.at[0], r_sem.at[c, s],
            device_id=target(OFFSETS[index]), device_id_type=MESH)

    per_block = cx // RUN

    def pack_face(c, s, source):
        value = jnp.zeros((cy, LANES), F32)
        for i in range(RUN):
            joined = source(i)
            for h in range(1, per_block):
                other = source(h * RUN + i)
                joined = jnp.where(slot == per_block + h, other, joined)
            moved = roll_lanes(joined, group * (per_block * i - per_block))
            value = jnp.where(slot // per_block == i, moved, value)
        face[c, s] = value

    def turn_own(c):
        for x in range(cx):
            main[c, 0, x + cx, pl.ds(cy, cy)] = roll_lanes(raw[c, 0, x + cx, pl.ds(cy, cy)], turn(x))

    def turn_back(source, out):
        for x in range(cx):
            out[x] = roll_lanes(source(x), -turn(x))

    def send(c, s):
        for index in far_first:
            @pl.when(exists(OFFSETS[index]))
            def _():
                for part in parts_of(c, s, index):
                    copy_to(c, s, index, part).start()

    around_it = [low[i].astype(jnp.int32) + high[i].astype(jnp.int32) for i in range(3)]
    choices = [{1: (0,), 2: (1,)}.get(n, (1, 2)) for n in counts]

    def tiles_of(c, s, ax, ay, az):
        sizes = {o: sum(n * h for _, n, h in parts_of(c, s, i)) for i, o in enumerate(OFFSETS)}
        in_rows = ax * sizes[1, 0, 0] + ay * sizes[0, 1, 0] + ax * ay * sizes[1, 1, 0]
        in_rows += az * (sizes[0, 0, 1] + ax * sizes[1, 0, 1] + ay * sizes[0, 1, 1] + ax * ay * sizes[1, 1, 1])
        return in_rows // 4

    def wait_bytes(sem, tiles):
        view = spare.at[pl.ds(0, tiles)]
        pltpu.make_async_copy(view, view, sem).wait()

    def wait_exchanges(sem, pairs):
        for ax in choices[0]:
            for ay in choices[1]:
                for az in choices[2]:
                    here = (around_it[0] == ax) & (around_it[1] == ay) & (around_it[2] == az)
                    tiles = sum(tiles_of(c, s, ax, ay, az) for c, s in pairs)
                    if tiles:
                        @pl.when(here)
                        def _():
                            wait_bytes(sem, tiles)

    def receive(c, s):
        wait_exchanges(r_sem.at[c, s], [(c, s)])
        scaled = (s == 1) == (c == P_CHAIN)
        into, z_into = (cbuf.at[c], czbuf.at[c]) if scaled else (main.at[c, 2 * s], pack.at[c, 2 * s])
        hi, at_block = wide(is_hi, TALL), [wide(slot // per_block == k, TALL) for k in range(3)]
        faces = [jnp.where(hi, got[c, s, 1, k], got[c, s, 0, k]) for k in range(3)]
        for b in range(RUN):
            value = jnp.zeros((TALL * cy, LANES), F32)
            for k in range(3):
                moved = roll_lanes(faces[k], group * per_block * (k - b))
                value = jnp.where(at_block[k], moved, value)
            z_into[b] = value * ztab[0, ZD + b] if scaled else value
        reach = REACH[s][c]
        for x in range(-reach, cx + reach):
            if 0 <= x < cx:
                ys = [0, 2 * cy]
            elif x in (-reach, cx + reach - 1):
                ys = [cy]
            else:
                ys = [0, cy, 2 * cy]
            for y in ys:
                ds = pl.ds(y, cy)
                value = roll_lanes(raw[c, s, x + cx, ds], turn(x))
                into[x + cx, ds] = value * d_tab[0, x + cx, ds] if scaled else value
            if scaled and s == 0 and 0 <= x < cx:
                ds = pl.ds(cy, cy)
                into[x + cx, ds] = main[c, 0, x + cx, ds] * d_tab[0, x + cx, ds]

    def own(c, f):
        return main[c, f, pl.ds(cx, cx), pl.ds(cy, cy)].reshape(cx * cy, LANES)

    def emit(c, f, slot_out):
        turn_back(lambda x: main[c, f, x + cx, pl.ds(cy, cy)], pow_ref.at[c, slot_out])

    place_of = {a: (P_CHAIN, a) for a in range(STEPS + 1)}
    place_of.update({STEPS + 1 + k: (Z_CHAIN, k + 1) for k in range(STEPS)})
    ready = []

    def account(a):
        ready.append(a)
        picture = image[a].reshape(cx * cy, LANES)
        for b in ready:
            part = jnp.sum(own(*place_of[b]) * picture, axis=0, keepdims=True)
            t_ref[pl.ds(a * total + b, 1), :] = part
            if a != b:
                t_ref[pl.ds(b * total + a, 1), :] = part
        t_ref[pl.ds(total * total + a, 1), :] = jnp.sum(
            own(*place_of[a]) * own(Z_CHAIN, 0), axis=0, keepdims=True)

    for copy in loads:
        copy.wait()
    for c in (Z_CHAIN, P_CHAIN):
        value = jnp.zeros((cy, LANES), F32)
        for x in range(cx):
            at = per_block * (x % RUN) + x // RUN
            value = jnp.where(slot == at, roll_lanes(raw[c, 0, x + cx, pl.ds(cy, cy)], group * at), value)
        face[c, 0] = value
    pl.semaphore_wait(barrier, expected)
    for c in (Z_CHAIN, P_CHAIN):
        send(c, 0)
    for c in (Z_CHAIN, P_CHAIN):
        turn_own(c)
    fill_zeros()
    fill_tables()
    t_ref[...] = jnp.zeros_like(t_ref)

    def finish_first(c, source):
        turn_back(source, raw.at[c, 1, pl.ds(cx, cx), pl.ds(cy, cy)])
        pack_face(c, 1, source)
        send(c, 1)

    first_z = STEPS + 1
    receive(Z_CHAIN, 0)
    apply_m(Z_CHAIN, 1, 3, TALL)
    apply_a(Z_CHAIN, 1, 2, first_z, SHORT)
    apply_m(Z_CHAIN, 2, 0, SHORT)
    finish_first(Z_CHAIN, lambda x: main[Z_CHAIN, 2, x + cx, pl.ds(cy, cy)])

    receive(P_CHAIN, 0)
    apply_a(P_CHAIN, 0, 6, 0, TALL)
    apply_m(P_CHAIN, 1, 4, TALL)
    apply_a(P_CHAIN, 1, 3, 1, SHORT)
    apply_m(P_CHAIN, 2, 1, SHORT)
    apply_a(P_CHAIN, 2, 0, 2, SHORT)
    finish_first(P_CHAIN, lambda x: image[2, x])
    for c in (Z_CHAIN, P_CHAIN):
        emit(c, 1, 0)
        emit(c, 2, 1)
    for a in (0, 1, 2, first_z):
        account(a)

    receive(Z_CHAIN, 1)
    apply_a(Z_CHAIN, 2, 6, first_z + 1, TALL)
    apply_m(Z_CHAIN, 3, 4, TALL)
    apply_a(Z_CHAIN, 3, 3, first_z + 2, SHORT)
    apply_m(Z_CHAIN, 4, 1, SHORT)
    apply_a(Z_CHAIN, 4, 0, first_z + 3, SHORT)
    for k in (1, 2, 3):
        account(first_z + k)
    for k in (3, 4):
        emit(Z_CHAIN, k, k - 1)

    receive(P_CHAIN, 1)
    apply_m(P_CHAIN, 3, 4, TALL)
    emit(P_CHAIN, 3, 2)
    apply_a(P_CHAIN, 3, 3, 3, SHORT)
    account(3)
    apply_m(P_CHAIN, 4, 1, SHORT)
    emit(P_CHAIN, 4, 3)
    apply_a(P_CHAIN, 4, 0, 4, SHORT)
    account(4)

    value = lax.dot_general(
        jnp.ones((8, LANES), F32), t_ref[...], (((1,), (1,)), ((), ())),
        precision=HIGHEST, preferred_element_type=F32)[0:1]

    def far_order(size, axes):
        def hops(k):
            far = 0
            for a in reversed(axes):
                n = counts[AXES.index(a)]
                k, step = divmod(k, n)
                far += min(step, n - step)
            return -far
        return sorted(range(1, size), key=hops)

    def gather(value, axes, buffer, send_sem, recv_sem, meanwhile=lambda: None):
        size, make = ahead(axes)
        buffer[0] = value

        def copy(k):
            return pltpu.make_async_remote_copy(
                buffer.at[0], buffer.at[k], send_sem.at[0], recv_sem.at[0],
                device_id=make(k), device_id_type=MESH)

        for k in far_order(size, axes):
            copy(k).start()
        meanwhile()
        rest = buffer.at[pl.ds(1, size - 1)]
        pltpu.make_async_copy(rest, rest, send_sem.at[0]).wait()
        pltpu.make_async_copy(rest, rest, recv_sem.at[0]).wait()
        result = jnp.zeros_like(value)
        for k in range(size):
            rest, at = k, 0
            scale = 1
            for a in reversed(axes):
                n = counts[AXES.index(a)]
                rest, want = divmod(rest, n)
                at = at + scale * lax.rem(place[AXES.index(a)] + n - want, n)
                scale *= n
            result = result + buffer[at]
        return result

    def finish():
        wait_exchanges(s_sem.at[0], [(c, s) for c in (0, 1) for s in (0, 1)])

    if near:
        value = gather(value, AXES, red0, s0_sem, r0_sem, finish)
    else:
        value = gather(value, ("gy", "gz"), red0, s0_sem, r0_sem, finish)
        value = gather(value, ("gx",), red1, s1_sem, r1_sem)
    value = value * (1.0 / (nx * cx * ny * cy * nz * cz))
    for a in range(total):
        gram_ref[a:a + 1, :] = value[0:1, a * total:(a + 1) * total]
    proj_ref[...] = value[0:1, total * total:total * total + total]


def store(pow_ref, gram_ref, proj_ref, pow_out, gram_out, proj_out, sem):
    pairs = ((pow_ref, pow_out), (gram_ref, gram_out), (proj_ref, proj_out))
    copies = [pltpu.make_async_copy(a, b, sem.at[i]) for i, (a, b) in enumerate(pairs)]
    for copy in copies:
        copy.start()
    for copy in copies:
        copy.wait()


def solution(mesh):
    counts = tuple(mesh.shape[a] for a in AXES)
    near = max(counts) <= 4
    devices = counts[0] * counts[1] * counts[2]
    plane = devices if near else counts[1] * counts[2]

    def local(residual, direction):
        dims = residual.shape
        cx, cy, cz = dims
        assert cz == LANES and LANES % cx == 0 and cy % 8 == 0
        assert min(cx, cy, LANES // cx // 2) > max(max(r) for r in REACH)
        total = 2 * STEPS + 1
        fields = STEPS + 1
        dma = pltpu.SemaphoreType.DMA
        vm = pl.BlockSpec(memory_space=pltpu.VMEM)
        hbm = pl.BlockSpec(memory_space=pltpu.HBM)
        ext = (3 * cx, 3 * cy, LANES)
        zext = (RUN, 3 * cy, LANES)
        powers, gram, proj = pl.pallas_call(
            functools.partial(kernel, counts, dims, near),
            out_shape=(
                jax.ShapeDtypeStruct((2, STEPS) + dims, F32),
                jax.ShapeDtypeStruct((total, total), F32),
                jax.ShapeDtypeStruct((1, total), F32),
            ),
            in_specs=[hbm, hbm],
            out_specs=(vm, vm, vm),
            scratch_shapes=[
                pltpu.VMEM((2, 2) + ext, F32),
                pltpu.VMEM((2, fields) + ext, F32),
                pltpu.VMEM((2, fields) + zext, F32),
                pltpu.VMEM((2, 2, 2, 3, 3 * cy, LANES), F32),
                pltpu.VMEM((2, 2, cy, LANES), F32),
                pltpu.VMEM((2, STEPS) + dims, F32),
                pltpu.VMEM((2,) + ext, F32),
                pltpu.VMEM((2,) + zext, F32),
                pltpu.VMEM((2,) + ext, F32),
                pltpu.VMEM((2,) + zext, F32),
                pltpu.VMEM((total,) + dims, F32),
                pltpu.VMEM((2,) + ext, F32),
                pltpu.VMEM((2,) + zext, F32),
                pltpu.VMEM((2, 8, 3 * cy, LANES), F32),
                pltpu.VMEM((2, 6 * RUN, 3 * cy, LANES), F32),
                pltpu.VMEM((3 * cx // RUN + 1, cy, LANES), F32),
                pltpu.VMEM((2,) + ext, F32),
                pltpu.VMEM((2,) + ext, F32),
                pltpu.VMEM((LANES, LANES), F32),
                pltpu.VMEM((plane, 1, LANES), F32),
                pltpu.VMEM((counts[0], 1, LANES), F32),
                pltpu.VMEM((4 * 9 * cx * (cy // 4), 4, LANES), F32),
                dma((2,)), dma((1,)),
                dma((1,)), dma((2, 2)),
                dma((1,)), dma((1,)),
                dma((1,)), dma((1,)),
            ],
            compiler_params=pltpu.CompilerParams(collective_id=0, has_side_effects=True, vmem_limit_bytes=24 << 20),
            name="powers_basis",
        )(*[pltpu.with_memory_space_constraint(v, pltpu.HBM) for v in (residual, direction)])
        powers, gram, proj = pl.pallas_call(
            store,
            out_shape=(
                jax.ShapeDtypeStruct((2, STEPS) + dims, F32),
                jax.ShapeDtypeStruct((total, total), F32),
                jax.ShapeDtypeStruct((1, total), F32),
            ),
            in_specs=[vm, vm, vm],
            out_specs=(hbm, hbm, hbm),
            scratch_shapes=[dma((3,))],
            compiler_params=pltpu.CompilerParams(vmem_limit_bytes=1 << 20),
            name="store",
        )(powers, gram, proj)
        return powers, gram, proj.reshape(total)

    placed = (P("gx", "gy", "gz"), P("gx", "gy", "gz"))
    return jax.shard_map(
        local,
        mesh=mesh,
        in_specs=placed,
        out_specs=(P(None, None, "gx", "gy", "gz"), P(), P()),
        check_vma=False,
    )
```

```python
import functools

import jax
import jax.numpy as jnp
from jax import lax
from jax.experimental import pallas as pl
from jax.experimental.pallas import tpu as pltpu
from jax.sharding import PartitionSpec as P

STEPS = 4
LANES = 128
MESH = pl.DeviceIdType.MESH
HIGHEST = lax.Precision.HIGHEST
F32 = jnp.float32
AXES = ("gx", "gy", "gz")
GAMMA, BETA, ALPHA, DELTA = 13.0 / 81.0, 5.0 / 243.0, 1.0 / 729.0, 1.0 / 1458.0
P_CHAIN, Z_CHAIN = 0, 1
REACH = ((7, 5), (6, 7))
CHUNK = 4
RUN = 4
OFFSETS = [(dx, dy, dz) for dx in (-1, 0, 1) for dy in (-1, 0, 1) for dz in (-1, 0, 1) if (dx, dy, dz) != (0, 0, 0)]


def as_f32(flag):
    return jnp.where(flag, 1.0, 0.0).astype(F32)


def axis_terms(at, width, low, high, place, count):
    inside = (place * width + at >= 0) & (place * width + at < count * width)
    cover = ((at == -1) | (at == 0)) & low | ((at == width - 1) | (at == width)) & high
    inner = ((at == -2) | (at == 1)) & low | ((at == width - 2) | (at == width + 1)) & high
    below = (at == 1) & low | (at == width + 1) & high
    above = (at == -2) & low | (at == width - 2) & high
    mask = as_f32(inside)
    return (1.0 + as_f32(cover)) * mask, as_f32(inner), 1.0 - 0.5 * as_f32(below), 1.0 - 0.5 * as_f32(above), mask


def kernel(
    counts, dims, near, res_ref, dir_ref, pow_ref, gram_ref, proj_ref,
    raw, main, pack, got, face, flat, cbuf, czbuf, sbuf, szbuf, image, zsum, zzsum, tab, ztab, half_tab, d_tab, g_tab, t_ref, red0, red1, spare,
    in_sem, out_sem, s_sem, r_sem, s0_sem, r0_sem, s1_sem, r1_sem,
):
    nx, ny, nz = counts
    cx, cy, cz = dims
    group = LANES // cx
    half = group // 2
    rows = 3 * cy
    place = [lax.axis_index(a) for a in AXES]
    gx, gy, gz = place
    low = [place[i] > 0 for i in range(3)]
    high = [place[i] < counts[i] - 1 for i in range(3)]
    total = 2 * STEPS + 1

    def exists(offset):
        ok = None
        for i, step in enumerate(offset):
            if step:
                test = low[i] if step < 0 else high[i]
                ok = test if ok is None else jnp.logical_and(ok, test)
        return ok

    def flip(offset):
        return tuple(-s for s in offset)

    def target(offset):
        return {AXES[i]: place[i] + s for i, s in enumerate(offset) if s}

    def ahead(axes):
        def make(k):
            out = {}
            for a in reversed(axes):
                k, step = divmod(k, counts[AXES.index(a)])
                if step:
                    out[a] = lax.rem(place[AXES.index(a)] + step, counts[AXES.index(a)])
            return out
        size = 1
        for a in axes:
            size *= counts[AXES.index(a)]
        return size, make

    loads = [
        pltpu.make_async_copy(ref, raw.at[c, 0, pl.ds(cx, cx), pl.ds(cy, cy)], in_sem.at[c])
        for c, ref in ((Z_CHAIN, res_ref), (P_CHAIN, dir_ref))
    ]
    for copy in loads:
        copy.start()

    barrier = pltpu.get_barrier_semaphore()
    expected = 0
    far_first = sorted(range(len(OFFSETS)), key=lambda i: -sum(abs(v) for v in OFFSETS[i]))
    for offset in [OFFSETS[i] for i in far_first]:
        @pl.when(exists(offset))
        def _():
            pl.semaphore_signal(barrier, 1, device_id=target(offset), device_id_type=MESH)
        expected = expected + exists(offset).astype(jnp.int32)
    if not near:
        for axes in (("gy", "gz"), ("gx",)):
            size, make = ahead(axes)
            for k in range(1, size):
                pl.semaphore_signal(barrier, 1, device_id=make(k), device_id_type=MESH)
            expected = expected + (size - 1)

    row = lax.broadcasted_iota(jnp.int32, (cy, LANES), 0)
    lane = lax.broadcasted_iota(jnp.int32, (cy, LANES), 1)
    top, bottom = row == 0, row == cy - 1
    runs = 3 * cx // RUN
    slot = (lane + half) // group % cx
    deep = (lane + half) % group - half
    is_hi = deep >= 0
    at_first, at_last = deep == 0, deep == -1
    is_first = [lane == group * g for g in range(runs)]
    is_last = [lane == (group * g - 1) % LANES for g in range(runs)]
    is_edge = [is_first[g] | is_last[g] for g in range(runs)]

    def x_terms(x):
        return axis_terms(jnp.int32(x), cx, low[0], high[0], gx, nx)

    below_1, above_6 = x_terms(1)[2], x_terms(cx - 2)[3]

    def turn(x):
        return group * ((x + cx) // RUN)

    TALL, SHORT = 3, 2
    AM0, M0, UPY, DOWNY = 0, 3, 6, 7
    ZD, ZAM, ZM, ZG, ZUX, ZDX = (RUN * k for k in range(6))

    def fill_tables():
        half_z = 1.0 - 0.5 * (as_f32((lane == 0) & low[2]) + as_f32((lane == LANES - 1) & high[2]))
        for g in range(runs):
            half_tab[g] = roll_lanes(half_z, group * g)
        half_tab[runs] = 1.0 - 0.5 * as_f32(at_first | at_last)
        wz, fz, _, _, mz = axis_terms(lane, cz, low[2], high[2], gz, nz)
        z_at = jnp.where(is_hi, deep + cz, deep)
        wzz, fzz, _, _, mzz = axis_terms(z_at, cz, low[2], high[2], gz, nz)
        along = [axis_terms(slot * RUN + (b - cx), cx, low[0], high[0], gx, nx) for b in range(RUN)]
        for high_rows in (TALL, SHORT):
            t = TALL - high_rows
            for k in range(high_rows):
                ds = pl.ds(k * cy, cy)
                if high_rows == TALL:
                    y = row + (k - 1) * cy
                elif k == 0:
                    y = jnp.where(row < cy // 2, row + cy, row - cy)
                else:
                    y = row
                wy, fy, up_y, down_y, my = axis_terms(y, cy, low[1], high[1], gy, ny)
                wyz, myz, gyz = wy * wz, my * mz, GAMMA + DELTA * (fy + fz)
                for n, x in enumerate((-3, 3, cx + 2)):
                    mask = myz * x_terms(x)[4]
                    tab[t, AM0 + n, ds] = mask * ALPHA
                    tab[t, M0 + n, ds] = mask
                tab[t, UPY, ds], tab[t, DOWNY, ds] = up_y, down_y
                for g in range(runs):
                    d_run, g_run = roll_lanes(wyz, group * g), roll_lanes(gyz, group * g)
                    for n in range(RUN * g, RUN * g + RUN):
                        cover, inner = x_terms(n - cx)[:2]
                        d_tab[t, n, ds] = d_run * cover
                        g_tab[t, n, ds] = g_run + DELTA * inner
                for b in range(RUN):
                    wx, fx, up_x, down_x, mx = along[b]
                    ztab[t, ZD + b, ds] = wx * wy * wzz
                    ztab[t, ZAM + b, ds] = mx * my * mzz * ALPHA
                    ztab[t, ZM + b, ds] = mx * my * mzz
                    ztab[t, ZG + b, ds] = GAMMA + DELTA * (fx + fy + fzz)
                    ztab[t, ZUX + b, ds] = up_x
                    ztab[t, ZDX + b, ds] = down_x

    def fill_zeros():
        fields = [(c, f) for c in (0, 1) for f in (0, 1)]
        for flag, xs, ys in (
            (low[0], pl.ds(0, cx), pl.ds(0, rows)), (high[0], pl.ds(2 * cx, cx), pl.ds(0, rows)),
            (low[1], pl.ds(0, 3 * cx), pl.ds(0, cy)), (high[1], pl.ds(0, 3 * cx), pl.ds(2 * cy, cy)),
        ):
            @pl.when(jnp.logical_not(flag))
            def _():
                for c, f in fields:
                    raw[c, f, xs, ys] = jnp.zeros((xs.size, ys.size, LANES), F32)
        for flag, ss, xs, ys in (
            (low[2], 0, pl.ds(0, 3), pl.ds(0, rows)), (high[2], 1, pl.ds(0, 3), pl.ds(0, rows)),
            (low[0], None, pl.ds(0, 1), pl.ds(0, rows)), (high[0], None, pl.ds(2, 1), pl.ds(0, rows)),
            (low[1], None, pl.ds(0, 3), pl.ds(0, cy)), (high[1], None, pl.ds(0, 3), pl.ds(2 * cy, cy)),
        ):
            @pl.when(jnp.logical_not(flag))
            def _():
                for c in (0, 1):
                    for s in (0, 1):
                        for side in ((0, 1) if ss is None else (ss,)):
                            got[c, s, side, xs, ys] = jnp.zeros((xs.size, ys.size, LANES), F32)

    def roll_rows(v, shift):
        return pltpu.roll(v, shift % v.shape[0], 0)

    def roll_lanes(v, shift):
        shift = shift % LANES
        return v if shift == 0 else pltpu.roll(v, shift, 1)

    def planes(reach):
        xs = list(range(-reach, cx + reach))
        return [xs[i:i + CHUNK] for i in range(0, len(xs), CHUNK)]

    def table(t, at, xs, n):
        ks = [at + (x + cx) // cx for x in xs]
        if len(set(ks)) == 1:
            return tab[t, ks[0], pl.ds(0, n)][None]
        return jnp.stack([tab[t, k, pl.ds(0, n)] for k in ks])

    def spread(v, tiles):
        return jnp.concatenate([v] * tiles, axis=0)

    def wide(mask, tiles):
        return jnp.concatenate([mask] * tiles, axis=0)

    def put(dst, xs, value, reach, tiles):
        for i, x in enumerate(xs):
            if reach > 0 and -reach < x < cx + reach - 1:
                dst[x + cx, pl.ds(0, tiles * cy)] = value[i]
            else:
                dst[x + cx, pl.ds(cy, cy)] = value[i, cy:2 * cy]

    flips = [0]

    def stream(src, z_src, reach, weighted, tiles):
        flips[0] ^= 1
        out, z_out = zsum.at[flips[0]], zzsum.at[flips[0]]
        t, n = TALL - tiles, tiles * cy
        ds = pl.ds(0, n)
        for x in range(-reach, cx + reach):
            g, b = divmod(x + cx, RUN)
            mid, extra = src[x + cx, ds], z_src[b, ds]
            if weighted:
                mid = mid * spread(half_tab[g], tiles)
            up = roll_lanes(jnp.where(wide(is_last[g], tiles), extra, mid), 1)
            down = roll_lanes(jnp.where(wide(is_first[g], tiles), extra, mid), -1)
            part = up + down
            if b == 0:
                part = part + roll_lanes(src[x + cx - 1, ds], group)
            if b == RUN - 1:
                part = part + roll_lanes(src[x + cx + 1, ds], -group)
            put(out, [x], part[None], reach, tiles)
        for b in range(RUN if reach > 0 else 0):
            mid = z_src[b, ds]
            inject = jnp.zeros((n, LANES), F32)
            for g in range(runs):
                x = g * RUN + b - cx
                if -reach <= x < cx + reach:
                    inject = jnp.where(wide(is_edge[g], tiles), src[x + cx, ds], inject)
            if weighted:
                mid = mid * spread(half_tab[runs], tiles)
            part = roll_lanes(jnp.where(wide(at_last, tiles), inject, mid), 1)
            part = part + roll_lanes(jnp.where(wide(at_first, tiles), inject, mid), -1)
            if b == 0:
                before = roll_lanes(z_src[RUN - 1, ds], group)
                part = part + (before * ztab[t, ZUX, ds] if weighted else before)
            if b == RUN - 1:
                after = roll_lanes(z_src[0, ds], -group)
                part = part + (after * ztab[t, ZDX + b, ds] if weighted else after)
            z_out[b, ds] = part
        return out, z_out

    def along_y(parts, weighted, tiles):
        t = TALL - tiles
        ahead_of = [pltpu.roll(v, 1, v.ndim - 2) for v in parts]
        behind = [pltpu.roll(v, cy - 1, v.ndim - 2) for v in parts]
        sums = []
        for k in range(tiles):
            left, right = ahead_of[k], behind[k]
            before = k - 1 if tiles == TALL else 1 - k
            after = k + 1 if tiles == TALL else 1 - k
            if before >= 0:
                left = jnp.where(top, ahead_of[before], left)
            if after < tiles:
                right = jnp.where(bottom, behind[after], right)
            if weighted and not (tiles == TALL and k == 0):
                left = left * tab[t, UPY, pl.ds(k * cy, cy)]
            if weighted and not (tiles == TALL and k == 2):
                right = right * tab[t, DOWNY, pl.ds(k * cy, cy)]
            sums.append(left + right)
        return jnp.concatenate(sums, axis=-2)

    def beside(src, sums, xs, weighted, tiles):
        lo = xs[0] + cx
        ds = pl.ds(0, tiles * cy)
        mid = src[pl.ds(lo, len(xs)), ds]
        parts = []
        for x in xs:
            b = (x + cx) % RUN
            part = sums[x + cx, ds]
            if b > 0:
                value = src[x + cx - 1, ds]
                if weighted and x == 1:
                    value = value * below_1
                if weighted and x == cx + 1:
                    value = value * 0.5
                part = part + value
            if b < RUN - 1:
                value = src[x + cx + 1, ds]
                if weighted and x == cx - 2:
                    value = value * above_6
                if weighted and x == -2:
                    value = value * 0.5
                part = part + value
            columns = [src[x + cx, pl.ds(k * cy, cy)] for k in range(tiles)]
            parts.append(part + along_y(columns, weighted, tiles))
        return mid, jnp.stack(parts)

    def z_beside(z_src, z_sums, b, weighted, tiles):
        t, ds = TALL - tiles, pl.ds(0, tiles * cy)
        around = z_sums[b, ds] + along_y([z_src[b, pl.ds(k * cy, cy)] for k in range(tiles)], weighted, tiles)
        if b > 0:
            value = z_src[b - 1, ds]
            around = around + (value * ztab[t, ZUX + b, ds] if weighted else value)
        if b < RUN - 1:
            value = z_src[b + 1, ds]
            around = around + (value * ztab[t, ZDX + b, ds] if weighted else value)
        return z_src[b, ds], around

    def shorten(v):
        outer = jnp.where(row < cy // 2, v[..., 2 * cy:, :], v[..., :cy, :])
        return jnp.concatenate([outer, v[..., cy:2 * cy, :]], axis=-2)

    def apply_a(c, f, reach, index, tiles):
        t, n = TALL - tiles, tiles * cy
        src, z_src = main.at[c, f], pack.at[c, f]
        sums, z_sums = stream(src, z_src, reach, False, tiles)
        for b in range(RUN if reach > 0 else 0):
            mid, around = z_beside(z_src, z_sums, b, False, tiles)
            czbuf[c, b, pl.ds(0, n)] = (6.0 * mid - around) * ztab[t, ZD + b, pl.ds(0, n)]
        for xs in planes(reach):
            mid, around = beside(src, sums, xs, False, tiles)
            value = 6.0 * mid - around
            for i, x in enumerate(xs):
                if 0 <= x < cx:
                    image[index, x] = value[i, cy:2 * cy]
            ds = pl.ds(xs[0] + cx, len(xs))
            put(cbuf.at[c], xs, value * d_tab[t, ds, pl.ds(0, n)], reach, tiles)

    def apply_m(c, f, reach, tiles):
        t, n = TALL - tiles, tiles * cy
        rows = pl.ds(0, n)
        src, z_src = cbuf.at[c], czbuf.at[c]
        sums, z_sums = stream(src, z_src, reach + 1, True, tiles)
        for b in range(RUN):
            mid, around = z_beside(z_src, z_sums, b, True, tiles)
            szbuf[c, b, rows] = BETA * mid + around * ztab[t, ZAM + b, rows]
        for xs in planes(reach + 1):
            mid, around = beside(src, sums, xs, True, tiles)
            put(sbuf.at[c], xs, BETA * mid + around * table(t, AM0, xs, n), reach + 1, tiles)
        s_src, sz_src = sbuf.at[c], szbuf.at[c]
        sums, z_sums = stream(s_src, sz_src, reach, True, tiles)
        for b in range(RUN if reach > 0 else 0):
            _, around = z_beside(sz_src, z_sums, b, True, tiles)
            value = z_src[b, rows] * ztab[t, ZG + b, rows] + around * ztab[t, ZM + b, rows]
            pack[c, f, b, pl.ds(0, SHORT * cy)] = shorten(value) if tiles == TALL else value
        for xs in planes(reach):
            ds = pl.ds(xs[0] + cx, len(xs))
            _, around = beside(s_src, sums, xs, True, tiles)
            value = src[ds, rows] * g_tab[t, ds, rows]
            if reach > 0:
                value = value + around * table(t, M0, xs, n)
            else:
                value = value + around
            if tiles == TALL:
                value = shorten(value)
            put(main.at[c, f], xs, value, reach, SHORT)

    def parts_of(c, s, index):
        dx, dy, dz = OFFSETS[index]
        reach = REACH[s][c]
        if dz:
            return [(0, 1, cy // 2 if dx and dy and reach - 2 <= cy // 2 else cy)]
        if dx == 0:
            return [(0, cx, cy)]
        if dy == 0:
            return [(0, reach, cy)]
        full = max(0, reach - cy // 2 - 1)
        return [p for p in ((0, full, cy), (full, reach - 1 - full, cy // 2)) if p[1] > 0]

    def copy_to(c, s, index, part):
        dx, dy, dz = OFFSETS[index]
        if dz == 0:
            skip, n, h = part
            first = cx + skip if dx <= 0 else 2 * cx - skip - n
            here = pl.ds(cy if dy <= 0 else 2 * cy - h, h)
            there = pl.ds(here.start - cy * dy, h)
            source = raw.at[c, s, pl.ds(first, n), here]
            sink = raw.at[c, s, pl.ds(first - cx * dx, n), there]
        else:
            skip, n, h = part
            here = pl.ds(0 if dy <= 0 else cy - h, h)
            source = face.at[c, s, here]
            sink = got.at[c, s, 0 if dz > 0 else 1, 1 - dx, pl.ds(here.start + cy - cy * dy, h)]
        return pltpu.make_async_remote_copy(
            source, sink, s_sem.at[0], r_sem.at[c, s],
            device_id=target(OFFSETS[index]), device_id_type=MESH)

    per_block = cx // RUN

    def pack_face(c, s, source):
        value = jnp.zeros((cy, LANES), F32)
        for i in range(RUN):
            joined = source(i)
            for h in range(1, per_block):
                other = source(h * RUN + i)
                joined = jnp.where(slot == per_block + h, other, joined)
            moved = roll_lanes(joined, group * (per_block * i - per_block))
            value = jnp.where(slot // per_block == i, moved, value)
        face[c, s] = value

    def turn_own(c):
        for x in range(cx):
            main[c, 0, x + cx, pl.ds(cy, cy)] = roll_lanes(raw[c, 0, x + cx, pl.ds(cy, cy)], turn(x))

    def turn_back(source, out):
        for x in range(cx):
            out[x] = roll_lanes(source(x), -turn(x))

    def send(c, s):
        for index in far_first:
            @pl.when(exists(OFFSETS[index]))
            def _():
                for part in parts_of(c, s, index):
                    copy_to(c, s, index, part).start()

    around_it = [low[i].astype(jnp.int32) + high[i].astype(jnp.int32) for i in range(3)]
    choices = [{1: (0,), 2: (1,)}.get(n, (1, 2)) for n in counts]

    def tiles_of(c, s, ax, ay, az):
        sizes = {o: sum(n * h for _, n, h in parts_of(c, s, i)) for i, o in enumerate(OFFSETS)}
        in_rows = ax * sizes[1, 0, 0] + ay * sizes[0, 1, 0] + ax * ay * sizes[1, 1, 0]
        in_rows += az * (sizes[0, 0, 1] + ax * sizes[1, 0, 1] + ay * sizes[0, 1, 1] + ax * ay * sizes[1, 1, 1])
        return in_rows // 4

    def wait_bytes(sem, tiles):
        view = spare.at[pl.ds(0, tiles)]
        pltpu.make_async_copy(view, view, sem).wait()

    def wait_exchanges(sem, pairs):
        for ax in choices[0]:
            for ay in choices[1]:
                for az in choices[2]:
                    here = (around_it[0] == ax) & (around_it[1] == ay) & (around_it[2] == az)
                    tiles = sum(tiles_of(c, s, ax, ay, az) for c, s in pairs)
                    if tiles:
                        @pl.when(here)
                        def _():
                            wait_bytes(sem, tiles)

    def receive(c, s):
        wait_exchanges(r_sem.at[c, s], [(c, s)])
        scaled = (s == 1) == (c == P_CHAIN)
        into, z_into = (cbuf.at[c], czbuf.at[c]) if scaled else (main.at[c, 2 * s], pack.at[c, 2 * s])
        hi, at_block = wide(is_hi, TALL), [wide(slot // per_block == k, TALL) for k in range(3)]
        faces = [jnp.where(hi, got[c, s, 1, k], got[c, s, 0, k]) for k in range(3)]
        for b in range(RUN):
            value = jnp.zeros((TALL * cy, LANES), F32)
            for k in range(3):
                moved = roll_lanes(faces[k], group * per_block * (k - b))
                value = jnp.where(at_block[k], moved, value)
            z_into[b] = value * ztab[0, ZD + b] if scaled else value
        reach = REACH[s][c]
        for x in range(-reach, cx + reach):
            if 0 <= x < cx:
                ys = [0, 2 * cy]
            elif x in (-reach, cx + reach - 1):
                ys = [cy]
            else:
                ys = [0, cy, 2 * cy]
            for y in ys:
                ds = pl.ds(y, cy)
                value = roll_lanes(raw[c, s, x + cx, ds], turn(x))
                into[x + cx, ds] = value * d_tab[0, x + cx, ds] if scaled else value
            if scaled and s == 0 and 0 <= x < cx:
                ds = pl.ds(cy, cy)
                into[x + cx, ds] = main[c, 0, x + cx, ds] * d_tab[0, x + cx, ds]

    def own(c, f):
        return main[c, f, pl.ds(cx, cx), pl.ds(cy, cy)].reshape(cx * cy, LANES)

    def emit(c, f, slot_out):
        turn_back(lambda x: main[c, f, x + cx, pl.ds(cy, cy)], pow_ref.at[c, slot_out])

    place_of = {a: (P_CHAIN, a) for a in range(STEPS + 1)}
    place_of.update({STEPS + 1 + k: (Z_CHAIN, k + 1) for k in range(STEPS)})
    ready = []

    def account(a):
        ready.append(a)
        picture = image[a].reshape(cx * cy, LANES)
        for b in ready:
            part = jnp.sum(own(*place_of[b]) * picture, axis=0, keepdims=True)
            t_ref[pl.ds(a * total + b, 1), :] = part
            if a != b:
                t_ref[pl.ds(b * total + a, 1), :] = part
        t_ref[pl.ds(total * total + a, 1), :] = jnp.sum(
            own(*place_of[a]) * own(Z_CHAIN, 0), axis=0, keepdims=True)

    for copy in loads:
        copy.wait()
    for c in (Z_CHAIN, P_CHAIN):
        value = jnp.zeros((cy, LANES), F32)
        for x in range(cx):
            at = per_block * (x % RUN) + x // RUN
            value = jnp.where(slot == at, roll_lanes(raw[c, 0, x + cx, pl.ds(cy, cy)], group * at), value)
        face[c, 0] = value
    pl.semaphore_wait(barrier, expected)
    for c in (Z_CHAIN, P_CHAIN):
        send(c, 0)
    for c in (Z_CHAIN, P_CHAIN):
        turn_own(c)
    fill_zeros()
    fill_tables()
    t_ref[...] = jnp.zeros_like(t_ref)

    def finish_first(c, source):
        turn_back(source, raw.at[c, 1, pl.ds(cx, cx), pl.ds(cy, cy)])
        pack_face(c, 1, source)
        send(c, 1)

    first_z = STEPS + 1
    receive(Z_CHAIN, 0)
    apply_m(Z_CHAIN, 1, 3, TALL)
    apply_a(Z_CHAIN, 1, 2, first_z, SHORT)
    apply_m(Z_CHAIN, 2, 0, SHORT)
    finish_first(Z_CHAIN, lambda x: main[Z_CHAIN, 2, x + cx, pl.ds(cy, cy)])

    receive(P_CHAIN, 0)
    apply_a(P_CHAIN, 0, 6, 0, TALL)
    apply_m(P_CHAIN, 1, 4, TALL)
    apply_a(P_CHAIN, 1, 3, 1, SHORT)
    apply_m(P_CHAIN, 2, 1, SHORT)
    apply_a(P_CHAIN, 2, 0, 2, SHORT)
    finish_first(P_CHAIN, lambda x: image[2, x])
    for c in (Z_CHAIN, P_CHAIN):
        emit(c, 1, 0)
        emit(c, 2, 1)
    for a in (0, 1, 2, first_z):
        account(a)

    receive(Z_CHAIN, 1)
    apply_a(Z_CHAIN, 2, 6, first_z + 1, TALL)
    apply_m(Z_CHAIN, 3, 4, TALL)
    apply_a(Z_CHAIN, 3, 3, first_z + 2, SHORT)
    apply_m(Z_CHAIN, 4, 1, SHORT)
    apply_a(Z_CHAIN, 4, 0, first_z + 3, SHORT)
    for k in (1, 2, 3):
        account(first_z + k)
    for k in (3, 4):
        emit(Z_CHAIN, k, k - 1)

    receive(P_CHAIN, 1)
    apply_m(P_CHAIN, 3, 4, TALL)
    emit(P_CHAIN, 3, 2)
    apply_a(P_CHAIN, 3, 3, 3, SHORT)
    account(3)
    apply_m(P_CHAIN, 4, 1, SHORT)
    emit(P_CHAIN, 4, 3)
    apply_a(P_CHAIN, 4, 0, 4, SHORT)
    account(4)

    value = lax.dot_general(
        jnp.ones((8, LANES), F32), t_ref[...], (((1,), (1,)), ((), ())),
        precision=HIGHEST, preferred_element_type=F32)[0:1]

    def far_order(size, axes):
        def hops(k):
            far = 0
            for a in reversed(axes):
                n = counts[AXES.index(a)]
                k, step = divmod(k, n)
                far += min(step, n - step)
            return -far
        return sorted(range(1, size), key=hops)

    def gather(value, axes, buffer, send_sem, recv_sem, meanwhile=lambda: None):
        size, make = ahead(axes)
        mine = 0
        for a in axes:
            mine = mine * counts[AXES.index(a)] + place[AXES.index(a)]
        buffer[mine] = value

        def copy(k):
            return pltpu.make_async_remote_copy(
                buffer.at[mine], buffer.at[mine], send_sem.at[0], recv_sem.at[0],
                device_id=make(k), device_id_type=MESH)

        for k in far_order(size, axes):
            copy(k).start()
        meanwhile()
        rest = buffer.at[pl.ds(1, size - 1)]
        pltpu.make_async_copy(rest, rest, send_sem.at[0]).wait()
        pltpu.make_async_copy(rest, rest, recv_sem.at[0]).wait()
        parts = [buffer[k] for k in range(size)]
        while len(parts) > 1:
            parts = [sum(parts[i:i + 2][1:], parts[i]) for i in range(0, len(parts), 2)]
        result = parts[0]
        return result

    def finish():
        wait_exchanges(s_sem.at[0], [(c, s) for c in (0, 1) for s in (0, 1)])

    if near:
        value = gather(value, AXES, red0, s0_sem, r0_sem, finish)
    else:
        value = gather(value, ("gy", "gz"), red0, s0_sem, r0_sem, finish)
        value = gather(value, ("gx",), red1, s1_sem, r1_sem)
    value = value * (1.0 / (nx * cx * ny * cy * nz * cz))
    for a in range(total):
        gram_ref[a:a + 1, :] = value[0:1, a * total:(a + 1) * total]
    proj_ref[...] = value[0:1, total * total:total * total + total]


def store(pow_ref, gram_ref, proj_ref, pow_out, gram_out, proj_out, sem):
    pairs = ((pow_ref, pow_out), (gram_ref, gram_out), (proj_ref, proj_out))
    copies = [pltpu.make_async_copy(a, b, sem.at[i]) for i, (a, b) in enumerate(pairs)]
    for copy in copies:
        copy.start()
    for copy in copies:
        copy.wait()


def solution(mesh):
    counts = tuple(mesh.shape[a] for a in AXES)
    near = max(counts) <= 4
    devices = counts[0] * counts[1] * counts[2]
    plane = devices if near else counts[1] * counts[2]

    def local(residual, direction):
        dims = residual.shape
        cx, cy, cz = dims
        assert cz == LANES and LANES % cx == 0 and cy % 8 == 0
        assert min(cx, cy, LANES // cx // 2) > max(max(r) for r in REACH)
        total = 2 * STEPS + 1
        fields = STEPS + 1
        dma = pltpu.SemaphoreType.DMA
        vm = pl.BlockSpec(memory_space=pltpu.VMEM)
        hbm = pl.BlockSpec(memory_space=pltpu.HBM)
        ext = (3 * cx, 3 * cy, LANES)
        zext = (RUN, 3 * cy, LANES)
        powers, gram, proj = pl.pallas_call(
            functools.partial(kernel, counts, dims, near),
            out_shape=(
                jax.ShapeDtypeStruct((2, STEPS) + dims, F32),
                jax.ShapeDtypeStruct((total, total), F32),
                jax.ShapeDtypeStruct((1, total), F32),
            ),
            in_specs=[hbm, hbm],
            out_specs=(vm, vm, vm),
            scratch_shapes=[
                pltpu.VMEM((2, 2) + ext, F32),
                pltpu.VMEM((2, fields) + ext, F32),
                pltpu.VMEM((2, fields) + zext, F32),
                pltpu.VMEM((2, 2, 2, 3, 3 * cy, LANES), F32),
                pltpu.VMEM((2, 2, cy, LANES), F32),
                pltpu.VMEM((2, STEPS) + dims, F32),
                pltpu.VMEM((2,) + ext, F32),
                pltpu.VMEM((2,) + zext, F32),
                pltpu.VMEM((2,) + ext, F32),
                pltpu.VMEM((2,) + zext, F32),
                pltpu.VMEM((total,) + dims, F32),
                pltpu.VMEM((2,) + ext, F32),
                pltpu.VMEM((2,) + zext, F32),
                pltpu.VMEM((2, 8, 3 * cy, LANES), F32),
                pltpu.VMEM((2, 6 * RUN, 3 * cy, LANES), F32),
                pltpu.VMEM((3 * cx // RUN + 1, cy, LANES), F32),
                pltpu.VMEM((2,) + ext, F32),
                pltpu.VMEM((2,) + ext, F32),
                pltpu.VMEM((LANES, LANES), F32),
                pltpu.VMEM((plane, 1, LANES), F32),
                pltpu.VMEM((counts[0], 1, LANES), F32),
                pltpu.VMEM((4 * 9 * cx * (cy // 4), 4, LANES), F32),
                dma((2,)), dma((1,)),
                dma((1,)), dma((2, 2)),
                dma((1,)), dma((1,)),
                dma((1,)), dma((1,)),
            ],
            compiler_params=pltpu.CompilerParams(collective_id=0, has_side_effects=True, vmem_limit_bytes=24 << 20),
            name="powers_basis",
        )(*[pltpu.with_memory_space_constraint(v, pltpu.HBM) for v in (residual, direction)])
        powers, gram, proj = pl.pallas_call(
            store,
            out_shape=(
                jax.ShapeDtypeStruct((2, STEPS) + dims, F32),
                jax.ShapeDtypeStruct((total, total), F32),
                jax.ShapeDtypeStruct((1, total), F32),
            ),
            in_specs=[vm, vm, vm],
            out_specs=(hbm, hbm, hbm),
            scratch_shapes=[dma((3,))],
            compiler_params=pltpu.CompilerParams(vmem_limit_bytes=1 << 20),
            name="store",
        )(powers, gram, proj)
        return powers, gram, proj.reshape(total)

    placed = (P("gx", "gy", "gz"), P("gx", "gy", "gz"))
    return jax.shard_map(
        local,
        mesh=mesh,
        in_specs=placed,
        out_specs=(P(None, None, "gx", "gy", "gz"), P(), P()),
        check_vma=False,
    )
```
